256 devices in a mesh: tm: 8 (over z), space: 32 (over y, x, core).
Axes of the slice: x: 4, y: 4, z: 8, core: 2. Of those that a mesh axis runs over, the one named last changes fastest.
Arguments:
- labels: int32 [128, 64, 256], P('space'), may hold values from 0 to 3
- conductivity: float32 [4], replicated, may hold values from 0.02 to 1
- coil_pattern: float32 [3, 128, 64, 256], P(None, 'space'), may hold values from -18 to 18
- currents: float32 [8, 2, 3], P('tm'), may hold values from -4 to 4
- initial_state: float32 [128, 64, 256], P('space'), may hold values from -6 to 6
Outputs:
- slice_starts: float32 [8, 128, 64, 256], P('tm', 'space')
- fine_ends: float32 [8, 128, 64, 256], P('tm', 'space')
The draws below stay inside these ranges and needn't reach their ends.
All inputs are finite; a program needn't handle non-finite values.
Results may differ from the reference program's by a relative error of at most 0.00021.
Values sent between devices are 32-bit elements; how exact they have to be, the bound alone decides.
No kernel may reach another device: no remote copies, remote signals or barrier semaphores. Data moves between devices by JAX's collectives and lax.ppermute only.
A program may use at most 64 MiB of HBM per device.

```python
import math
import jax
import jax.numpy as jnp

NY = 64
NZ = 256
REGIONS = 4
PHASES = 3
FINE_STEPS = 2
CG_FINE = 2
CG_COARSE = 4
PARA_ITERS = 2
SLICES = 8
NX = 128


def draw_coil_pattern(key, part):
    shape = (PHASES, NX, NY, NZ)
    rows = jnp.arange(NX, dtype=jnp.float32) / max(NX - 1, 1)
    noise = jax.random.truncated_normal(key, -4.0, 4.0, shape, jnp.float32)
    return noise * (3.0 ** rows)[None, :, None, None]


def with_ends(entries, stream_key, low, high):
    shape = entries.shape
    index_at = [jax.random.randint(jax.random.fold_in(stream_key, axis), (), 0, shape[axis]) for axis in range(len(shape))]
    entries = entries.at[tuple(index_at)].set(low)
    longest = shape.index(max(shape))
    index_at[longest] = (index_at[longest] + 1) % shape[longest]
    return entries.at[tuple(index_at)].set(high)


def block_scale(own_key, shape, cuts, least, high):
    def one(axis_at, shards_of):
        heights = jax.random.uniform(jax.random.fold_in(jax.random.fold_in(own_key, 6), axis_at), (shards_of,), jnp.float32, least / len(cuts), high / len(cuts))
        return jnp.repeat(jnp.exp(heights), shape[axis_at] // shards_of).reshape((-1,) + (1,) * (len(shape) - axis_at - 1))

    factor_of = one(*cuts[0])
    for cut in cuts[1:]:
        factor_of = factor_of * one(*cut)
    return factor_of


def gaussian(own_key, dims, deviation, limit, pieces=(), kind=jnp.bfloat16):
    factor_of = block_scale(own_key, dims, pieces, -0.22, 0.18) if pieces else 1.0
    array = jax.random.normal(own_key, dims, jnp.float32) * deviation * factor_of
    return jnp.minimum(jnp.maximum(array, -limit), limit).astype(kind)


def setup_inputs(seed: int = 0) -> dict:
    key_list = jax.random.split(jax.random.key(seed), 6)
    return {
        "labels": with_ends(jax.random.randint(key_list[0], (NX, NY, NZ), 0, REGIONS), jax.random.fold_in(key_list[0], 1), 0, REGIONS - 1).astype(jnp.int32),
        "conductivity": jnp.clip(jnp.exp(jax.random.uniform(key_list[1], (REGIONS,), jnp.float32, math.log(0.02), math.log(1.0))), 0.02, 1.0),
        "coil_pattern": draw_coil_pattern(jax.random.fold_in(key_list[5], 71), 0),
        "currents": gaussian(key_list[3], (SLICES, FINE_STEPS, PHASES), 1.0, 4.0, ((0, 8),), jnp.float32),
        "initial_state": gaussian(key_list[4], (NX, NY, NZ), 1.0, 6.0, ((0, 32),), jnp.float32),
    }


def restrict(volume):
    first_dim, second_dim, third_dim = volume.shape
    blocks = volume.reshape(first_dim // 4, 4, second_dim // 4, 4, third_dim // 4, 4)
    return jnp.mean(blocks, axis=(1, 3, 5))


def prolong(coarse_field):
    first_dim, second_dim, third_dim = coarse_field.shape
    spread = jnp.broadcast_to(coarse_field[:, None, :, None, :, None], (first_dim, 4, second_dim, 4, third_dim, 4))
    return spread.reshape(first_dim * 4, second_dim * 4, third_dim * 4)


def neighbours(padded):
    summed = padded[2:, 1:-1, 1:-1] + padded[:-2, 1:-1, 1:-1]
    summed = summed + padded[1:-1, 2:, 1:-1] + padded[1:-1, :-2, 1:-1]
    return summed + padded[1:-1, 1:-1, 2:] + padded[1:-1, 1:-1, :-2]


def fine_operator(volume, weight):
    beside = neighbours(jnp.pad(volume, 1))
    return weight * volume + (6.0 * volume - beside)


def coarse_operator(volume, weight):
    beside = neighbours(jnp.pad(volume, 1))
    return weight * volume + 0.0625 * (6.0 * volume - beside)


def conjugate(operator, right_side, guess, count):
    solution = guess
    residual = right_side - operator(solution)
    direction = residual
    res_norm = jnp.sum(residual * residual)
    for sweep_step in range(count):
        applied = operator(direction)
        step_len = res_norm / jnp.sum(direction * applied)
        solution = solution + step_len * direction
        residual = residual - step_len * applied
        if sweep_step + 1 < count:
            new_norm = jnp.sum(residual * residual)
            direction = residual + (new_norm / res_norm) * direction
            res_norm = new_norm
    return solution


def reference(labels, conductivity, coil_pattern, currents, initial_state):
    sigma_cell = conductivity[labels]
    sigma_coarse = restrict(sigma_cell)
    coils_coarse = jnp.stack([restrict(coil_pattern[phase_index]) for phase_index in range(PHASES)])
    weight_coarse = sigma_coarse / float(FINE_STEPS)

    def fine_run(slice_index, volume):
        for step_index in range(FINE_STEPS):
            source = currents[slice_index, step_index, 0] * coil_pattern[0]
            for phase_index in range(1, PHASES):
                source = source + currents[slice_index, step_index, phase_index] * coil_pattern[phase_index]
            right_side = sigma_cell * volume + source
            volume = conjugate(lambda vector_in: fine_operator(vector_in, sigma_cell), right_side, volume, CG_FINE)
        return volume

    def coarse_run(slice_index, volume):
        coarse_start = restrict(volume)
        mean_current = jnp.mean(currents[slice_index], axis=0)
        source = mean_current[0] * coils_coarse[0]
        for phase_index in range(1, PHASES):
            source = source + mean_current[phase_index] * coils_coarse[phase_index]
        right_side = weight_coarse * coarse_start + source
        solved = conjugate(lambda vector_in: coarse_operator(vector_in, weight_coarse), right_side, coarse_start, CG_COARSE)
        return prolong(solved)

    starts = [initial_state]
    coarse_out = []
    for slice_index in range(SLICES):
        coarse_out.append(coarse_run(slice_index, starts[slice_index]))
        starts.append(coarse_out[slice_index])
    fine_out = []
    for para_index in range(PARA_ITERS):
        fine_out = [fine_run(slice_index, starts[slice_index]) for slice_index in range(SLICES)]
        new_starts = [starts[SLICES]]
        new_coarse = []
        for slice_index in range(SLICES):
            coarse_result = coarse_run(slice_index, new_starts[slice_index])
            new_coarse.append(coarse_result)
            new_starts.append(coarse_result + fine_out[slice_index] - coarse_out[slice_index])
        starts = new_starts
        coarse_out = new_coarse
    return jnp.stack(starts[:SLICES]), jnp.stack(fine_out)
```

```python
import functools

import jax
import jax.numpy as jnp
from jax import lax
from jax.experimental import pallas as pl
from jax.experimental.pallas import tpu as pltpu
from jax.sharding import PartitionSpec as P

PHASES = 3
CG_COARSE = 4
F32 = jnp.float32
HIGHEST = lax.Precision.HIGHEST
VMEM = pltpu.MemorySpace.VMEM
SMEM = pltpu.MemorySpace.SMEM
INTERPRET = False
LIMIT = 20 << 20


def iota(shape, dim):
    return lax.broadcasted_iota(jnp.int32, shape, dim)


def dot(a, b):
    return lax.dot_general(a, b, (((1,), (0,)), ((), ())), precision=HIGHEST, preferred_element_type=F32)


def total(x):
    while x.ndim > 2:
        x = jnp.sum(x, axis=0)
    return jnp.sum(jnp.sum(x, axis=0, keepdims=True), axis=1, keepdims=True)


def restrict_packed(summed):
    columns = (iota((256, 128), 0) >> 2) == (iota((256, 128), 1) & 63)
    rows = (iota((16, 64), 1) >> 2) == iota((16, 64), 0)
    half = dot(summed, jnp.where(columns, 1.0 / 64.0, 0.0).astype(F32))
    both = dot(jnp.where(rows, 1.0, 0.0).astype(F32), half)
    return jnp.where(iota((8, 128), 1) < 64, both[:8], both[8:])


def widen(planes):
    columns = (iota((128, 256), 1) >> 2) == iota((128, 256), 0)
    rows = (iota((64, 16), 0) >> 2) == iota((64, 16), 1)
    wide = dot(planes, jnp.where(columns, 1.0, 0.0).astype(F32))
    lift = jnp.where(rows, 1.0, 0.0).astype(F32)
    return [dot(lift, wide[k : k + 16]) for k in range(0, planes.shape[0], 16)]


def unpack(low, high):
    axis = low.ndim - 1
    left = iota(low.shape, axis) < 64
    top = jnp.where(left, low, pltpu.roll(high, 64, axis))
    bottom = jnp.where(left, pltpu.roll(low, 64, axis), high)
    return jnp.concatenate([top, bottom], axis=axis - 1)


def coarse_beside(v):
    one = (1, 16, 128)
    lane, row = iota(one, 2), iota(one, 1)
    left = lane < 64
    first, last = pltpu.roll(v[:1], 64, 2), pltpu.roll(v[15:], 64, 2)
    after = jnp.concatenate([v[1:], jnp.where(left, first, 0.0)], axis=0)
    before = jnp.concatenate([jnp.where(left, 0.0, last), v[:15]], axis=0)
    out = after + before
    out = out + jnp.where(row == 0, 0.0, pltpu.roll(v, 1, 1)) + jnp.where(row == 15, 0.0, pltpu.roll(v, 15, 1))
    inner = lane & 63
    return out + jnp.where(inner == 0, 0.0, pltpu.roll(v, 1, 2)) + jnp.where(inner == 63, 0.0, pltpu.roll(v, 127, 2))


def coarse_solve(start, source, diagonal):
    def apply(v):
        return diagonal * v - 0.0625 * coarse_beside(v)

    x = start
    residual = source - 0.375 * start + 0.0625 * coarse_beside(start)
    image = apply(residual)
    norm, product = total(residual * residual), total(residual * image)
    step = norm / product
    direction, moved = residual, image
    for turn in range(CG_COARSE):
        x = x + step[None] * direction
        if turn + 1 < CG_COARSE:
            residual = residual - step[None] * moved
            image = apply(residual)
            new, product = total(residual * residual), total(residual * image)
            ratio = new / norm
            step = new / (product - ratio * new / step)
            direction = residual + ratio[None] * direction
            moved = image + ratio[None] * moved
            norm = new
    return x


def cut_planes(state, place, offsets):
    out = []
    lane = iota((16, 128), 1)
    for offset in offsets:
        at = place + offset
        inside = jnp.logical_and(at >= 0, at < 32).astype(jnp.int32)
        at = jnp.clip(at, 0, 31)
        plane = state[at & 15]
        plane = jnp.where((at >> 4) * jnp.ones_like(lane) == 1, pltpu.roll(plane, 64, 1), plane)
        out.append(jnp.where(lane < 64 * inside, plane, 0.0))
    return out


def call(body, outs, args, small=(), scratch=(), flops=0):
    specs = [pl.BlockSpec(memory_space=SMEM if k in small else VMEM) for k in range(len(args))]
    return pl.pallas_call(
        body,
        out_shape=tuple(jax.ShapeDtypeStruct(s, F32) for s in outs),
        in_specs=specs,
        out_specs=tuple(pl.BlockSpec(memory_space=VMEM) for _ in outs),
        scratch_shapes=tuple(pltpu.VMEM(s, F32) for s in scratch),
        cost_estimate=pl.CostEstimate(flops=flops, bytes_accessed=1 << 20, transcendentals=0) if flops else None,
        compiler_params=pltpu.CompilerParams(vmem_limit_bytes=LIMIT),
        interpret=INTERPRET,
    )(*args)


def setup_kernel(cond, cur, labels, coils, initial, sigma, sources, up, down, far, packed):
    region = labels[...]
    cell = jnp.where(region == 0, cond[0], 0.0)
    for k in range(1, 4):
        cell = cell + jnp.where(region == k, cond[k], 0.0)
    sigma[...] = cell
    pattern = [coils[p] for p in range(PHASES)]
    for step in range(2):
        source = cur[step, 0] * pattern[0]
        for p in range(1, PHASES):
            source = source + cur[step, p] * pattern[p]
        sources[step] = source
    up[0:2] = sigma[2:4]
    up[2:5] = sources[0, 1:4]
    up[5:6] = sources[1, 3:4]
    down[0:3] = sigma[0:3]
    down[3:7] = sources[0]
    down[7:9] = sources[1, 0:2]
    up[6:10] = initial[...]
    down[9:13] = initial[...]
    far[...] = initial[0:1]
    fields = [initial[...], cell, *pattern]
    rows = [restrict_packed(jnp.sum(f, axis=0)) for f in fields]
    rows = jnp.concatenate([*rows, jnp.zeros((8, 128), F32)], axis=0)
    packed[...] = jnp.broadcast_to(rows[None], packed.shape)


def unpack_all(whole, at):
    return unpack(whole[0:16, at : at + 8, :], whole[16:32, at : at + 8, :])


def sweep(where, cur, state, static, advanced, planes, correction, count):
    mine, place = where[0], where[1]
    diagonal = static[1] * 0.5 + 0.375

    def turn(n, carry):
        if planes is not None:

            @pl.when(n == mine)
            def _():
                for k, plane in enumerate(cut_planes(state, place, (-1, 0, 1, 2))):
                    planes[16 * k : 16 * k + 16] = plane

        source = jnp.zeros((16, 16, 128), F32)
        for p in range(PHASES):
            mean = 0.5 * (cur[n, p] + cur[n, PHASES + p])
            source = source + mean * static[2 + p]
        solved = coarse_solve(state[...], source, static[1] * 0.5 + 0.375)
        if advanced is not None:
            advanced[n] = solved
        state[...] = solved if correction is None else solved + correction[n]
        return carry

    lax.fori_loop(0, count, turn, 0)


def first_sweep_kernel(where, cur, whole, static, planes, advanced, state):
    for k in range(5):
        static[k] = unpack_all(whole, 8 * k)
    state[...] = static[0]
    sweep(where, cur, state, static, advanced, planes, None, 8)


def load_corrections(where, ends, before, correction):
    for end, offset in zip(ends, OFFSETS):
        n = (where[0] + offset) & 7
        correction[n] = unpack(end[0:16], end[16:32]) - before[n]


OFFSETS = (0, -1, 1, -2, 2, -3, 3, -4)


def next_sweep_kernel(where, cur, static, before, begin, *refs):
    ends, (planes, advanced, state, correction) = refs[:8], refs[8:]
    load_corrections(where, ends, before, correction)
    state[...] = begin[...]
    sweep(where, cur, state, static, advanced, planes, correction, 8)


def last_sweep_kernel(where, cur, static, before, begin, rest_first, rest_other, *refs):
    ends, (start, state, correction, planes) = refs[:8], refs[8:]
    load_corrections(where, ends, before, correction)
    state[...] = begin[...]

    def keep():
        (plane,) = cut_planes(state, where[1], (0,))
        planes[...] = plane

    mine = where[0]

    def turn(n, carry):
        source = jnp.zeros((16, 16, 128), F32)
        for p in range(PHASES):
            mean = 0.5 * (cur[n, p] + cur[n, PHASES + p])
            source = source + mean * static[2 + p]
        state[...] = coarse_solve(state[...], source, static[1] * 0.5 + 0.375) + correction[n]
        return carry

    lax.fori_loop(0, mine, turn, 0)
    keep()
    (own,) = widen(planes[...])
    first = (mine == 0).astype(F32)
    start[...] = own[None] + (first * rest_first[...] + (1.0 - first) * rest_other[...])


def fine_beside(v):
    rows, lanes = iota(v.shape, 0), iota(v.shape, 1)
    out = jnp.where(rows == 0, 0.0, pltpu.roll(v, 1, 0)) + jnp.where(rows == 63, 0.0, pltpu.roll(v, 63, 0))
    return out + jnp.where(lanes == 0, 0.0, pltpu.roll(v, 1, 1)) + jnp.where(lanes == 255, 0.0, pltpu.roll(v, 255, 1))


def inside(plane):
    return jnp.logical_and(plane >= 0, plane < 128).astype(F32)


def each(pieces, body):
    at = 0
    for read, count in pieces:

        def one(i, carry, read=read, at=at):
            body(at + i, read(i))
            return carry

        lax.fori_loop(0, count, one, 0)
        at += count


def residual_planes(field, source, out, first):
    def body(j, piece):
        v = field[j + 1]
        r = piece - 6.0 * v + (field[j] + field[j + 2]) + fine_beside(v)
        out[j] = inside(first + j) * r

    each(source, body)


def image_planes(field, weight, out, first):
    def body(j, piece):
        v = field[j + 1]
        w = (piece + 6.0) * v - (field[j] + field[j + 2]) - fine_beside(v)
        out[j] = inside(first + j) * w

    each(weight, body)


def moments(r, r_at, w, w_at, sigma):
    def body(i, sums):
        a, b, c = r[r_at + i], w[w_at + i], w[w_at + i + 1]
        cross = (sigma[i] + 6.0) * b - fine_beside(b) - 2.0 * c
        return (sums[0] + a * a, sums[1] + a * b, sums[2] + b * b, sums[3] + b * cross)

    zero = jnp.zeros((64, 256), F32)
    sums = lax.fori_loop(0, 4, body, (zero,) * 4)
    lane = iota((1, 128), 1)
    row = jnp.zeros((1, 128), F32)
    for k in range(4):
        row = jnp.where(lane == k, total(sums[k]), row)
    return row


def weights(row):
    lane = iota((1, 128), 1)
    m0, m1, m2, m3 = (jnp.sum(jnp.where(lane == k, row, 0.0), axis=1, keepdims=True) for k in range(4))
    step = m0 / m1
    new = step * step * m2 - m0
    product = m1 - 2.0 * step * m2 + step * step * m3
    ratio = new / m0
    second = new / (product - ratio * new / step)
    return step + second * (1.0 + ratio), -step * second


def fine_one_kernel(initial, where, planes, rest, rest_up, rest_down, rest_far, sigma, sources, up, down,
                    u_out, r_out, w_out, packed, u, r):
    first = 4 * where[1]
    zero = (where[0] == 0).astype(F32)
    scale = (1.0 - zero, zero) if initial else (1.0, 1.0 - zero)
    above, below = (6, 9) if initial else (0, 0)
    lifted = widen(planes[...])
    pieces = [(rest_up, above + k) for k in range(4)] + [(rest, k) for k in range(4)]
    pieces = pieces + [(rest_down, below + k) for k in range(4)] + [(rest_far, 0)]
    for j, (piece, k) in enumerate(pieces):
        u[j] = scale[0] * lifted[j // 4] + scale[1] * piece[k]
    source = ((lambda i: up[2 + i], 3), (lambda i: sources[0, i], 4), (lambda i: down[3 + i], 4))
    residual_planes(u, source, r, first - 3)
    weight = ((lambda i: up[i], 2), (lambda i: sigma[i], 4), (lambda i: down[i], 3))
    image_planes(r, weight, w_out, first - 2)
    u_out[...] = u[2:11]
    r_out[...] = r[1:10]
    packed[...] = jnp.broadcast_to(moments(r, 3, w_out, 2, sigma), packed.shape)


def fine_two_kernel(where, sums, u, r, w, sigma, sources, up, down, u_out, r_out, w_out, packed, u1, r1, w1):
    first = 4 * where[1]
    a, b = weights(jnp.sum(sums[...], axis=0, keepdims=True))

    def move(j, carry):
        u1[j] = u[j] + a * r[j] + b * w[j]
        return carry

    lax.fori_loop(0, 9, move, 0)
    source = ((lambda i: up[5 + i], 1), (lambda i: sources[1, i], 4), (lambda i: down[7 + i], 2))
    residual_planes(u1, source, r1, first - 1)
    weight = ((lambda i: sigma[i], 4), (lambda i: down[i], 1))
    image_planes(r1, weight, w1, first)
    u_out[...] = u1[2:6]
    r_out[...] = r1[1:5]
    w_out[...] = w1[0:4]
    row = moments(r1, 1, w1, 0, sigma)
    parts = [restrict_packed(jnp.sum(f[...], axis=0)) for f in (u_out, r_out, w_out)]
    rows = jnp.concatenate([*parts, jnp.broadcast_to(row, (8, 128))], axis=0)
    packed[...] = jnp.broadcast_to(rows[None], packed.shape)


def fine_three_kernel(where, whole, u, r, w, fine, rest, ends):
    a, b = weights(jnp.sum(whole[:, 24, :], axis=0, keepdims=True))
    ends[...] = whole[:, 0:8, :] + a[None] * whole[:, 8:16, :] + b[None] * whole[:, 16:24, :]
    own = ends[where[1]]
    left = iota((8, 128), 1) < 64
    plane = jnp.concatenate([jnp.where(left, own, 0.0), jnp.where(left, pltpu.roll(own, 64, 1), 0.0)], axis=0)
    (lifted,) = widen(plane)
    for i in range(4):
        value = u[i] + a * r[i] + b * w[i]
        fine[i] = value
        rest[i] = value - lifted


def shifted(x, axis, by, ring):
    n = lax.axis_size(axis)
    pairs = [(i, (i + by) % n) for i in range(n) if ring or 0 <= i + by < n]
    return lax.ppermute(x, axis, pairs)


def exchange(x, axis):
    return lax.all_to_all(x, axis, split_axis=0, concat_axis=0, tiled=True)


def around(x):
    ends, ahead, behind = [x], x, x
    for k in range(1, 5):
        ahead = shifted(ahead, "tm", 1, True)
        ends.append(ahead)
        if k < 4:
            behind = shifted(behind, "tm", -1, True)
            ends.append(behind)
    return ends


def halos(x):
    return (
        shifted(x, "space", 1, False),
        shifted(x, "space", -1, False),
        shifted(x[:1], "space", -2, False),
    )


def body(labels, conductivity, coil_pattern, currents, initial_state):
    tm, place = lax.axis_index("tm"), lax.axis_index("space")
    where = jnp.stack([tm, place]).astype(jnp.int32)
    block, field = (4, 64, 256), (16, 16, 128)

    slices, across = lax.axis_size("tm"), lax.axis_size("space")
    pairs = [
        (b * across + slices * a + t, t * across + slices * a + b)
        for t in range(slices)
        for b in range(slices)
        for a in range(across // slices)
    ]
    theirs = lax.ppermute(jnp.pad(currents.reshape(1, 6), ((0, 0), (0, 122))), ("tm", "space"), pairs)

    sigma, sources, up, down, far, packed = call(
        setup_kernel,
        (block, (2, *block), (10, 64, 256), (13, 64, 256), (1, 64, 256), (32, 48, 128)),
        (conductivity, currents[0], labels, coil_pattern, initial_state),
        small=(0, 1),
    )
    packed = lax.dynamic_update_slice(packed, jnp.broadcast_to(theirs[None], (32, 1, 128)), (0, 40, 0))
    whole = exchange(packed, "space")
    table = whole[:8, 40, :]
    up, down = shifted(up, "space", 1, False), shifted(down, "space", -1, False)
    far = shifted(far, "space", -2, False)
    static, planes, advanced, state = call(
        first_sweep_kernel,
        ((5, *field), (64, 128), (8, *field), field),
        (where, table, whole),
        small=(0, 1),
        flops=1 << 26,
    )

    def fine(initial, planes, rest, around_rest):
        u, r, w, sums = call(
            functools.partial(fine_one_kernel, initial),
            ((9, 64, 256), (9, 64, 256), (9, 64, 256), (32, 128)),
            (where, planes, rest, *around_rest, sigma, sources, up, down),
            small=(0,),
            scratch=((13, 64, 256), (11, 64, 256)),
        )
        u, r, w, packed = call(
            fine_two_kernel,
            (block, block, block, (32, 32, 128)),
            (where, exchange(sums, "space"), u, r, w, sigma, sources, up, down),
            small=(0,),
            scratch=((9, 64, 256), (7, 64, 256), (5, 64, 256)),
        )
        return call(
            fine_three_kernel,
            (block, block, (32, 8, 128)),
            (where, exchange(packed, "space"), u, r, w),
            small=(0,),
        )

    _, rest, ends = fine(True, planes, initial_state, (up, down, far))
    rest_first = shifted(rest, "tm", 1, True)
    planes, advanced_next, state_next = call(
        next_sweep_kernel,
        ((64, 128), (8, *field), field),
        (where, table, static, advanced, state, *around(ends)),
        small=(0, 1),
        scratch=((8, *field),),
        flops=1 << 26,
    )
    fine_state, rest, ends = fine(False, planes, rest_first, halos(rest_first))
    rest_other = shifted(rest, "tm", 1, False)
    (start,) = call(
        last_sweep_kernel,
        (block,),
        (where, table, static, advanced_next, state_next, rest_first, rest_other, *around(ends)),
        small=(0, 1),
        scratch=(field, (8, *field), (16, 128)),
        flops=1 << 26,
    )
    return (start[None], fine_state[None])


def solution(mesh):
    in_specs = (
        P("space", None, None),
        P(),
        P(None, "space", None, None),
        P("tm", None, None),
        P("space", None, None),
    )
    out_specs = (P("tm", "space", None, None), P("tm", "space", None, None))
    return jax.shard_map(body, mesh=mesh, in_specs=in_specs, out_specs=out_specs, check_vma=False)
```

```python
import functools

import jax
import jax.numpy as jnp
from jax import lax
from jax.experimental import pallas as pl
from jax.experimental.pallas import tpu as pltpu
from jax.sharding import PartitionSpec as P

PHASES = 3
CG_COARSE = 4
F32 = jnp.float32
HIGHEST = lax.Precision.HIGHEST
VMEM = pltpu.MemorySpace.VMEM
SMEM = pltpu.MemorySpace.SMEM
INTERPRET = False
LIMIT = 20 << 20


def iota(shape, dim):
    return lax.broadcasted_iota(jnp.int32, shape, dim)


def dot(a, b):
    return lax.dot_general(a, b, (((1,), (0,)), ((), ())), precision=HIGHEST, preferred_element_type=F32)


def total(x):
    while x.ndim > 2:
        x = jnp.sum(x, axis=0)
    return jnp.sum(jnp.sum(x, axis=0, keepdims=True), axis=1, keepdims=True)


def restrict_packed(summed):
    columns = (iota((256, 128), 0) >> 2) == (iota((256, 128), 1) & 63)
    rows = (iota((16, 64), 1) >> 2) == iota((16, 64), 0)
    half = dot(summed, jnp.where(columns, 1.0 / 64.0, 0.0).astype(F32))
    both = dot(jnp.where(rows, 1.0, 0.0).astype(F32), half)
    return jnp.where(iota((8, 128), 1) < 64, both[:8], both[8:])


def widen(planes):
    columns = (iota((128, 256), 1) >> 2) == iota((128, 256), 0)
    rows = (iota((64, 16), 0) >> 2) == iota((64, 16), 1)
    wide = dot(planes, jnp.where(columns, 1.0, 0.0).astype(F32))
    lift = jnp.where(rows, 1.0, 0.0).astype(F32)
    return [dot(lift, wide[k : k + 16]) for k in range(0, planes.shape[0], 16)]


def unpack(low, high):
    axis = low.ndim - 1
    left = iota(low.shape, axis) < 64
    top = jnp.where(left, low, pltpu.roll(high, 64, axis))
    bottom = jnp.where(left, pltpu.roll(low, 64, axis), high)
    return jnp.concatenate([top, bottom], axis=axis - 1)


def coarse_beside(v):
    one = (1, 16, 128)
    lane, row = iota(one, 2), iota(one, 1)
    left = lane < 64
    first, last = pltpu.roll(v[:1], 64, 2), pltpu.roll(v[15:], 64, 2)
    after = jnp.concatenate([v[1:], jnp.where(left, first, 0.0)], axis=0)
    before = jnp.concatenate([jnp.where(left, 0.0, last), v[:15]], axis=0)
    out = after + before
    out = out + jnp.where(row == 0, 0.0, pltpu.roll(v, 1, 1)) + jnp.where(row == 15, 0.0, pltpu.roll(v, 15, 1))
    inner = lane & 63
    return out + jnp.where(inner == 0, 0.0, pltpu.roll(v, 1, 2)) + jnp.where(inner == 63, 0.0, pltpu.roll(v, 127, 2))


def coarse_solve(start, source, diagonal):
    def apply(v):
        return diagonal * v - 0.0625 * coarse_beside(v)

    x = start
    residual = source - 0.375 * start + 0.0625 * coarse_beside(start)
    image = apply(residual)
    norm, product = total(residual * residual), total(residual * image)
    step = norm / product
    direction, moved = residual, image
    for turn in range(CG_COARSE):
        inverse = 1.0 / norm
        scaled = inverse / step
        x = x + step[None] * direction
        if turn + 1 < CG_COARSE:
            residual = residual - step[None] * moved
            image = apply(residual)
            new, product = total(residual * residual), total(residual * image)
            ratio = new * inverse
            step = new / (product - new * (new * scaled))
            direction = residual + ratio[None] * direction
            moved = image + ratio[None] * moved
            norm = new
    return x


def cut_planes(state, place, offsets):
    out = []
    lane = iota((16, 128), 1)
    for offset in offsets:
        at = place + offset
        inside = jnp.logical_and(at >= 0, at < 32).astype(jnp.int32)
        at = jnp.clip(at, 0, 31)
        plane = state[at & 15]
        plane = jnp.where((at >> 4) * jnp.ones_like(lane) == 1, pltpu.roll(plane, 64, 1), plane)
        out.append(jnp.where(lane < 64 * inside, plane, 0.0))
    return out


def call(body, outs, args, small=(), scratch=(), flops=0):
    specs = [pl.BlockSpec(memory_space=SMEM if k in small else VMEM) for k in range(len(args))]
    return pl.pallas_call(
        body,
        out_shape=tuple(jax.ShapeDtypeStruct(s, F32) for s in outs),
        in_specs=specs,
        out_specs=tuple(pl.BlockSpec(memory_space=VMEM) for _ in outs),
        scratch_shapes=tuple(pltpu.VMEM(s, F32) for s in scratch),
        cost_estimate=pl.CostEstimate(flops=flops, bytes_accessed=1 << 20, transcendentals=0) if flops else None,
        compiler_params=pltpu.CompilerParams(vmem_limit_bytes=LIMIT),
        interpret=INTERPRET,
    )(*args)


def setup_kernel(cond, cur, theirs, labels, coils, initial, sigma, sources, up, down, far, packed):
    region = labels[...]
    cell = jnp.where(region == 0, cond[0], 0.0)
    for k in range(1, 4):
        cell = cell + jnp.where(region == k, cond[k], 0.0)
    sigma[...] = cell
    pattern = [coils[p] for p in range(PHASES)]
    for step in range(2):
        source = cur[step, 0] * pattern[0]
        for p in range(1, PHASES):
            source = source + cur[step, p] * pattern[p]
        sources[step] = source
    up[0:2] = sigma[2:4]
    up[2:5] = sources[0, 1:4]
    up[5:6] = sources[1, 3:4]
    down[0:3] = sigma[0:3]
    down[3:7] = sources[0]
    down[7:9] = sources[1, 0:2]
    up[6:10] = initial[...]
    down[9:13] = initial[...]
    far[...] = initial[0:1]
    fields = [initial[...], cell, *pattern]
    rows = [restrict_packed(jnp.sum(f, axis=0)) for f in fields]
    rows = jnp.concatenate([*rows, jnp.broadcast_to(theirs[...], (8, 128))], axis=0)
    packed[...] = jnp.broadcast_to(rows[None], packed.shape)


def unpack_all(whole, at):
    return unpack(whole[0:16, at : at + 8, :], whole[16:32, at : at + 8, :])


def sweep(where, cur, state, static, advanced, planes, correction, count):
    mine, place = where[0], where[1]
    diagonal = static[1] * 0.5 + 0.375

    def turn(n, carry):
        if planes is not None:

            @pl.when(n == mine)
            def _():
                for k, plane in enumerate(cut_planes(state, place, (-1, 0, 1, 2))):
                    planes[16 * k : 16 * k + 16] = plane

        source = jnp.zeros((16, 16, 128), F32)
        for p in range(PHASES):
            mean = 0.5 * (cur[n, p] + cur[n, PHASES + p])
            source = source + mean * static[2 + p]
        solved = coarse_solve(state[...], source, static[1] * 0.5 + 0.375)
        if advanced is not None:
            advanced[n] = solved
        state[...] = solved if correction is None else solved + correction[n]
        return carry

    lax.fori_loop(0, count, turn, 0)


def first_sweep_kernel(where, cur, whole, static, planes, advanced, state):
    for k in range(5):
        static[k] = unpack_all(whole, 8 * k)
    state[...] = static[0]
    sweep(where, cur, state, static, advanced, planes, None, 8)


def load_corrections(ends, before, correction):
    for n in range(8):
        correction[n] = unpack_all(ends, 8 * n) - before[n]


def next_sweep_kernel(where, cur, static, before, begin, ends, planes, advanced, state, correction):
    load_corrections(ends, before, correction)
    state[...] = begin[...]
    sweep(where, cur, state, static, advanced, planes, correction, 8)


def last_sweep_kernel(where, cur, static, before, begin, rest_first, rest_other, ends,
                      start, state, correction, planes):
    load_corrections(ends, before, correction)
    state[...] = begin[...]

    def keep():
        (plane,) = cut_planes(state, where[1], (0,))
        planes[...] = plane

    mine = where[0]

    def turn(n, carry):
        source = jnp.zeros((16, 16, 128), F32)
        for p in range(PHASES):
            mean = 0.5 * (cur[n, p] + cur[n, PHASES + p])
            source = source + mean * static[2 + p]
        state[...] = coarse_solve(state[...], source, static[1] * 0.5 + 0.375) + correction[n]
        return carry

    lax.fori_loop(0, mine, turn, 0)
    keep()
    (own,) = widen(planes[...])
    first = (mine == 0).astype(F32)
    start[...] = own[None] + (first * rest_first[...] + (1.0 - first) * rest_other[...])


def fine_beside(v):
    rows, lanes = iota(v.shape, 0), iota(v.shape, 1)
    out = jnp.where(rows == 0, 0.0, pltpu.roll(v, 1, 0)) + jnp.where(rows == 63, 0.0, pltpu.roll(v, 63, 0))
    return out + jnp.where(lanes == 0, 0.0, pltpu.roll(v, 1, 1)) + jnp.where(lanes == 255, 0.0, pltpu.roll(v, 255, 1))


def inside(plane):
    return jnp.logical_and(plane >= 0, plane < 128).astype(F32)


def guarded(value, plane, first):
    return value if 0 <= plane < 4 else inside(first + plane) * value


def part(value):
    folded = jnp.sum(value.reshape(8, 8, 256), axis=0)
    return folded[:, :128] + folded[:, 128:]


def fine_kernel(initial, where, planes, rest, rest_up, rest_down, rest_far, sigma, sources, up, down,
                fields, packed, u, r, w, q, a):
    first = 4 * where[1]
    zero = (where[0] == 0).astype(F32)
    scale = (1.0 - zero, zero) if initial else (1.0, 1.0 - zero)
    above, below = (6, 9) if initial else (0, 0)
    lifted = widen(planes[...])
    pieces = [(rest_up, above + k) for k in range(4)] + [(rest, k) for k in range(4)]
    pieces = pieces + [(rest_down, below + k) for k in range(4)] + [(rest_far, 0)]
    for j, (piece, k) in enumerate(pieces):
        u[j] = scale[0] * lifted[j // 4] + scale[1] * piece[k]

    def weight(plane):
        return up[2 + plane] if plane < 0 else sigma[plane] if plane < 4 else down[plane - 4]

    def source(step, plane):
        before, after = ((5, 3), (6, 7))[step]
        return up[before + plane] if plane < 0 else sources[step, plane] if plane < 4 else down[after + plane - 4]

    def spread(field, low, plane):
        j = plane - low
        v = field[j]
        return field[j - 1] + field[j + 1] + fine_beside(v) - 6.0 * v

    for plane in range(-3, 8):
        r[plane + 3] = guarded(source(0, plane) + spread(u, -4, plane), plane, first)
    for plane in range(-2, 7):
        w[plane + 2] = guarded(weight(plane) * r[plane + 3] - spread(r, -3, plane), plane, first)
    for plane in range(-1, 6):
        q[0, plane + 1] = guarded(source(1, plane) + spread(u, -4, plane), plane, first)
        q[1, plane + 1] = guarded(spread(r, -3, plane), plane, first)
        q[2, plane + 1] = guarded(spread(w, -2, plane), plane, first)
    for plane in range(5):
        for k in range(3):
            image = weight(plane) * q[k, plane + 1] - spread(q.at[k], -1, plane)
            a[k, plane] = guarded(image, plane, first)
    sums = [jnp.zeros((8, 128), F32)] * 28
    for plane in range(4):
        terms = []
        rv, wv = r[plane + 3], w[plane + 2]
        heavy = weight(plane) + 6.0
        terms += [rv * rv, rv * wv, wv * wv]
        terms += [wv * (heavy * wv - fine_beside(wv) - 2.0 * w[plane + 3])]
        qs = [q[k, plane + 1] for k in range(3)]
        images = [a[k, plane] for k in range(3)]
        twice = []
        for k in range(3):
            value = heavy * images[k] - fine_beside(images[k]) - a[k, plane + 1]
            twice.append(value - a[k, plane - 1] if plane else value)
        for i, j in PAIRS:
            last = images[i] * twice[j]
            if plane == 3:
                last = last - a[i, 4] * images[j]
            terms += [qs[i] * qs[j], qs[i] * images[j], images[i] * images[j], last]
        sums = [s + part(v) for s, v in zip(sums, terms)]
    lane = iota((1, 128), 1)
    row = jnp.zeros((1, 128), F32)
    for k in range(28):
        row = jnp.where(lane == k, total(sums[k]), row)
    packed[...] = jnp.broadcast_to(row, packed.shape)
    fields[0] = u[4:8]
    fields[1] = r[3:7]
    fields[2] = w[2:6]
    for k in range(3):
        fields[3 + k] = q[k, 1:5]
        fields[6 + k] = a[k, 0:4]


PAIRS = ((0, 0), (0, 1), (0, 2), (1, 1), (1, 2), (2, 2))


def weights(m0, m1, m2, m3):
    step = m0 / m1
    new = step * step * m2 - m0
    product = m1 - 2.0 * step * m2 + step * step * m3
    ratio = new / m0
    second = new / (product - ratio * new / step)
    return step + second * (1.0 + ratio), -step * second


def finish_kernel(sums, fields, fine, rest, ends):
    row = jnp.sum(sums[...], axis=0, keepdims=True)
    lane = iota((1, 128), 1)
    m = [jnp.sum(jnp.where(lane == k, row, 0.0), axis=1, keepdims=True) for k in range(28)]
    a, b = weights(*m[:4])
    factor = {(0, 0): 1.0, (0, 1): 2.0 * a, (0, 2): 2.0 * b, (1, 1): a * a, (1, 2): 2.0 * (a * b), (2, 2): b * b}
    after = [sum(factor[pair] * m[4 + 4 * p + k] for p, pair in enumerate(PAIRS)) for k in range(4)]
    c, d = weights(*after)
    scales = (None, a, b, c, c * a, c * b, d, d * a, d * b)
    for i in range(4):
        value = fields[0, i]
        for k in range(1, 9):
            value = value + scales[k] * fields[k, i]
        fine[i] = value
    own = restrict_packed(jnp.sum(fine[...], axis=0))
    ends[...] = jnp.broadcast_to(own[None], ends.shape)
    left = iota((8, 128), 1) < 64
    plane = jnp.concatenate([jnp.where(left, own, 0.0), jnp.where(left, pltpu.roll(own, 64, 1), 0.0)], axis=0)
    (lifted,) = widen(plane)
    for i in range(4):
        rest[i] = fine[i] - lifted


def spread_kernel(ends, packed):
    packed[...] = jnp.broadcast_to(ends[...].reshape(1, 64, 128), packed.shape)


def shifted(x, axis, by, ring):
    n = lax.axis_size(axis)
    pairs = [(i, (i + by) % n) for i in range(n) if ring or 0 <= i + by < n]
    return lax.ppermute(x, axis, pairs)


def exchange(x, axis):
    return lax.all_to_all(x, axis, split_axis=0, concat_axis=0, tiled=True)


def everywhere(ends):
    (packed,) = call(spread_kernel, ((32, 64, 128),), (exchange(ends, "tm"),))
    return exchange(packed, "space")


def halos(x):
    return (
        shifted(x, "space", 1, False),
        shifted(x, "space", -1, False),
        shifted(x[:1], "space", -2, False),
    )


def body(labels, conductivity, coil_pattern, currents, initial_state):
    tm, place = lax.axis_index("tm"), lax.axis_index("space")
    where = jnp.stack([tm, place]).astype(jnp.int32)
    block, field = (4, 64, 256), (16, 16, 128)

    slices, across = lax.axis_size("tm"), lax.axis_size("space")
    pairs = [
        (b * across + slices * a + t, t * across + slices * a + b)
        for t in range(slices)
        for b in range(slices)
        for a in range(across // slices)
    ]
    theirs = lax.ppermute(jnp.pad(currents.reshape(1, 6), ((0, 0), (0, 122))), ("tm", "space"), pairs)

    sigma, sources, up, down, far, packed = call(
        setup_kernel,
        (block, (2, *block), (10, 64, 256), (13, 64, 256), (1, 64, 256), (32, 48, 128)),
        (conductivity, currents[0], theirs, labels, coil_pattern, initial_state),
        small=(0, 1),
    )
    whole = exchange(packed, "space")
    table = whole[:8, 40, :]
    up, down = shifted(up, "space", 1, False), shifted(down, "space", -1, False)
    far = shifted(far, "space", -2, False)
    static, planes, advanced, state = call(
        first_sweep_kernel,
        ((5, *field), (64, 128), (8, *field), field),
        (where, table, whole),
        small=(0, 1),
        flops=1 << 26,
    )

    def fine(initial, planes, rest, around_rest):
        fields, sums = call(
            functools.partial(fine_kernel, initial),
            ((9, *block), (32, 128)),
            (where, planes, rest, *around_rest, sigma, sources, up, down),
            small=(0,),
            scratch=((13, 64, 256), (11, 64, 256), (9, 64, 256), (3, 7, 64, 256), (3, 5, 64, 256)),
        )
        return call(
            finish_kernel,
            (block, block, (8, 8, 128)),
            (exchange(sums, "space"), fields),
        )

    _, rest, ends = fine(True, planes, initial_state, (up, down, far))
    rest_first = shifted(rest, "tm", 1, True)
    planes, advanced_next, state_next = call(
        next_sweep_kernel,
        ((64, 128), (8, *field), field),
        (where, table, static, advanced, state, everywhere(ends)),
        small=(0, 1),
        scratch=((8, *field),),
        flops=1 << 26,
    )
    fine_state, rest, ends = fine(False, planes, rest_first, halos(rest_first))
    rest_other = shifted(rest, "tm", 1, False)
    (start,) = call(
        last_sweep_kernel,
        (block,),
        (where, table, static, advanced_next, state_next, rest_first, rest_other, everywhere(ends)),
        small=(0, 1),
        scratch=(field, (8, *field), (16, 128)),
        flops=1 << 26,
    )
    return (start[None], fine_state[None])


def solution(mesh):
    in_specs = (
        P("space", None, None),
        P(),
        P(None, "space", None, None),
        P("tm", None, None),
        P("space", None, None),
    )
    out_specs = (P("tm", "space", None, None), P("tm", "space", None, None))
    return jax.shard_map(body, mesh=mesh, in_specs=in_specs, out_specs=out_specs, check_vma=False)
```

```python
import functools

import jax
import jax.numpy as jnp
from jax import lax
from jax.experimental import pallas as pl
from jax.experimental.pallas import tpu as pltpu
from jax.sharding import PartitionSpec as P

PHASES = 3
CG_COARSE = 4
F32 = jnp.float32
HIGHEST = lax.Precision.HIGHEST
VMEM = pltpu.MemorySpace.VMEM
SMEM = pltpu.MemorySpace.SMEM
INTERPRET = False
LIMIT = 12 << 20


def iota(shape, dim):
    return lax.broadcasted_iota(jnp.int32, shape, dim)


def dot(a, b):
    return lax.dot_general(a, b, (((1,), (0,)), ((), ())), precision=HIGHEST, preferred_element_type=F32)


def total(x):
    while x.ndim > 2:
        x = jnp.sum(x, axis=0)
    return jnp.sum(jnp.sum(x, axis=0, keepdims=True), axis=1, keepdims=True)


def restrict_packed(summed):
    columns = (iota((256, 128), 0) >> 2) == (iota((256, 128), 1) & 63)
    rows = (iota((16, 64), 1) >> 2) == iota((16, 64), 0)
    half = dot(summed, jnp.where(columns, 1.0 / 64.0, 0.0).astype(F32))
    both = dot(jnp.where(rows, 1.0, 0.0).astype(F32), half)
    return jnp.where(iota((8, 128), 1) < 64, both[:8], both[8:])


def widen(planes):
    columns = (iota((128, 256), 1) >> 2) == iota((128, 256), 0)
    rows = (iota((64, 16), 0) >> 2) == iota((64, 16), 1)
    wide = dot(planes, jnp.where(columns, 1.0, 0.0).astype(F32))
    lift = jnp.where(rows, 1.0, 0.0).astype(F32)
    return [dot(lift, wide[k : k + 16]) for k in range(0, planes.shape[0], 16)]


def unpack(low, high):
    axis = low.ndim - 1
    left = iota(low.shape, axis) < 64
    top = jnp.where(left, low, pltpu.roll(high, 64, axis))
    bottom = jnp.where(left, pltpu.roll(low, 64, axis), high)
    return jnp.concatenate([top, bottom], axis=axis - 1)


def coarse_beside(v):
    one = (1, 16, 128)
    lane, row = iota(one, 2), iota(one, 1)
    left = lane < 64
    first, last = pltpu.roll(v[:1], 64, 2), pltpu.roll(v[15:], 64, 2)
    after = jnp.concatenate([v[1:], jnp.where(left, first, 0.0)], axis=0)
    before = jnp.concatenate([jnp.where(left, 0.0, last), v[:15]], axis=0)
    out = after + before
    out = out + jnp.where(row == 0, 0.0, pltpu.roll(v, 1, 1)) + jnp.where(row == 15, 0.0, pltpu.roll(v, 15, 1))
    inner = lane & 63
    return out + jnp.where(inner == 0, 0.0, pltpu.roll(v, 1, 2)) + jnp.where(inner == 63, 0.0, pltpu.roll(v, 127, 2))


def coarse_solve(start, source, diagonal):
    def apply(v):
        return diagonal * v - 0.0625 * coarse_beside(v)

    x = start
    residual = source - 0.375 * start + 0.0625 * coarse_beside(start)
    image = apply(residual)
    norm, product = total(residual * residual), total(residual * image)
    step = norm / product
    direction, moved = residual, image
    for turn in range(CG_COARSE):
        inverse = 1.0 / norm
        scaled = inverse / step
        x = x + step[None] * direction
        if turn + 1 < CG_COARSE:
            residual = residual - step[None] * moved
            image = apply(residual)
            new, product = total(residual * residual), total(residual * image)
            ratio = new * inverse
            step = new / (product - new * (new * scaled))
            direction = residual + ratio[None] * direction
            moved = image + ratio[None] * moved
            norm = new
    return x


def cut_planes(state, place, offsets):
    out = []
    lane = iota((16, 128), 1)
    for offset in offsets:
        at = place + offset
        inside = jnp.logical_and(at >= 0, at < 32).astype(jnp.int32)
        at = jnp.clip(at, 0, 31)
        plane = state[at & 15]
        plane = jnp.where((at >> 4) * jnp.ones_like(lane) == 1, pltpu.roll(plane, 64, 1), plane)
        out.append(jnp.where(lane < 64 * inside, plane, 0.0))
    return out


def call(body, outs, args, small=(), far=(), scratch=(), flops=0, copies=0, limit=LIMIT):
    spaces = [SMEM if k in small else pltpu.MemorySpace.HBM if k in far else VMEM for k in range(len(args))]
    specs = [pl.BlockSpec(memory_space=space) for space in spaces]
    return pl.pallas_call(
        body,
        out_shape=tuple(jax.ShapeDtypeStruct(s, F32) for s in outs),
        in_specs=specs,
        out_specs=tuple(pl.BlockSpec(memory_space=VMEM) for _ in outs),
        scratch_shapes=(
            *(pltpu.VMEM(s, F32) if isinstance(s, tuple) else s for s in scratch),
            *(pltpu.SemaphoreType.DMA for _ in range(copies)),
        ),
        cost_estimate=pl.CostEstimate(flops=flops, bytes_accessed=1 << 20, transcendentals=0) if flops else None,
        compiler_params=pltpu.CompilerParams(vmem_limit_bytes=limit),
        interpret=INTERPRET,
    )(*args)


def setup_kernel(cond, cur, theirs, labels_far, coils_far, initial_far, sigma, sources, up, down, far, packed,
                 labels, coils, initial, labels_sem, coils_sem, initial_sem):
    copies = [
        pltpu.make_async_copy(labels_far, labels, labels_sem),
        pltpu.make_async_copy(coils_far, coils, coils_sem),
        pltpu.make_async_copy(initial_far, initial, initial_sem),
    ]
    for copy in copies:
        copy.start()
    for copy in copies:
        copy.wait()
    region = labels[...]
    cell = jnp.where(region == 0, cond[0], 0.0)
    for k in range(1, 4):
        cell = cell + jnp.where(region == k, cond[k], 0.0)
    sigma[...] = cell
    pattern = [coils[p] for p in range(PHASES)]
    for step in range(2):
        source = cur[step, 0] * pattern[0]
        for p in range(1, PHASES):
            source = source + cur[step, p] * pattern[p]
        sources[step] = source
    up[0:2] = sigma[2:4]
    up[2:5] = sources[0, 1:4]
    up[5:6] = sources[1, 3:4]
    down[0:3] = sigma[0:3]
    down[3:7] = sources[0]
    down[7:9] = sources[1, 0:2]
    up[6:10] = initial[...]
    down[9:13] = initial[...]
    far[...] = initial[0:1]
    fields = [initial[...], cell, *pattern]
    rows = [restrict_packed(jnp.sum(f, axis=0)) for f in fields]
    lane = iota((8, 128), 1)
    row = jnp.zeros((8, 128), F32)
    for k in range(6):
        row = jnp.where(lane == k, theirs[k // 3, k % 3], row)
    rows = jnp.concatenate([*rows, row], axis=0)
    packed[...] = jnp.broadcast_to(rows[None], packed.shape)


def unpack_all(whole, at):
    return unpack(whole[0:16, at : at + 8, :], whole[16:32, at : at + 8, :])


def slice_source(cur, static, n):
    source = jnp.zeros((16, 16, 128), F32)
    for p in range(PHASES):
        source = source + 0.5 * (cur[n, p] + cur[n, PHASES + p]) * static[2 + p]
    return source


def sweep(where, cur, state, static, advanced, planes, correction):
    mine, place = where[0], where[1]

    def turn(n, carry):
        @pl.when(n == mine)
        def _():
            for k, plane in enumerate(cut_planes(state, place, (-1, 0, 1, 2))):
                planes[16 * k : 16 * k + 16] = plane

        state[...] = coarse_solve(state[...], slice_source(cur, static, n), static[1] * 0.5 + 0.375)

        @pl.when(n == mine)
        def _():
            (plane,) = cut_planes(state, place, (0,))
            advanced[...] = plane[:8] + pltpu.roll(plane[8:], 64, 1)

        if correction is not None:
            state[...] = state[...] + correction[n]
        return carry

    lax.fori_loop(0, 8, turn, 0)


def first_sweep_kernel(where, cur, whole, static, planes, advanced, state):
    for k in range(5):
        static[k] = unpack_all(whole, 8 * k)
    state[...] = static[0]
    sweep(where, cur, state, static, advanced, planes, None)


def load_corrections(ends, correction):
    for n in range(8):
        correction[n] = unpack_all(ends, 8 * n)


def next_sweep_kernel(where, cur, static, begin, ends, planes, advanced, state, correction):
    load_corrections(ends, correction)
    state[...] = begin[...]
    sweep(where, cur, state, static, advanced, planes, correction)


def last_sweep_kernel(where, cur, static, begin, rest_first, rest_other, ends,
                      start, state, correction, planes):
    load_corrections(ends, correction)
    state[...] = begin[...]

    def keep():
        (plane,) = cut_planes(state, where[1], (0,))
        planes[...] = plane

    mine = where[0]

    def turn(n, carry):
        solved = coarse_solve(state[...], slice_source(cur, static, n), static[1] * 0.5 + 0.375)
        state[...] = solved + correction[n]
        return carry

    lax.fori_loop(0, mine, turn, 0)
    keep()
    (own,) = widen(planes[...])
    first = (mine == 0).astype(F32)
    start[...] = own[None] + (first * rest_first[...] + (1.0 - first) * rest_other[...])


def fine_beside(v):
    rows, lanes = iota(v.shape, 0), iota(v.shape, 1)
    out = jnp.where(rows == 0, 0.0, pltpu.roll(v, 1, 0)) + jnp.where(rows == 63, 0.0, pltpu.roll(v, 63, 0))
    return out + jnp.where(lanes == 0, 0.0, pltpu.roll(v, 1, 1)) + jnp.where(lanes == 255, 0.0, pltpu.roll(v, 255, 1))


def inside(plane):
    return jnp.logical_and(plane >= 0, plane < 128).astype(F32)


def guarded(value, plane, first):
    return value if 0 <= plane < 4 else inside(first + plane) * value


def part(value):
    folded = jnp.sum(value.reshape(8, 8, 256), axis=0)
    return folded[:, :128] + folded[:, 128:]


def fine_kernel(initial, where, planes, rest, rest_up, rest_down, rest_far, sigma, sources, up, down,
                fields, packed, u, r, w, q, a):
    first = 4 * where[1]
    zero = (where[0] == 0).astype(F32)
    scale = (1.0 - zero, zero) if initial else (1.0, 1.0 - zero)
    above, below = (6, 9) if initial else (0, 0)
    lifted = widen(planes[...])
    pieces = [(rest_up, above + k) for k in range(4)] + [(rest, k) for k in range(4)]
    pieces = pieces + [(rest_down, below + k) for k in range(4)] + [(rest_far, 0)]
    for j, (piece, k) in enumerate(pieces):
        u[j] = scale[0] * lifted[j // 4] + scale[1] * piece[k]

    def weight(plane):
        return up[2 + plane] if plane < 0 else sigma[plane] if plane < 4 else down[plane - 4]

    def source(step, plane):
        before, after = ((5, 3), (6, 7))[step]
        return up[before + plane] if plane < 0 else sources[step, plane] if plane < 4 else down[after + plane - 4]

    def beside(field, low, plane):
        j = plane - low
        return field[j - 1] + field[j + 1] + fine_beside(field[j])

    def spread(field, low, plane):
        return beside(field, low, plane) - 6.0 * field[plane - low]

    for plane in range(-3, 8):
        r[plane + 3] = guarded(source(0, plane) + spread(u, -4, plane), plane, first)
    for plane in range(-2, 7):
        w[plane + 2] = guarded(weight(plane) * r[plane + 3] - beside(r, -3, plane), plane, first)
    for plane in range(-1, 6):
        q[0, plane + 1] = guarded(source(1, plane) + spread(u, -4, plane), plane, first)
        q[1, plane + 1] = guarded(spread(r, -3, plane), plane, first)
        q[2, plane + 1] = guarded(spread(w, -2, plane), plane, first)
    for plane in range(5):
        for k in range(3):
            image = weight(plane) * q[k, plane + 1] - beside(q.at[k], -1, plane)
            a[k, plane] = guarded(image, plane, first)
    sums = [jnp.zeros((8, 128), F32)] * 28
    for plane in range(4):
        terms = []
        rv, wv = r[plane + 3], w[plane + 2]
        heavy = weight(plane) + 6.0
        terms += [rv * rv, rv * wv, wv * wv]
        terms += [wv * (heavy * wv - fine_beside(wv) - 2.0 * w[plane + 3])]
        qs = [q[k, plane + 1] for k in range(3)]
        images = [a[k, plane] for k in range(3)]
        twice = []
        for k in range(3):
            value = heavy * images[k] - fine_beside(images[k]) - a[k, plane + 1]
            twice.append(value - a[k, plane - 1] if plane else value)
        for i, j in PAIRS:
            last = images[i] * twice[j]
            if plane == 3:
                last = last - a[i, 4] * images[j]
            terms += [qs[i] * qs[j], qs[i] * images[j], images[i] * images[j], last]
        sums = [s + part(v) for s, v in zip(sums, terms)]
    lane = iota((1, 128), 1)
    row = jnp.zeros((1, 128), F32)
    for k in range(28):
        row = jnp.where(lane == k, total(sums[k]), row)
    packed[...] = jnp.broadcast_to(row, packed.shape)
    fields[0] = u[4:8]
    fields[1] = r[3:7]
    fields[2] = w[2:6]
    for k in range(3):
        fields[3 + k] = q[k, 1:5]
        fields[6 + k] = a[k, 0:4]


PAIRS = ((0, 0), (0, 1), (0, 2), (1, 1), (1, 2), (2, 2))


def weights(norm, cross, square, product):
    first = cross + 6.0 * norm
    step = norm / first
    keep = 1.0 - 6.0 * step
    new = keep * keep * norm - 2.0 * keep * step * cross + step * step * square
    second = keep * keep * first - 2.0 * keep * step * (square + 6.0 * cross) + step * step * product
    ratio = new / norm
    second = new / (second - ratio * new / step)
    return step + second * (keep + ratio), -second * step


def finish_kernel(sums, fields, advanced, fine, rest, ends):
    row = jnp.sum(sums[...], axis=0, keepdims=True)
    lane = iota((1, 128), 1)
    m = [jnp.sum(jnp.where(lane == k, row, 0.0), axis=1, keepdims=True) for k in range(28)]
    a, b = weights(*m[:4])
    factor = {(0, 0): 1.0, (0, 1): 2.0 * a, (0, 2): 2.0 * b, (1, 1): a * a, (1, 2): 2.0 * (a * b), (2, 2): b * b}
    after = [sum(factor[pair] * m[4 + 4 * p + k] for p, pair in enumerate(PAIRS)) for k in range(4)]
    c, d = weights(*after)
    scales = (None, a, b, c, c * a, c * b, d, d * a, d * b)
    for i in range(4):
        value = fields[0, i]
        for k in range(1, 9):
            value = value + scales[k] * fields[k, i]
        fine[i] = value
    own = restrict_packed(jnp.sum(fine[...], axis=0))
    ends[...] = jnp.broadcast_to((own - advanced[...])[None], ends.shape)
    left = iota((8, 128), 1) < 64
    plane = jnp.concatenate([jnp.where(left, own, 0.0), jnp.where(left, pltpu.roll(own, 64, 1), 0.0)], axis=0)
    (lifted,) = widen(plane)
    for i in range(4):
        rest[i] = fine[i] - lifted


def spread_kernel(ends, rest, packed):
    packed[...] = jnp.broadcast_to(ends[...].reshape(1, 64, 128), packed.shape)


def shifted(x, axis, by, ring):
    n = lax.axis_size(axis)
    pairs = [(i, (i + by) % n) for i in range(n) if ring or 0 <= i + by < n]
    return lax.ppermute(x, axis, pairs)


def exchange(x, axis):
    return lax.all_to_all(x, axis, split_axis=0, concat_axis=0, tiled=True)


def everywhere(ends, rest):
    (packed,) = call(spread_kernel, ((32, 64, 128),), (exchange(ends, "tm"), rest), far=(1,))
    return exchange(packed, "space")


def halos(x):
    return (
        shifted(x, "space", 1, False),
        shifted(x, "space", -1, False),
        shifted(x[:1], "space", -2, False),
    )


def body(labels, conductivity, coil_pattern, currents, initial_state):
    tm, place = lax.axis_index("tm"), lax.axis_index("space")
    where = jnp.stack([tm, place]).astype(jnp.int32)
    block, field = (4, 64, 256), (16, 16, 128)

    slices, across = lax.axis_size("tm"), lax.axis_size("space")
    pairs = [
        (b * across + slices * a + t, t * across + slices * a + b)
        for t in range(slices)
        for b in range(slices)
        for a in range(across // slices)
    ]
    theirs = lax.ppermute(currents[0], ("tm", "space"), pairs)

    sigma, sources, up, down, far, packed = call(
        setup_kernel,
        (block, (2, *block), (10, 64, 256), (13, 64, 256), (1, 64, 256), (32, 48, 128)),
        (conductivity, currents[0], theirs, labels, coil_pattern, initial_state),
        small=(0, 1, 2),
        far=(3, 4, 5),
        scratch=(pltpu.VMEM(block, jnp.int32), (3, *block), block),
        copies=3,
        limit=60 << 20,
    )
    whole = exchange(packed, "space")
    table = whole[:8, 40, :]
    up, down = shifted(up, "space", 1, False), shifted(down, "space", -1, False)
    far = shifted(far, "space", -2, False)
    static, planes, advanced, state = call(
        first_sweep_kernel,
        ((5, *field), (64, 128), (8, 128), field),
        (where, table, whole),
        small=(0, 1),
        flops=1 << 26,
    )

    def fine(initial, planes, advanced, rest, around_rest):
        fields, sums = call(
            functools.partial(fine_kernel, initial),
            ((9, *block), (32, 128)),
            (where, planes, rest, *around_rest, sigma, sources, up, down),
            small=(0,),
            scratch=((13, 64, 256), (11, 64, 256), (9, 64, 256), (3, 7, 64, 256), (3, 5, 64, 256)),
        )
        return call(
            finish_kernel,
            (block, block, (8, 8, 128)),
            (exchange(sums, "space"), fields, advanced),
        )

    _, rest, ends = fine(True, planes, advanced, initial_state, (up, down, far))
    rest_first = shifted(rest, "tm", 1, True)
    planes, advanced_next, state_next = call(
        next_sweep_kernel,
        ((64, 128), (8, 128), field),
        (where, table, static, state, everywhere(ends, rest_first)),
        small=(0, 1),
        scratch=((8, *field),),
        flops=1 << 26,
    )
    fine_state, rest, ends = fine(False, planes, advanced_next, rest_first, halos(rest_first))
    rest_other = shifted(rest, "tm", 1, False)
    (start,) = call(
        last_sweep_kernel,
        (block,),
        (where, table, static, state_next, rest_first, rest_other, everywhere(ends, rest_other)),
        small=(0, 1),
        scratch=(field, (8, *field), (16, 128)),
        flops=1 << 26,
    )
    return (start[None], fine_state[None])


def solution(mesh):
    in_specs = (
        P("space", None, None),
        P(),
        P(None, "space", None, None),
        P("tm", None, None),
        P("space", None, None),
    )
    out_specs = (P("tm", "space", None, None), P("tm", "space", None, None))
    return jax.shard_map(body, mesh=mesh, in_specs=in_specs, out_specs=out_specs, check_vma=False)
```

```python
import functools

import jax
import jax.numpy as jnp
from jax import lax
from jax.experimental import pallas as pl
from jax.experimental.pallas import tpu as pltpu
from jax.sharding import PartitionSpec as P

PHASES = 3
CG_COARSE = 4
F32 = jnp.float32
HIGHEST = lax.Precision.HIGHEST
VMEM = pltpu.MemorySpace.VMEM
SMEM = pltpu.MemorySpace.SMEM
INTERPRET = False
LIMIT = 12 << 20


def iota(shape, dim):
    return lax.broadcasted_iota(jnp.int32, shape, dim)


def dot(a, b):
    return lax.dot_general(a, b, (((1,), (0,)), ((), ())), precision=HIGHEST, preferred_element_type=F32)


def total(x):
    while x.ndim > 2:
        x = jnp.sum(x, axis=0)
    return jnp.sum(jnp.sum(x, axis=0, keepdims=True), axis=1, keepdims=True)


def restrict_packed(summed):
    columns = (iota((256, 128), 0) >> 2) == (iota((256, 128), 1) & 63)
    rows = (iota((16, 64), 1) >> 2) == iota((16, 64), 0)
    half = dot(summed, jnp.where(columns, 1.0 / 64.0, 0.0).astype(F32))
    both = dot(jnp.where(rows, 1.0, 0.0).astype(F32), half)
    return jnp.where(iota((8, 128), 1) < 64, both[:8], both[8:])


def widen(planes):
    columns = (iota((128, 256), 1) >> 2) == iota((128, 256), 0)
    rows = (iota((64, 16), 0) >> 2) == iota((64, 16), 1)
    wide = dot(planes, jnp.where(columns, 1.0, 0.0).astype(F32))
    lift = jnp.where(rows, 1.0, 0.0).astype(F32)
    return [dot(lift, wide[k : k + 16]) for k in range(0, planes.shape[0], 16)]


def unpack(low, high):
    axis = low.ndim - 1
    left = iota(low.shape, axis) < 64
    top = jnp.where(left, low, pltpu.roll(high, 64, axis))
    bottom = jnp.where(left, pltpu.roll(low, 64, axis), high)
    return jnp.concatenate([top, bottom], axis=axis - 1)


def coarse_beside(v):
    one = (1, 16, 128)
    lane, row = iota(one, 2), iota(one, 1)
    left = lane < 64
    first, last = pltpu.roll(v[:1], 64, 2), pltpu.roll(v[15:], 64, 2)
    after = jnp.concatenate([v[1:], jnp.where(left, first, 0.0)], axis=0)
    before = jnp.concatenate([jnp.where(left, 0.0, last), v[:15]], axis=0)
    out = after + before
    out = out + jnp.where(row == 0, 0.0, pltpu.roll(v, 1, 1)) + jnp.where(row == 15, 0.0, pltpu.roll(v, 15, 1))
    inner = lane & 63
    return out + jnp.where(inner == 0, 0.0, pltpu.roll(v, 1, 2)) + jnp.where(inner == 63, 0.0, pltpu.roll(v, 127, 2))


def coarse_solve(start, source, diagonal):
    def apply(v):
        return diagonal * v - 0.0625 * coarse_beside(v)

    x = start
    residual = source - 0.375 * start + 0.0625 * coarse_beside(start)
    image = apply(residual)
    norm, product = total(residual * residual), total(residual * image)
    step = norm / product
    direction, moved = residual, image
    for turn in range(CG_COARSE):
        inverse = 1.0 / norm
        scaled = inverse / step
        x = x + step[None] * direction
        if turn + 1 < CG_COARSE:
            residual = residual - step[None] * moved
            image = apply(residual)
            new, product = total(residual * residual), total(residual * image)
            ratio = new * inverse
            step = new / (product - new * (new * scaled))
            direction = residual + ratio[None] * direction
            moved = image + ratio[None] * moved
            norm = new
    return x


def cut_planes(state, place, offsets):
    out = []
    lane = iota((16, 128), 1)
    for offset in offsets:
        at = place + offset
        inside = jnp.logical_and(at >= 0, at < 32).astype(jnp.int32)
        at = jnp.clip(at, 0, 31)
        plane = state[at & 15]
        plane = jnp.where((at >> 4) * jnp.ones_like(lane) == 1, pltpu.roll(plane, 64, 1), plane)
        out.append(jnp.where(lane < 64 * inside, plane, 0.0))
    return out


def call(body, outs, args, small=(), far=(), scratch=(), flops=0, copies=0, limit=LIMIT):
    spaces = [SMEM if k in small else pltpu.MemorySpace.HBM if k in far else VMEM for k in range(len(args))]
    specs = [pl.BlockSpec(memory_space=space) for space in spaces]
    return pl.pallas_call(
        body,
        out_shape=tuple(jax.ShapeDtypeStruct(s, F32) for s in outs),
        in_specs=specs,
        out_specs=tuple(pl.BlockSpec(memory_space=VMEM) for _ in outs),
        scratch_shapes=(
            *(pltpu.VMEM(s, F32) if isinstance(s, tuple) else s for s in scratch),
            *(pltpu.SemaphoreType.DMA for _ in range(copies)),
        ),
        cost_estimate=pl.CostEstimate(flops=flops, bytes_accessed=1 << 20, transcendentals=0) if flops else None,
        compiler_params=pltpu.CompilerParams(vmem_limit_bytes=limit),
        interpret=INTERPRET,
    )(*args)


def setup_kernel(cond, cur, theirs, labels_far, coils_far, initial_far, own, up, down, far, packed,
                 labels, coils, initial, labels_sem, coils_sem, initial_sem):
    copies = [
        pltpu.make_async_copy(labels_far, labels, labels_sem),
        pltpu.make_async_copy(coils_far, coils, coils_sem),
        pltpu.make_async_copy(initial_far, initial, initial_sem),
    ]
    for copy in copies:
        copy.start()
    for copy in copies:
        copy.wait()
    region = labels[...]
    cell = jnp.where(region == 0, cond[0], 0.0)
    for k in range(1, 4):
        cell = cell + jnp.where(region == k, cond[k], 0.0)
    own[0] = cell
    own[3] = initial[...]
    pattern = [coils[p] for p in range(PHASES)]
    for step in range(2):
        source = cur[step, 0] * pattern[0]
        for p in range(1, PHASES):
            source = source + cur[step, p] * pattern[p]
        own[1 + step] = source
    up[0:2] = own[0, 2:4]
    up[2:5] = own[1, 1:4]
    up[5:6] = own[2, 3:4]
    down[0:3] = own[0, 0:3]
    down[3:7] = own[1]
    down[7:9] = own[2, 0:2]
    up[6:10] = initial[...]
    down[9:13] = initial[...]
    far[...] = initial[0:1]
    fields = [initial[...], cell, *pattern]
    rows = [restrict_packed(jnp.sum(f, axis=0)) for f in fields]
    lane = iota((8, 128), 1)
    row = jnp.zeros((8, 128), F32)
    for k in range(6):
        row = jnp.where(lane == k, theirs[k // 3, k % 3], row)
    rows = jnp.concatenate([*rows, row], axis=0)
    packed[...] = jnp.broadcast_to(rows[None], packed.shape)


def unpack_all(whole, at):
    return unpack(whole[0:16, at : at + 8, :], whole[16:32, at : at + 8, :])


def slice_source(cur, static, n):
    source = jnp.zeros((16, 16, 128), F32)
    for p in range(PHASES):
        source = source + 0.5 * (cur[n, p] + cur[n, PHASES + p]) * static[2 + p]
    return source


def sweep(where, cur, state, static, advanced, planes, correction):
    mine, place = where[0], where[1]

    def turn(n, carry):
        @pl.when(n == mine)
        def _():
            for k, plane in enumerate(cut_planes(state, place, (-1, 0, 1, 2))):
                planes[16 * k : 16 * k + 16] = plane

        state[...] = coarse_solve(state[...], slice_source(cur, static, n), static[1] * 0.5 + 0.375)

        @pl.when(n == mine)
        def _():
            (plane,) = cut_planes(state, place, (0,))
            advanced[...] = plane[:8] + pltpu.roll(plane[8:], 64, 1)

        if correction is not None:
            state[...] = state[...] + correction[n]
        return carry

    lax.fori_loop(0, 8, turn, 0)


def first_sweep_kernel(where, cur, whole, static, planes, advanced, state):
    for k in range(5):
        static[k] = unpack_all(whole, 8 * k)
    state[...] = static[0]
    sweep(where, cur, state, static, advanced, planes, None)


def load_corrections(where, ours, theirs, correction):
    odd = where[1] & 1
    for k in range(4):
        correction[4 * odd + k] = unpack_all(ours, 8 * k)
        correction[4 * (1 - odd) + k] = unpack_all(theirs, 8 * k)


def next_sweep_kernel(where, cur, static, begin, ours, theirs, planes, advanced, state, correction):
    load_corrections(where, ours, theirs, correction)
    state[...] = begin[...]
    sweep(where, cur, state, static, advanced, planes, correction)


def last_sweep_kernel(where, cur, static, begin, rest_first, rest_other, ours, theirs,
                      start, state, correction, planes):
    load_corrections(where, ours, theirs, correction)
    state[...] = begin[...]

    def keep():
        (plane,) = cut_planes(state, where[1], (0,))
        planes[...] = plane

    mine = where[0]

    def turn(n, carry):
        solved = coarse_solve(state[...], slice_source(cur, static, n), static[1] * 0.5 + 0.375)
        state[...] = solved + correction[n]
        return carry

    lax.fori_loop(0, mine, turn, 0)
    keep()
    (own,) = widen(planes[...])
    first = (mine == 0).astype(F32)
    start[...] = own[None] + (first * rest_first[...] + (1.0 - first) * rest_other[...])


def fine_beside(v):
    rows, lanes = iota(v.shape, 0), iota(v.shape, 1)
    out = jnp.where(rows == 0, 0.0, pltpu.roll(v, 1, 0)) + jnp.where(rows == 63, 0.0, pltpu.roll(v, 63, 0))
    return out + jnp.where(lanes == 0, 0.0, pltpu.roll(v, 1, 1)) + jnp.where(lanes == 255, 0.0, pltpu.roll(v, 255, 1))


def inside(plane):
    return jnp.logical_and(plane >= 0, plane < 128).astype(F32)


def guarded(value, plane, first):
    return value if 0 <= plane < 4 else inside(first + plane) * value


def part(value):
    folded = jnp.sum(value.reshape(8, 8, 256), axis=0)
    return folded[:, :128] + folded[:, 128:]


def fine_kernel(initial, where, planes, own, up, down, *refs):
    if initial:
        (rest_far,), refs = refs[:1], refs[1:]
        rest, rest_up, rest_down = own.at[3], up, down
    else:
        (rest, rest_up, rest_down, rest_far), refs = refs[:4], refs[4:]
    fields, packed, u, r, w, q, a = refs
    first = 4 * where[1]
    zero = (where[0] == 0).astype(F32)
    scale = (1.0 - zero, zero) if initial else (1.0, 1.0 - zero)
    above, below = (6, 9) if initial else (0, 0)
    lifted = widen(planes[...])
    pieces = [(rest_up, above + k) for k in range(4)] + [(rest, k) for k in range(4)]
    pieces = pieces + [(rest_down, below + k) for k in range(4)] + [(rest_far, 0)]
    for j, (piece, k) in enumerate(pieces):
        u[j] = scale[0] * lifted[j // 4] + scale[1] * piece[k]

    def weight(plane):
        return up[2 + plane] if plane < 0 else own[0, plane] if plane < 4 else down[plane - 4]

    def source(step, plane):
        before, after = ((5, 3), (6, 7))[step]
        return up[before + plane] if plane < 0 else own[1 + step, plane] if plane < 4 else down[after + plane - 4]

    def beside(field, low, plane):
        j = plane - low
        return field[j - 1] + field[j + 1] + fine_beside(field[j])

    def spread(field, low, plane):
        return beside(field, low, plane) - 6.0 * field[plane - low]

    for plane in range(-3, 8):
        r[plane + 3] = guarded(source(0, plane) + spread(u, -4, plane), plane, first)
    for plane in range(-2, 7):
        w[plane + 2] = guarded(weight(plane) * r[plane + 3] - beside(r, -3, plane), plane, first)
    for plane in range(-1, 6):
        q[0, plane + 1] = guarded(source(1, plane) + spread(u, -4, plane), plane, first)
        q[1, plane + 1] = guarded(spread(r, -3, plane), plane, first)
        q[2, plane + 1] = guarded(spread(w, -2, plane), plane, first)
    for plane in range(5):
        for k in range(3):
            image = weight(plane) * q[k, plane + 1] - beside(q.at[k], -1, plane)
            a[k, plane] = guarded(image, plane, first)
    sums = [jnp.zeros((8, 128), F32)] * 28
    for plane in range(4):
        terms = []
        rv, wv = r[plane + 3], w[plane + 2]
        heavy = weight(plane) + 6.0
        terms += [rv * rv, rv * wv, wv * wv]
        terms += [wv * (heavy * wv - fine_beside(wv) - 2.0 * w[plane + 3])]
        qs = [q[k, plane + 1] for k in range(3)]
        images = [a[k, plane] for k in range(3)]
        twice = []
        for k in range(3):
            value = heavy * images[k] - fine_beside(images[k]) - a[k, plane + 1]
            twice.append(value - a[k, plane - 1] if plane else value)
        for i, j in PAIRS:
            last = images[i] * twice[j]
            if plane == 3:
                last = last - a[i, 4] * images[j]
            terms += [qs[i] * qs[j], qs[i] * images[j], images[i] * images[j], last]
        sums = [s + part(v) for s, v in zip(sums, terms)]
    lane = iota((1, 128), 1)
    row = jnp.zeros((1, 128), F32)
    for k in range(28):
        row = jnp.where(lane == k, total(sums[k]), row)
    packed[...] = jnp.broadcast_to(row, packed.shape)
    fields[0] = u[4:8]
    fields[1] = r[3:7]
    fields[2] = w[2:6]
    for k in range(3):
        fields[3 + k] = q[k, 1:5]
        fields[6 + k] = a[k, 0:4]


PAIRS = ((0, 0), (0, 1), (0, 2), (1, 1), (1, 2), (2, 2))


def weights(norm, cross, square, product):
    first = cross + 6.0 * norm
    step = norm / first
    keep = 1.0 - 6.0 * step
    new = keep * keep * norm - 2.0 * keep * step * cross + step * step * square
    second = keep * keep * first - 2.0 * keep * step * (square + 6.0 * cross) + step * step * product
    ratio = new / norm
    second = new / (second - ratio * new / step)
    return step + second * (keep + ratio), -second * step


def finish_kernel(sums, fields, advanced, fine, rest, ends):
    row = jnp.sum(sums[...], axis=0, keepdims=True)
    lane = iota((1, 128), 1)
    m = [jnp.sum(jnp.where(lane == k, row, 0.0), axis=1, keepdims=True) for k in range(28)]
    a, b = weights(*m[:4])
    factor = {(0, 0): 1.0, (0, 1): 2.0 * a, (0, 2): 2.0 * b, (1, 1): a * a, (1, 2): 2.0 * (a * b), (2, 2): b * b}
    after = [sum(factor[pair] * m[4 + 4 * p + k] for p, pair in enumerate(PAIRS)) for k in range(4)]
    c, d = weights(*after)
    scales = (None, a, b, c, c * a, c * b, d, d * a, d * b)
    for i in range(4):
        value = fields[0, i]
        for k in range(1, 9):
            value = value + scales[k] * fields[k, i]
        fine[i] = value
    own = restrict_packed(jnp.sum(fine[...], axis=0))
    ends[...] = jnp.broadcast_to((own - advanced[...])[None], ends.shape)
    left = iota((8, 128), 1) < 64
    plane = jnp.concatenate([jnp.where(left, own, 0.0), jnp.where(left, pltpu.roll(own, 64, 1), 0.0)], axis=0)
    (lifted,) = widen(plane)
    for i in range(4):
        rest[i] = fine[i] - lifted


def spread_kernel(ends, rest, packed):
    for half in range(2):
        rows = ends[4 * half : 4 * half + 4].reshape(1, 32, 128)
        for k in range(half, packed.shape[0], 2):
            packed[k : k + 1] = rows


def shifted(x, axis, by, ring):
    n = lax.axis_size(axis)
    pairs = [(i, (i + by) % n) for i in range(n) if ring or 0 <= i + by < n]
    return lax.ppermute(x, axis, pairs)


def exchange(x, axis):
    return lax.all_to_all(x, axis, split_axis=0, concat_axis=0, tiled=True)


def everywhere(ends, rest):
    (packed,) = call(spread_kernel, ((32, 32, 128),), (exchange(ends, "tm"), rest), far=(1,))
    half = exchange(packed, "space")
    places = lax.axis_size("space")
    return half, lax.ppermute(half, "space", [(i, i ^ 1) for i in range(places)])


def halos(x):
    return (
        shifted(x, "space", 1, False),
        shifted(x, "space", -1, False),
        shifted(x[:1], "space", -2, False),
    )


def body(labels, conductivity, coil_pattern, currents, initial_state):
    tm, place = lax.axis_index("tm"), lax.axis_index("space")
    where = jnp.stack([tm, place]).astype(jnp.int32)
    block, field = (4, 64, 256), (16, 16, 128)

    slices, across = lax.axis_size("tm"), lax.axis_size("space")
    pairs = [
        (b * across + slices * a + t, t * across + slices * a + b)
        for t in range(slices)
        for b in range(slices)
        for a in range(across // slices)
    ]
    theirs = lax.ppermute(currents[0], ("tm", "space"), pairs)

    own, up, down, far, packed = call(
        setup_kernel,
        ((4, *block), (10, 64, 256), (13, 64, 256), (1, 64, 256), (32, 48, 128)),
        (conductivity, currents[0], theirs, labels, coil_pattern, initial_state),
        small=(0, 1, 2),
        far=(3, 4, 5),
        scratch=(pltpu.VMEM(block, jnp.int32), (3, *block), block),
        copies=3,
        limit=60 << 20,
    )
    whole = exchange(packed, "space")
    table = whole[:8, 40, :]
    up, down, far, whole = lax.optimization_barrier((up, down, far, whole))
    up, down = shifted(up, "space", 1, False), shifted(down, "space", -1, False)
    far = shifted(far, "space", -2, False)
    static, planes, advanced, state = call(
        first_sweep_kernel,
        ((5, *field), (64, 128), (8, 128), field),
        (where, table, whole),
        small=(0, 1),
        flops=1 << 26,
    )

    def fine(initial, planes, advanced, rest):
        fields, sums = call(
            functools.partial(fine_kernel, initial),
            ((9, *block), (32, 128)),
            (where, planes, own, up, down, *rest),
            small=(0,),
            scratch=((13, 64, 256), (11, 64, 256), (9, 64, 256), (3, 7, 64, 256), (3, 5, 64, 256)),
        )
        return call(
            finish_kernel,
            (block, block, (8, 8, 128)),
            (exchange(sums, "space"), fields, advanced),
        )

    _, rest, ends = fine(True, planes, advanced, (far,))
    rest_first = shifted(rest, "tm", 1, True)
    planes, advanced_next, state_next = call(
        next_sweep_kernel,
        ((64, 128), (8, 128), field),
        (where, table, static, state, *everywhere(ends, rest_first)),
        small=(0, 1),
        scratch=((8, *field),),
        flops=1 << 26,
    )
    fine_state, rest, ends = fine(
        False, planes, advanced_next, (rest_first, *halos(rest_first))
    )
    rest_other = shifted(rest, "tm", 1, False)
    (start,) = call(
        last_sweep_kernel,
        (block,),
        (where, table, static, state_next, rest_first, rest_other, *everywhere(ends, rest_other)),
        small=(0, 1),
        scratch=(field, (8, *field), (16, 128)),
        flops=1 << 26,
    )
    return (start[None], fine_state[None])


def solution(mesh):
    in_specs = (
        P("space", None, None),
        P(),
        P(None, "space", None, None),
        P("tm", None, None),
        P("space", None, None),
    )
    out_specs = (P("tm", "space", None, None), P("tm", "space", None, None))
    return jax.shard_map(body, mesh=mesh, in_specs=in_specs, out_specs=out_specs, check_vma=False)
```

```python
import functools

import jax
import jax.numpy as jnp
from jax import lax
from jax.experimental import pallas as pl
from jax.experimental.pallas import tpu as pltpu
from jax.sharding import PartitionSpec as P

PHASES = 3
F32 = jnp.float32
HIGHEST = lax.Precision.HIGHEST
VMEM = pltpu.MemorySpace.VMEM
SMEM = pltpu.MemorySpace.SMEM
INTERPRET = False
LIMIT = 12 << 20


def iota(shape, dim):
    return lax.broadcasted_iota(jnp.int32, shape, dim)


def dot(a, b):
    return lax.dot_general(a, b, (((1,), (0,)), ((), ())), precision=HIGHEST, preferred_element_type=F32)


def total(x):
    while x.ndim > 2:
        x = jnp.sum(x, axis=0)
    return jnp.sum(jnp.sum(x, axis=0, keepdims=True), axis=1, keepdims=True)


def restrict_packed(summed):
    columns = (iota((256, 128), 0) >> 2) == (iota((256, 128), 1) & 63)
    rows = (iota((16, 64), 1) >> 2) == iota((16, 64), 0)
    half = dot(summed, jnp.where(columns, 1.0 / 64.0, 0.0).astype(F32))
    both = dot(jnp.where(rows, 1.0, 0.0).astype(F32), half)
    return jnp.where(iota((8, 128), 1) < 64, both[:8], both[8:])


def widen(planes):
    columns = (iota((128, 256), 1) >> 2) == iota((128, 256), 0)
    rows = (iota((64, 16), 0) >> 2) == iota((64, 16), 1)
    wide = dot(planes, jnp.where(columns, 1.0, 0.0).astype(F32))
    lift = jnp.where(rows, 1.0, 0.0).astype(F32)
    return [dot(lift, wide[k : k + 16]) for k in range(0, planes.shape[0], 16)]


def unpack(low, high):
    axis = low.ndim - 1
    left = iota(low.shape, axis) < 64
    top = jnp.where(left, low, pltpu.roll(high, 64, axis))
    bottom = jnp.where(left, pltpu.roll(low, 64, axis), high)
    return jnp.concatenate([top, bottom], axis=axis - 1)


def coarse_beside(v):
    one = (1, 16, 128)
    lane, row = iota(one, 2), iota(one, 1)
    left = lane < 64
    first, last = pltpu.roll(v[:1], 64, 2), pltpu.roll(v[15:], 64, 2)
    after = jnp.concatenate([v[1:], jnp.where(left, first, 0.0)], axis=0)
    before = jnp.concatenate([jnp.where(left, 0.0, last), v[:15]], axis=0)
    out = after + before
    out = out + jnp.where(row == 0, 0.0, pltpu.roll(v, 1, 1)) + jnp.where(row == 15, 0.0, pltpu.roll(v, 15, 1))
    inner = lane & 63
    return out + jnp.where(inner == 0, 0.0, pltpu.roll(v, 1, 2)) + jnp.where(inner == 63, 0.0, pltpu.roll(v, 127, 2))


def coarse_solve(start, source, scaled):
    def apply(v):
        return scaled * v - 0.1 * coarse_beside(v)

    v0 = source - 0.375 * start + 0.0625 * coarse_beside(start)
    v1 = apply(v0)
    v2 = 2.0 * apply(v1) - v0
    v3 = 2.0 * apply(v2) - v1
    p = [total(a * b) for a, b in ((v0, v0), (v0, v1), (v1, v1), (v1, v2), (v2, v2), (v2, v3), (v3, v3))]
    m = p[:2] + [2.0 * p[k] - p[k & 1] for k in range(2, 7)]
    last = total(v3 * apply(v3))

    def entry(i, j):
        both = 0.5 * (m[i + j] + m[abs(i - j)])
        if i == j == 3:
            return both + last
        return both + 0.25 * (m[i + j + 1] + m[abs(i + j - 1)] + m[abs(i - j + 1)] + m[abs(i - j - 1)])

    right = m[:4]
    rows = {(i, j): entry(i, j) for i in range(4) for j in range(i + 1)}
    whole = [rows[k, k] for k in range(4)]
    inverse = []
    for k in range(4):
        inverse.append(jnp.where(rows[k, k] > 1e-6 * whole[k], 1.0 / rows[k, k], 0.0))
        for i in range(k + 1, 4):
            factor = rows[i, k] * inverse[k]
            right[i] = right[i] - factor * right[k]
            for j in range(k + 1, i + 1):
                rows[i, j] = rows[i, j] - factor * rows[j, k]
    y = [None] * 4
    for k in (3, 2, 1, 0):
        y[k] = (right[k] - sum(rows[i, k] * y[i] for i in range(k + 1, 4))) * inverse[k]
    y = [1.6 * value[None] for value in y]
    return start + (y[0] * v0 + y[1] * v1) + (y[2] * v2 + y[3] * v3)


def cut_planes(state, place, offsets):
    out = []
    lane = iota((16, 128), 1)
    for offset in offsets:
        at = place + offset
        inside = jnp.logical_and(at >= 0, at < 32).astype(jnp.int32)
        at = jnp.clip(at, 0, 31)
        plane = state[at & 15]
        plane = jnp.where((at >> 4) * jnp.ones_like(lane) == 1, pltpu.roll(plane, 64, 1), plane)
        out.append(jnp.where(lane < 64 * inside, plane, 0.0))
    return out


def call(body, outs, args, small=(), far=(), scratch=(), flops=0, copies=0, limit=LIMIT):
    spaces = [SMEM if k in small else pltpu.MemorySpace.HBM if k in far else VMEM for k in range(len(args))]
    specs = [pl.BlockSpec(memory_space=space) for space in spaces]
    return pl.pallas_call(
        body,
        out_shape=tuple(jax.ShapeDtypeStruct(s, F32) for s in outs),
        in_specs=specs,
        out_specs=tuple(pl.BlockSpec(memory_space=VMEM) for _ in outs),
        scratch_shapes=(
            *(pltpu.VMEM(s, F32) if isinstance(s, tuple) else s for s in scratch),
            *(pltpu.SemaphoreType.DMA for _ in range(copies)),
        ),
        cost_estimate=pl.CostEstimate(flops=flops, bytes_accessed=1 << 20, transcendentals=0) if flops else None,
        compiler_params=pltpu.CompilerParams(vmem_limit_bytes=limit),
        interpret=INTERPRET,
    )(*args)


def setup_kernel(cond, cur, theirs, labels_far, coils_far, initial_far, own, up, down, far, packed,
                 labels, coils, initial, labels_sem, coils_sem, initial_sem):
    copies = [
        pltpu.make_async_copy(labels_far, labels, labels_sem),
        pltpu.make_async_copy(coils_far, coils, coils_sem),
        pltpu.make_async_copy(initial_far, initial, initial_sem),
    ]
    for copy in copies:
        copy.start()
    for copy in copies:
        copy.wait()
    region = labels[...]
    cell = jnp.where(region == 0, cond[0], 0.0)
    for k in range(1, 4):
        cell = cell + jnp.where(region == k, cond[k], 0.0)
    own[0] = cell
    own[3] = initial[...]
    pattern = [coils[p] for p in range(PHASES)]
    for step in range(2):
        source = cur[step, 0] * pattern[0]
        for p in range(1, PHASES):
            source = source + cur[step, p] * pattern[p]
        own[1 + step] = source
    up[0:2] = own[0, 2:4]
    up[2:5] = own[1, 1:4]
    up[5:6] = own[2, 3:4]
    down[0:3] = own[0, 0:3]
    down[3:7] = own[1]
    down[7:9] = own[2, 0:2]
    up[6:10] = initial[...]
    down[9:13] = initial[...]
    far[...] = initial[0:1]
    fields = [initial[...], cell, *pattern]
    rows = [restrict_packed(jnp.sum(f, axis=0)) for f in fields]
    lane = iota((8, 128), 1)
    row = jnp.zeros((8, 128), F32)
    for k in range(6):
        row = jnp.where(lane == k, theirs[k // 3, k % 3], row)
    rows = jnp.concatenate([*rows, row], axis=0)
    packed[...] = jnp.broadcast_to(rows[None], packed.shape)


def unpack_all(whole, at):
    return unpack(whole[0:16, at : at + 8, :], whole[16:32, at : at + 8, :])


def slice_source(cur, static, n):
    source = jnp.zeros((16, 16, 128), F32)
    for p in range(PHASES):
        source = source + 0.5 * (cur[n, p] + cur[n, PHASES + p]) * static[2 + p]
    return source


def solve_slice(cur, state, static, n):
    state[...] = coarse_solve(state[...], slice_source(cur, static, n), 0.8 * static[1] - 0.4)


AROUND = (-1, 0, 1, 2)


def first_sweep_kernel(where, cur, whole, static, planes, advanced, state):
    mine, place = where[0], where[1]
    for k in range(5):
        static[k] = unpack_all(whole, 8 * k)
    state[...] = static[0]

    def turn(n, carry):
        @pl.when(n == mine)
        def _():
            for k, plane in enumerate(cut_planes(state, place, AROUND)):
                planes[16 * k : 16 * k + 16] = plane

        solve_slice(cur, state, static, n)

        @pl.when(n == mine)
        def _():
            advanced[...] = pack(*cut_planes(state, place, (0,)))

        return carry

    lax.fori_loop(0, 8, turn, 0)


def pack(plane):
    return plane[:8] + pltpu.roll(plane[8:], 64, 1)


def load_corrections(where, ours, theirs, correction):
    odd = where[1] & 1
    for k in range(4):
        correction[4 * odd + k] = unpack_all(ours, 8 * k)
        correction[4 * (1 - odd) + k] = unpack_all(theirs, 8 * k)


def next_sweep_kernel(where, cur, static, begin, old, ours, theirs, planes, advanced, state, kept, correction):
    mine, place = where[0], where[1]
    load_corrections(where, ours, theirs, correction)
    state[...] = begin[...]

    @pl.when(mine == 0)
    def _():
        for k, plane in enumerate(cut_planes(state, place, AROUND)):
            planes[16 * k : 16 * k + 16] = plane

    def turn(n, carry):
        solve_slice(cur, state, static, n)

        @pl.when(n == mine)
        def _():
            advanced[...] = pack(*cut_planes(state, place, (0,)))

        @pl.when(n == mine - 1)
        def _():
            around = cut_planes(state, place, AROUND)
            kept[...] = around[1]
            for k, plane in enumerate(around):
                planes[16 * k : 16 * k + 16] = plane - old[16 * k : 16 * k + 16]

        @pl.when(jnp.logical_and(n == 7, mine == 0))
        def _():
            (new,), (before,) = cut_planes(state, place, (0,)), cut_planes(begin, place, (0,))
            kept[...] = new - before

        state[...] = state[...] + correction[n]
        return carry

    lax.fori_loop(0, 8, turn, 0)


def last_sweep_kernel(where, cur, static, begin, kept, moved_first, moved_other, ours, theirs,
                      start, state, correction, plane):
    mine, place = where[0], where[1]
    load_corrections(where, ours, theirs, correction)
    state[...] = begin[...]
    plane[...] = kept[...]

    def turn(n, carry):
        solve_slice(cur, state, static, n)

        @pl.when(n == mine - 1)
        def _():
            (new,) = cut_planes(state, place, (0,))
            plane[...] = new - kept[...]

        state[...] = state[...] + correction[n]
        return carry

    lax.fori_loop(0, mine, turn, 0)
    (own,) = widen(plane[...])
    first = (mine == 0).astype(F32)
    start[...] = own[None] + (first * moved_first[0:4] + (1.0 - first) * moved_other[0:4])


def fine_beside(v):
    rows, lanes = iota(v.shape, 0), iota(v.shape, 1)
    out = jnp.where(rows == 0, 0.0, pltpu.roll(v, 1, 0)) + jnp.where(rows == 63, 0.0, pltpu.roll(v, 63, 0))
    return out + jnp.where(lanes == 0, 0.0, pltpu.roll(v, 1, 1)) + jnp.where(lanes == 255, 0.0, pltpu.roll(v, 255, 1))


def inside(plane):
    return jnp.logical_and(plane >= 0, plane < 128).astype(F32)


def guarded(value, plane, first):
    return value if 0 <= plane < 4 else inside(first + plane) * value


def part(value):
    folded = jnp.sum(value.reshape(8, 8, 256), axis=0)
    return folded[:, :128] + folded[:, 128:]


def fine_kernel(initial, where, planes, own, up, down, *refs):
    if initial:
        (rest_far,), refs = refs[:1], refs[1:]
        rest, rest_up, rest_down = own.at[3], up, down
    else:
        (rest, rest_up, rest_down), refs = refs[:3], refs[3:]
        rest_far = rest_down.at[4:5]
    fields, packed, u, r, w, q, a = refs
    first = 4 * where[1]
    zero = (where[0] == 0).astype(F32)
    scale = (1.0 - zero, zero) if initial else (1.0, 1.0 - zero)
    above, below = (6, 9) if initial else (0, 0)
    lifted = widen(planes[...])
    pieces = [(rest_up, above + k) for k in range(4)] + [(rest, k) for k in range(4)]
    pieces = pieces + [(rest_down, below + k) for k in range(4)] + [(rest_far, 0)]
    for j, (piece, k) in enumerate(pieces):
        u[j] = scale[0] * lifted[j // 4] + scale[1] * piece[k]

    def weight(plane):
        return up[2 + plane] if plane < 0 else own[0, plane] if plane < 4 else down[plane - 4]

    def source(step, plane):
        before, after = ((5, 3), (6, 7))[step]
        return up[before + plane] if plane < 0 else own[1 + step, plane] if plane < 4 else down[after + plane - 4]

    def beside(field, low, plane):
        j = plane - low
        return field[j - 1] + field[j + 1] + fine_beside(field[j])

    def spread(field, low, plane):
        return beside(field, low, plane) - 6.0 * field[plane - low]

    for plane in range(-3, 8):
        r[plane + 3] = guarded(source(0, plane) + spread(u, -4, plane), plane, first)
    for plane in range(-2, 7):
        w[plane + 2] = guarded(weight(plane) * r[plane + 3] - beside(r, -3, plane), plane, first)
    for plane in range(-1, 6):
        q[0, plane + 1] = guarded(source(1, plane) + spread(u, -4, plane), plane, first)
        q[1, plane + 1] = guarded(spread(r, -3, plane), plane, first)
        q[2, plane + 1] = guarded(spread(w, -2, plane), plane, first)
    for plane in range(5):
        for k in range(3):
            image = weight(plane) * q[k, plane + 1] - beside(q.at[k], -1, plane)
            a[k, plane] = guarded(image, plane, first)
    sums = [jnp.zeros((8, 128), F32)] * 28
    for plane in range(4):
        terms = []
        rv, wv = r[plane + 3], w[plane + 2]
        heavy = weight(plane) + 6.0
        terms += [rv * rv, rv * wv, wv * wv]
        terms += [wv * (heavy * wv - fine_beside(wv) - 2.0 * w[plane + 3])]
        qs = [q[k, plane + 1] for k in range(3)]
        images = [a[k, plane] for k in range(3)]
        twice = []
        for k in range(3):
            value = heavy * images[k] - fine_beside(images[k]) - a[k, plane + 1]
            twice.append(value - a[k, plane - 1] if plane else value)
        for i, j in PAIRS:
            last = images[i] * twice[j]
            if plane == 3:
                last = last - a[i, 4] * images[j]
            terms += [qs[i] * qs[j], qs[i] * images[j], images[i] * images[j], last]
        sums = [s + part(v) for s, v in zip(sums, terms)]
    lane = iota((1, 128), 1)
    row = jnp.zeros((1, 128), F32)
    for k in range(28):
        row = jnp.where(lane == k, total(sums[k]), row)
    packed[...] = jnp.broadcast_to(row, packed.shape)
    fields[0] = u[4:9]
    fields[1] = r[3:8]
    fields[2] = w[2:7]
    for k in range(3):
        fields[3 + k] = q[k, 1:6]
        fields[6 + k] = a[k, 0:5]


PAIRS = ((0, 0), (0, 1), (0, 2), (1, 1), (1, 2), (2, 2))


def weights(norm, cross, square, product):
    first = cross + 6.0 * norm
    step = norm / first
    keep = 1.0 - 6.0 * step
    new = keep * keep * norm - 2.0 * keep * step * cross + step * step * square
    second = keep * keep * first - 2.0 * keep * step * (square + 6.0 * cross) + step * step * product
    ratio = new / norm
    second = new / (second - ratio * new / step)
    return step + second * (keep + ratio), -second * step


def finish_kernel(sums, fields, advanced, fine, moved, ends):
    row = jnp.sum(sums[...], axis=0, keepdims=True)
    lane = iota((1, 128), 1)
    m = [jnp.sum(jnp.where(lane == k, row, 0.0), axis=1, keepdims=True) for k in range(28)]
    a, b = weights(*m[:4])
    factor = {(0, 0): 1.0, (0, 1): 2.0 * a, (0, 2): 2.0 * b, (1, 1): a * a, (1, 2): 2.0 * (a * b), (2, 2): b * b}
    after = [sum(factor[pair] * m[4 + 4 * p + k] for p, pair in enumerate(PAIRS)) for k in range(4)]
    c, d = weights(*after)
    scales = (None, a, b, c, c * a, c * b, d, d * a, d * b)
    for i in range(5):
        value = fields[0, i]
        for k in range(1, 9):
            value = value + scales[k] * fields[k, i]
        moved[i] = value
        if i < 4:
            fine[i] = value
    own = restrict_packed(jnp.sum(moved[0:4], axis=0))
    ends[...] = jnp.broadcast_to((own - advanced[...])[None], ends.shape)


def spread_kernel(ends, rest, packed):
    for half in range(2):
        rows = ends[4 * half : 4 * half + 4].reshape(1, 32, 128)
        for k in range(half, packed.shape[0], 2):
            packed[k : k + 1] = rows


def shifted(x, axis, by, ring):
    n = lax.axis_size(axis)
    pairs = [(i, (i + by) % n) for i in range(n) if ring or 0 <= i + by < n]
    return lax.ppermute(x, axis, pairs)


def exchange(x, axis):
    return lax.all_to_all(x, axis, split_axis=0, concat_axis=0, tiled=True)


def everywhere(ends, rest):
    (packed,) = call(spread_kernel, ((32, 32, 128),), (exchange(ends, "tm"), rest), far=(1,))
    half = exchange(packed, "space")
    places = lax.axis_size("space")
    return half, lax.ppermute(half, "space", [(i, i ^ 1) for i in range(places)])


def body(labels, conductivity, coil_pattern, currents, initial_state):
    tm, place = lax.axis_index("tm"), lax.axis_index("space")
    where = jnp.stack([tm, place]).astype(jnp.int32)
    block, field = (4, 64, 256), (16, 16, 128)

    slices, across = lax.axis_size("tm"), lax.axis_size("space")
    pairs = [
        (b * across + slices * a + t, t * across + slices * a + b)
        for t in range(slices)
        for b in range(slices)
        for a in range(across // slices)
    ]
    theirs = lax.ppermute(currents[0], ("tm", "space"), pairs)

    own, up, down, far, packed = call(
        setup_kernel,
        ((4, *block), (10, 64, 256), (13, 64, 256), (1, 64, 256), (32, 48, 128)),
        (conductivity, currents[0], theirs, labels, coil_pattern, initial_state),
        small=(0, 1, 2),
        far=(3, 4, 5),
        scratch=(pltpu.VMEM(block, jnp.int32), (3, *block), block),
        copies=3,
        limit=60 << 20,
    )
    whole = exchange(packed, "space")
    table = whole[:8, 40, :]
    up, down, far, whole = lax.optimization_barrier((up, down, far, whole))
    up, down = shifted(up, "space", 1, False), shifted(down, "space", -1, False)
    far = shifted(far, "space", -2, False)
    static, planes, advanced, state = call(
        first_sweep_kernel,
        ((5, *field), (64, 128), (8, 128), field),
        (where, table, whole),
        small=(0, 1),
        flops=1 << 26,
    )

    def fine(initial, planes, advanced, rest):
        fields, sums = call(
            functools.partial(fine_kernel, initial),
            ((9, 5, 64, 256), (32, 128)),
            (where, planes, own, up, down, *rest),
            small=(0,),
            scratch=((13, 64, 256), (11, 64, 256), (9, 64, 256), (3, 7, 64, 256), (3, 5, 64, 256)),
        )
        return call(
            finish_kernel,
            (block, (5, 64, 256), (8, 8, 128)),
            (exchange(sums, "space"), fields, advanced),
        )

    _, moved, ends = fine(True, planes, advanced, (far,))
    moved_first = shifted(moved, "tm", 1, True)
    planes, advanced, state, kept = call(
        next_sweep_kernel,
        ((64, 128), (8, 128), field, (16, 128)),
        (where, table, static, state, planes, *everywhere(ends, moved_first)),
        small=(0, 1),
        scratch=((8, *field),),
        flops=1 << 26,
    )
    around = (shifted(moved_first, "space", 1, False), shifted(moved_first, "space", -1, False))
    fine_state, moved, ends = fine(False, planes, advanced, (moved_first, *around))
    moved_other = shifted(moved, "tm", 1, False)
    (start,) = call(
        last_sweep_kernel,
        (block,),
        (where, table, static, state, kept, moved_first, moved_other, *everywhere(ends, moved_other)),
        small=(0, 1),
        scratch=(field, (8, *field), (16, 128)),
        flops=1 << 26,
    )
    return (start[None], fine_state[None])


def solution(mesh):
    in_specs = (
        P("space", None, None),
        P(),
        P(None, "space", None, None),
        P("tm", None, None),
        P("space", None, None),
    )
    out_specs = (P("tm", "space", None, None), P("tm", "space", None, None))
    return jax.shard_map(body, mesh=mesh, in_specs=in_specs, out_specs=out_specs, check_vma=False)
```

```python
import functools

import jax
import jax.numpy as jnp
from jax import lax
from jax.experimental import pallas as pl
from jax.experimental.pallas import tpu as pltpu
from jax.sharding import PartitionSpec as P

PHASES = 3
CG_COARSE = 4
F32 = jnp.float32
HIGHEST = lax.Precision.HIGHEST
VMEM = pltpu.MemorySpace.VMEM
SMEM = pltpu.MemorySpace.SMEM
INTERPRET = False
LIMIT = 12 << 20


def iota(shape, dim):
    return lax.broadcasted_iota(jnp.int32, shape, dim)


def dot(a, b):
    return lax.dot_general(a, b, (((1,), (0,)), ((), ())), precision=HIGHEST, preferred_element_type=F32)


def total(x):
    while x.ndim > 2:
        x = jnp.sum(x, axis=0)
    return jnp.sum(jnp.sum(x, axis=0, keepdims=True), axis=1, keepdims=True)


def restrict_packed(summed):
    columns = (iota((256, 128), 0) >> 2) == (iota((256, 128), 1) & 63)
    rows = (iota((16, 64), 1) >> 2) == iota((16, 64), 0)
    half = dot(summed, jnp.where(columns, 1.0 / 64.0, 0.0).astype(F32))
    both = dot(jnp.where(rows, 1.0, 0.0).astype(F32), half)
    return jnp.where(iota((8, 128), 1) < 64, both[:8], both[8:])


def widen(planes):
    columns = (iota((128, 256), 1) >> 2) == iota((128, 256), 0)
    rows = (iota((64, 16), 0) >> 2) == iota((64, 16), 1)
    wide = dot(planes, jnp.where(columns, 1.0, 0.0).astype(F32))
    lift = jnp.where(rows, 1.0, 0.0).astype(F32)
    return [dot(lift, wide[k : k + 16]) for k in range(0, planes.shape[0], 16)]


def unpack(low, high):
    axis = low.ndim - 1
    left = iota(low.shape, axis) < 64
    top = jnp.where(left, low, pltpu.roll(high, 64, axis))
    bottom = jnp.where(left, pltpu.roll(low, 64, axis), high)
    return jnp.concatenate([top, bottom], axis=axis - 1)


def coarse_beside(v):
    one = (1, 16, 128)
    lane, row = iota(one, 2), iota(one, 1)
    left = lane < 64
    first, last = pltpu.roll(v[:1], 64, 2), pltpu.roll(v[15:], 64, 2)
    after = jnp.concatenate([v[1:], jnp.where(left, first, 0.0)], axis=0)
    before = jnp.concatenate([jnp.where(left, 0.0, last), v[:15]], axis=0)
    out = after + before
    out = out + jnp.where(row == 0, 0.0, pltpu.roll(v, 1, 1)) + jnp.where(row == 15, 0.0, pltpu.roll(v, 15, 1))
    inner = lane & 63
    return out + jnp.where(inner == 0, 0.0, pltpu.roll(v, 1, 2)) + jnp.where(inner == 63, 0.0, pltpu.roll(v, 127, 2))


def coarse_solve(start, source, diagonal):
    def apply(v):
        return diagonal * v - 0.0625 * coarse_beside(v)

    x = start
    residual = source - 0.375 * start + 0.0625 * coarse_beside(start)
    image = apply(residual)
    norm, product = total(residual * residual), total(residual * image)
    step = norm / product
    direction, moved = residual, image
    for turn in range(CG_COARSE):
        inverse = 1.0 / norm
        scaled = inverse / step
        x = x + step[None] * direction
        if turn + 1 < CG_COARSE:
            residual = residual - step[None] * moved
            image = apply(residual)
            new, product = total(residual * residual), total(residual * image)
            ratio = new * inverse
            step = new / (product - new * (new * scaled))
            direction = residual + ratio[None] * direction
            moved = image + ratio[None] * moved
            norm = new
    return x


def cut_planes(state, place, offsets):
    out = []
    lane = iota((16, 128), 1)
    for offset in offsets:
        at = place + offset
        inside = jnp.logical_and(at >= 0, at < 32).astype(jnp.int32)
        at = jnp.clip(at, 0, 31)
        plane = state[at & 15]
        plane = jnp.where((at >> 4) * jnp.ones_like(lane) == 1, pltpu.roll(plane, 64, 1), plane)
        out.append(jnp.where(lane < 64 * inside, plane, 0.0))
    return out


def call(body, outs, args, small=(), far=(), scratch=(), flops=0, copies=0, limit=LIMIT):
    spaces = [SMEM if k in small else pltpu.MemorySpace.HBM if k in far else VMEM for k in range(len(args))]
    specs = [pl.BlockSpec(memory_space=space) for space in spaces]
    return pl.pallas_call(
        body,
        out_shape=tuple(jax.ShapeDtypeStruct(s, F32) for s in outs),
        in_specs=specs,
        out_specs=tuple(pl.BlockSpec(memory_space=VMEM) for _ in outs),
        scratch_shapes=(
            *(pltpu.VMEM(s, F32) if isinstance(s, tuple) else s for s in scratch),
            *(pltpu.SemaphoreType.DMA for _ in range(copies)),
        ),
        cost_estimate=pl.CostEstimate(flops=flops, bytes_accessed=1 << 20, transcendentals=0) if flops else None,
        compiler_params=pltpu.CompilerParams(vmem_limit_bytes=limit),
        interpret=INTERPRET,
    )(*args)


def setup_kernel(cond, cur, theirs, labels_far, coils_far, initial_far, own, up, down, far, packed,
                 labels, coils, initial, labels_sem, coils_sem, initial_sem):
    copies = [
        pltpu.make_async_copy(labels_far, labels, labels_sem),
        pltpu.make_async_copy(coils_far, coils, coils_sem),
        pltpu.make_async_copy(initial_far, initial, initial_sem),
    ]
    for copy in copies:
        copy.start()
    for copy in copies:
        copy.wait()
    region = labels[...]
    cell = jnp.where(region == 0, cond[0], 0.0)
    for k in range(1, 4):
        cell = cell + jnp.where(region == k, cond[k], 0.0)
    own[0] = cell
    own[3] = initial[...]
    pattern = [coils[p] for p in range(PHASES)]
    for step in range(2):
        source = cur[step, 0] * pattern[0]
        for p in range(1, PHASES):
            source = source + cur[step, p] * pattern[p]
        own[1 + step] = source
    up[0:2] = own[0, 2:4]
    up[2:5] = own[1, 1:4]
    up[5:6] = own[2, 3:4]
    down[0:3] = own[0, 0:3]
    down[3:7] = own[1]
    down[7:9] = own[2, 0:2]
    up[6:10] = initial[...]
    down[9:13] = initial[...]
    far[...] = initial[0:1]
    fields = [initial[...], cell, *pattern]
    rows = [restrict_packed(jnp.sum(f, axis=0)) for f in fields]
    lane = iota((8, 128), 1)
    row = jnp.zeros((8, 128), F32)
    for k in range(6):
        row = jnp.where(lane == k, theirs[k // 3, k % 3], row)
    rows = jnp.concatenate([*rows, row], axis=0)
    packed[...] = jnp.broadcast_to(rows[None], packed.shape)


def unpack_all(whole, at):
    return unpack(whole[0:16, at : at + 8, :], whole[16:32, at : at + 8, :])


def slice_source(cur, static, n):
    source = jnp.zeros((16, 16, 128), F32)
    for p in range(PHASES):
        source = source + 0.5 * (cur[n, p] + cur[n, PHASES + p]) * static[2 + p]
    return source


def solve_slice(cur, state, static, n):
    state[...] = coarse_solve(state[...], slice_source(cur, static, n), 0.5 * static[1] + 0.375)


AROUND = (-1, 0, 1, 2)


def first_sweep_kernel(where, cur, whole, static, planes, advanced, state):
    mine, place = where[0], where[1]
    for k in range(5):
        static[k] = unpack_all(whole, 8 * k)
    state[...] = static[0]

    def turn(n, carry):
        @pl.when(n == mine)
        def _():
            for k, plane in enumerate(cut_planes(state, place, AROUND)):
                planes[16 * k : 16 * k + 16] = plane

        solve_slice(cur, state, static, n)

        @pl.when(n == mine)
        def _():
            advanced[...] = pack(*cut_planes(state, place, (0,)))

        return carry

    lax.fori_loop(0, 8, turn, 0)


def pack(plane):
    return plane[:8] + pltpu.roll(plane[8:], 64, 1)


def load_corrections(where, ours, theirs, correction):
    odd = where[1] & 1
    for k in range(4):
        correction[4 * odd + k] = unpack_all(ours, 8 * k)
        correction[4 * (1 - odd) + k] = unpack_all(theirs, 8 * k)


def next_sweep_kernel(where, cur, static, begin, old, ours, theirs, planes, advanced, state, kept, correction):
    mine, place = where[0], where[1]
    load_corrections(where, ours, theirs, correction)
    state[...] = begin[...]

    @pl.when(mine == 0)
    def _():
        for k, plane in enumerate(cut_planes(state, place, AROUND)):
            planes[16 * k : 16 * k + 16] = plane

    def turn(n, carry):
        solve_slice(cur, state, static, n)

        @pl.when(n == mine)
        def _():
            advanced[...] = pack(*cut_planes(state, place, (0,)))

        @pl.when(n == mine - 1)
        def _():
            around = cut_planes(state, place, AROUND)
            kept[...] = around[1]
            for k, plane in enumerate(around):
                planes[16 * k : 16 * k + 16] = plane - old[16 * k : 16 * k + 16]

        @pl.when(jnp.logical_and(n == 7, mine == 0))
        def _():
            (new,), (before,) = cut_planes(state, place, (0,)), cut_planes(begin, place, (0,))
            kept[...] = new - before

        state[...] = state[...] + correction[n]
        return carry

    lax.fori_loop(0, 8, turn, 0)


def last_sweep_kernel(where, cur, static, begin, kept, moved_first, moved_other, ours, theirs,
                      start, state, correction, plane):
    mine, place = where[0], where[1]
    load_corrections(where, ours, theirs, correction)
    state[...] = begin[...]
    plane[...] = kept[...]

    def turn(n, carry):
        solve_slice(cur, state, static, n)

        @pl.when(n == mine - 1)
        def _():
            (new,) = cut_planes(state, place, (0,))
            plane[...] = new - kept[...]

        state[...] = state[...] + correction[n]
        return carry

    lax.fori_loop(0, mine, turn, 0)
    (own,) = widen(plane[...])
    first = (mine == 0).astype(F32)
    start[...] = own[None] + (first * moved_first[0:4] + (1.0 - first) * moved_other[0:4])


def fine_beside(v):
    rows, lanes = iota(v.shape, 0), iota(v.shape, 1)
    out = jnp.where(rows == 0, 0.0, pltpu.roll(v, 1, 0)) + jnp.where(rows == 63, 0.0, pltpu.roll(v, 63, 0))
    return out + jnp.where(lanes == 0, 0.0, pltpu.roll(v, 1, 1)) + jnp.where(lanes == 255, 0.0, pltpu.roll(v, 255, 1))


def inside(plane):
    return jnp.logical_and(plane >= 0, plane < 128).astype(F32)


def guarded(value, plane, first):
    return value if 0 <= plane < 4 else inside(first + plane) * value


def part(value):
    folded = jnp.sum(value.reshape(8, 8, 256), axis=0)
    return folded[:, :128] + folded[:, 128:]


def fine_kernel(initial, where, planes, own, up, down, *refs):
    if initial:
        (rest_far,), refs = refs[:1], refs[1:]
        rest, rest_up, rest_down = own.at[3], up, down
    else:
        (rest, rest_up, rest_down), refs = refs[:3], refs[3:]
        rest_far = rest_down.at[4:5]
    fields, packed, u, r, w, q, a = refs
    first = 4 * where[1]
    zero = (where[0] == 0).astype(F32)
    scale = (1.0 - zero, zero) if initial else (1.0, 1.0 - zero)
    above, below = (6, 9) if initial else (0, 0)
    lifted = widen(planes[...])
    pieces = [(rest_up, above + k) for k in range(4)] + [(rest, k) for k in range(4)]
    pieces = pieces + [(rest_down, below + k) for k in range(4)] + [(rest_far, 0)]
    for j, (piece, k) in enumerate(pieces):
        u[j] = scale[0] * lifted[j // 4] + scale[1] * piece[k]

    def weight(plane):
        return up[2 + plane] if plane < 0 else own[0, plane] if plane < 4 else down[plane - 4]

    def source(step, plane):
        before, after = ((5, 3), (6, 7))[step]
        return up[before + plane] if plane < 0 else own[1 + step, plane] if plane < 4 else down[after + plane - 4]

    def beside(field, low, plane):
        j = plane - low
        return field[j - 1] + field[j + 1] + fine_beside(field[j])

    def spread(field, low, plane):
        return beside(field, low, plane) - 6.0 * field[plane - low]

    for plane in range(-3, 8):
        r[plane + 3] = guarded(source(0, plane) + spread(u, -4, plane), plane, first)
    for plane in range(-2, 7):
        w[plane + 2] = guarded(weight(plane) * r[plane + 3] - beside(r, -3, plane), plane, first)
    for plane in range(-1, 6):
        q[0, plane + 1] = guarded(source(1, plane) + spread(u, -4, plane), plane, first)
        q[1, plane + 1] = guarded(spread(r, -3, plane), plane, first)
        q[2, plane + 1] = guarded(spread(w, -2, plane), plane, first)
    for plane in range(5):
        for k in range(3):
            image = weight(plane) * q[k, plane + 1] - beside(q.at[k], -1, plane)
            a[k, plane] = guarded(image, plane, first)
    sums = [jnp.zeros((8, 128), F32)] * 28
    for plane in range(4):
        terms = []
        rv, wv = r[plane + 3], w[plane + 2]
        heavy = weight(plane) + 6.0
        terms += [rv * rv, rv * wv, wv * wv]
        terms += [wv * (heavy * wv - fine_beside(wv) - 2.0 * w[plane + 3])]
        qs = [q[k, plane + 1] for k in range(3)]
        images = [a[k, plane] for k in range(3)]
        twice = []
        for k in range(3):
            value = heavy * images[k] - fine_beside(images[k]) - a[k, plane + 1]
            twice.append(value - a[k, plane - 1] if plane else value)
        for i, j in PAIRS:
            last = images[i] * twice[j]
            if plane == 3:
                last = last - a[i, 4] * images[j]
            terms += [qs[i] * qs[j], qs[i] * images[j], images[i] * images[j], last]
        sums = [s + part(v) for s, v in zip(sums, terms)]
    lane = iota((1, 128), 1)
    row = jnp.zeros((1, 128), F32)
    for k in range(28):
        row = jnp.where(lane == k, total(sums[k]), row)
    packed[...] = jnp.broadcast_to(row, packed.shape)
    fields[0] = u[4:9]
    fields[1] = r[3:8]
    fields[2] = w[2:7]
    for k in range(3):
        fields[3 + k] = q[k, 1:6]
        fields[6 + k] = a[k, 0:5]


PAIRS = ((0, 0), (0, 1), (0, 2), (1, 1), (1, 2), (2, 2))


def weights(norm, cross, square, product):
    first = cross + 6.0 * norm
    step = norm / first
    keep = 1.0 - 6.0 * step
    new = keep * keep * norm - 2.0 * keep * step * cross + step * step * square
    second = keep * keep * first - 2.0 * keep * step * (square + 6.0 * cross) + step * step * product
    ratio = new / norm
    second = new / (second - ratio * new / step)
    return step + second * (keep + ratio), -second * step


def finish_kernel(sums, fields, advanced, fine, moved, ends):
    row = jnp.sum(sums[...], axis=0, keepdims=True)
    lane = iota((1, 128), 1)
    m = [jnp.sum(jnp.where(lane == k, row, 0.0), axis=1, keepdims=True) for k in range(28)]
    a, b = weights(*m[:4])
    factor = {(0, 0): 1.0, (0, 1): 2.0 * a, (0, 2): 2.0 * b, (1, 1): a * a, (1, 2): 2.0 * (a * b), (2, 2): b * b}
    after = [sum(factor[pair] * m[4 + 4 * p + k] for p, pair in enumerate(PAIRS)) for k in range(4)]
    c, d = weights(*after)
    scales = (None, a, b, c, c * a, c * b, d, d * a, d * b)
    for i in range(5):
        value = fields[0, i]
        for k in range(1, 9):
            value = value + scales[k] * fields[k, i]
        moved[i] = value
        if i < 4:
            fine[i] = value
    own = restrict_packed(jnp.sum(moved[0:4], axis=0))
    ends[...] = jnp.broadcast_to((own - advanced[...])[None], ends.shape)


def spread_kernel(ends, rest, packed):
    for half in range(2):
        rows = ends[4 * half : 4 * half + 4].reshape(1, 32, 128)
        for k in range(half, packed.shape[0], 2):
            packed[k : k + 1] = rows


def shifted(x, axis, by, ring):
    n = lax.axis_size(axis)
    pairs = [(i, (i + by) % n) for i in range(n) if ring or 0 <= i + by < n]
    return lax.ppermute(x, axis, pairs)


def exchange(x, axis):
    return lax.all_to_all(x, axis, split_axis=0, concat_axis=0, tiled=True)


def everywhere(ends, rest):
    (packed,) = call(spread_kernel, ((32, 32, 128),), (exchange(ends, "tm"), rest), far=(1,))
    half = exchange(packed, "space")
    places = lax.axis_size("space")
    return half, lax.ppermute(half, "space", [(i, i ^ 1) for i in range(places)])


def body(labels, conductivity, coil_pattern, currents, initial_state):
    tm, place = lax.axis_index("tm"), lax.axis_index("space")
    where = jnp.stack([tm, place]).astype(jnp.int32)
    block, field = (4, 64, 256), (16, 16, 128)

    slices, across = lax.axis_size("tm"), lax.axis_size("space")
    pairs = [
        (b * across + slices * a + t, t * across + slices * a + b)
        for t in range(slices)
        for b in range(slices)
        for a in range(across // slices)
    ]
    theirs = lax.ppermute(currents[0], ("tm", "space"), pairs)

    own, up, down, far, packed = call(
        setup_kernel,
        ((4, *block), (10, 64, 256), (13, 64, 256), (1, 64, 256), (32, 48, 128)),
        (conductivity, currents[0], theirs, labels, coil_pattern, initial_state),
        small=(0, 1, 2),
        far=(3, 4, 5),
        scratch=(pltpu.VMEM(block, jnp.int32), (3, *block), block),
        copies=3,
        limit=60 << 20,
    )
    whole = exchange(packed, "space")
    table = whole[:8, 40, :]
    up, down, far, whole = lax.optimization_barrier((up, down, far, whole))
    up, down = shifted(up, "space", 1, False), shifted(down, "space", -1, False)
    far = shifted(far, "space", -2, False)
    static, planes, advanced, state = call(
        first_sweep_kernel,
        ((5, *field), (64, 128), (8, 128), field),
        (where, table, whole),
        small=(0, 1),
        flops=1 << 26,
    )

    def fine(initial, planes, advanced, rest):
        fields, sums = call(
            functools.partial(fine_kernel, initial),
            ((9, 5, 64, 256), (32, 128)),
            (where, planes, own, up, down, *rest),
            small=(0,),
            scratch=((13, 64, 256), (11, 64, 256), (9, 64, 256), (3, 7, 64, 256), (3, 5, 64, 256)),
        )
        return call(
            finish_kernel,
            (block, (5, 64, 256), (8, 8, 128)),
            (exchange(sums, "space"), fields, advanced),
        )

    _, moved, ends = fine(True, planes, advanced, (far,))
    moved_first = shifted(moved, "tm", 1, True)
    planes, advanced, state, kept = call(
        next_sweep_kernel,
        ((64, 128), (8, 128), field, (16, 128)),
        (where, table, static, state, planes, *everywhere(ends, moved_first)),
        small=(0, 1),
        scratch=((8, *field),),
        flops=1 << 26,
    )
    around = (shifted(moved_first, "space", 1, False), shifted(moved_first, "space", -1, False))
    fine_state, moved, ends = fine(False, planes, advanced, (moved_first, *around))
    moved_other = shifted(moved, "tm", 1, False)
    (start,) = call(
        last_sweep_kernel,
        (block,),
        (where, table, static, state, kept, moved_first, moved_other, *everywhere(ends, moved_other)),
        small=(0, 1),
        scratch=(field, (8, *field), (16, 128)),
        flops=1 << 26,
    )
    return (start[None], fine_state[None])


def solution(mesh):
    in_specs = (
        P("space", None, None),
        P(),
        P(None, "space", None, None),
        P("tm", None, None),
        P("space", None, None),
    )
    out_specs = (P("tm", "space", None, None), P("tm", "space", None, None))
    return jax.shard_map(body, mesh=mesh, in_specs=in_specs, out_specs=out_specs, check_vma=False)
```

```python
import functools

import jax
import jax.numpy as jnp
from jax import lax
from jax.experimental import pallas as pl
from jax.experimental.pallas import tpu as pltpu
from jax.sharding import PartitionSpec as P

PHASES = 3
CG_COARSE = 4
F32 = jnp.float32
HIGHEST = lax.Precision.HIGHEST
VMEM = pltpu.MemorySpace.VMEM
SMEM = pltpu.MemorySpace.SMEM
INTERPRET = False
LIMIT = 12 << 20


def iota(shape, dim):
    return lax.broadcasted_iota(jnp.int32, shape, dim)


def dot(a, b):
    return lax.dot_general(a, b, (((1,), (0,)), ((), ())), precision=HIGHEST, preferred_element_type=F32)


def total(x):
    while x.ndim > 2:
        x = jnp.sum(x, axis=0)
    return jnp.sum(jnp.sum(x, axis=0, keepdims=True), axis=1, keepdims=True)


def restrict_packed(summed):
    columns = (iota((256, 128), 0) >> 2) == (iota((256, 128), 1) & 63)
    rows = (iota((16, 64), 1) >> 2) == iota((16, 64), 0)
    half = dot(summed, jnp.where(columns, 1.0 / 64.0, 0.0).astype(F32))
    both = dot(jnp.where(rows, 1.0, 0.0).astype(F32), half)
    return jnp.where(iota((8, 128), 1) < 64, both[:8], both[8:])


def widen(planes):
    columns = (iota((128, 256), 1) >> 2) == iota((128, 256), 0)
    rows = (iota((64, 16), 0) >> 2) == iota((64, 16), 1)
    wide = dot(planes, jnp.where(columns, 1.0, 0.0).astype(F32))
    lift = jnp.where(rows, 1.0, 0.0).astype(F32)
    return [dot(lift, wide[k : k + 16]) for k in range(0, planes.shape[0], 16)]


def unpack(low, high):
    axis = low.ndim - 1
    left = iota(low.shape, axis) < 64
    top = jnp.where(left, low, pltpu.roll(high, 64, axis))
    bottom = jnp.where(left, pltpu.roll(low, 64, axis), high)
    return jnp.concatenate([top, bottom], axis=axis - 1)


def coarse_beside(v):
    one = (1, 16, 128)
    lane, row = iota(one, 2), iota(one, 1)
    left = lane < 64
    first, last = pltpu.roll(v[:1], 64, 2), pltpu.roll(v[15:], 64, 2)
    after = jnp.concatenate([v[1:], jnp.where(left, first, 0.0)], axis=0)
    before = jnp.concatenate([jnp.where(left, 0.0, last), v[:15]], axis=0)
    out = after + before
    out = out + jnp.where(row == 0, 0.0, pltpu.roll(v, 1, 1)) + jnp.where(row == 15, 0.0, pltpu.roll(v, 15, 1))
    inner = lane & 63
    return out + jnp.where(inner == 0, 0.0, pltpu.roll(v, 1, 2)) + jnp.where(inner == 63, 0.0, pltpu.roll(v, 127, 2))


def coarse_solve(start, source, diagonal):
    def apply(v):
        return diagonal * v - 0.0625 * coarse_beside(v)

    x = start
    residual = source - 0.375 * start + 0.0625 * coarse_beside(start)
    image = apply(residual)
    norm, product = total(residual * residual), total(residual * image)
    step = norm / product
    direction, moved = residual, image
    for turn in range(CG_COARSE):
        inverse = 1.0 / norm
        scaled = inverse / step
        x = x + step[None] * direction
        if turn + 1 < CG_COARSE:
            residual = residual - step[None] * moved
            image = apply(residual)
            new, product = total(residual * residual), total(residual * image)
            ratio = new * inverse
            step = new / (product - new * (new * scaled))
            direction = residual + ratio[None] * direction
            moved = image + ratio[None] * moved
            norm = new
    return x


def cut_planes(state, place, offsets):
    out = []
    lane = iota((16, 128), 1)
    for offset in offsets:
        at = place + offset
        inside = jnp.logical_and(at >= 0, at < 32).astype(jnp.int32)
        at = jnp.clip(at, 0, 31)
        plane = state[at & 15]
        plane = jnp.where((at >> 4) * jnp.ones_like(lane) == 1, pltpu.roll(plane, 64, 1), plane)
        out.append(jnp.where(lane < 64 * inside, plane, 0.0))
    return out


def call(body, outs, args, small=(), far=(), scratch=(), flops=0, copies=0, limit=LIMIT):
    spaces = [SMEM if k in small else pltpu.MemorySpace.HBM if k in far else VMEM for k in range(len(args))]
    specs = [pl.BlockSpec(memory_space=space) for space in spaces]
    return pl.pallas_call(
        body,
        out_shape=tuple(jax.ShapeDtypeStruct(s, F32) for s in outs),
        in_specs=specs,
        out_specs=tuple(pl.BlockSpec(memory_space=VMEM) for _ in outs),
        scratch_shapes=(
            *(pltpu.VMEM(s, F32) if isinstance(s, tuple) else s for s in scratch),
            *(pltpu.SemaphoreType.DMA for _ in range(copies)),
        ),
        cost_estimate=pl.CostEstimate(flops=flops, bytes_accessed=1 << 20, transcendentals=0) if flops else None,
        compiler_params=pltpu.CompilerParams(vmem_limit_bytes=limit),
        interpret=INTERPRET,
    )(*args)


def setup_kernel(cond, cur, theirs, labels_far, coils_far, initial_far, own, up, down, far, packed,
                 labels, coils, initial, labels_sem, coils_sem, initial_sem):
    copies = [
        pltpu.make_async_copy(labels_far, labels, labels_sem),
        pltpu.make_async_copy(coils_far, coils, coils_sem),
        pltpu.make_async_copy(initial_far, initial, initial_sem),
    ]
    for copy in copies:
        copy.start()
    for copy in copies:
        copy.wait()
    region = labels[...]
    cell = jnp.where(region == 0, cond[0], 0.0)
    for k in range(1, 4):
        cell = cell + jnp.where(region == k, cond[k], 0.0)
    own[0] = cell
    own[3] = initial[...]
    pattern = [coils[p] for p in range(PHASES)]
    for step in range(2):
        source = cur[step, 0] * pattern[0]
        for p in range(1, PHASES):
            source = source + cur[step, p] * pattern[p]
        own[1 + step] = source
    up[0:2] = own[0, 2:4]
    up[2:5] = own[1, 1:4]
    up[5:6] = own[2, 3:4]
    down[0:3] = own[0, 0:3]
    down[3:7] = own[1]
    down[7:9] = own[2, 0:2]
    up[6:10] = initial[...]
    down[9:13] = initial[...]
    far[...] = initial[0:1]
    fields = [initial[...], cell, *pattern]
    rows = [restrict_packed(jnp.sum(f, axis=0)) for f in fields]
    lane = iota((8, 128), 1)
    row = jnp.zeros((8, 128), F32)
    for k in range(6):
        row = jnp.where(lane == k, theirs[k // 3, k % 3], row)
    rows = jnp.concatenate([*rows, row], axis=0)
    packed[...] = jnp.broadcast_to(rows[None], packed.shape)


def unpack_all(whole, at):
    return unpack(whole[0:16, at : at + 8, :], whole[16:32, at : at + 8, :])


def slice_source(cur, static, n):
    source = jnp.zeros((16, 16, 128), F32)
    for p in range(PHASES):
        source = source + 0.5 * (cur[n, p] + cur[n, PHASES + p]) * static[2 + p]
    return source


def solve_slice(cur, state, static, n):
    state[...] = coarse_solve(state[...], slice_source(cur, static, n), 0.5 * static[1] + 0.375)


AROUND = (-1, 0, 1, 2)


def first_sweep_kernel(where, cur, whole, static, planes, advanced, state):
    mine, place = where[0], where[1]
    for k in range(5):
        static[k] = unpack_all(whole, 8 * k)
    state[...] = static[0]

    def turn(n, carry):
        @pl.when(n == mine)
        def _():
            for k, plane in enumerate(cut_planes(state, place, AROUND)):
                planes[16 * k : 16 * k + 16] = plane

        solve_slice(cur, state, static, n)

        @pl.when(n == mine)
        def _():
            advanced[...] = pack(*cut_planes(state, place, (0,)))

        return carry

    lax.fori_loop(0, 8, turn, 0)


def pack(plane):
    return plane[:8] + pltpu.roll(plane[8:], 64, 1)


def load_corrections(where, ours, theirs, correction):
    odd = where[1] & 1
    for k in range(4):
        correction[4 * odd + k] = unpack_all(ours, 8 * k)
        correction[4 * (1 - odd) + k] = unpack_all(theirs, 8 * k)


def next_sweep_kernel(where, cur, static, begin, old, ours, theirs, planes, advanced, state, kept, correction):
    mine, place = where[0], where[1]
    load_corrections(where, ours, theirs, correction)
    state[...] = begin[...]

    @pl.when(mine == 0)
    def _():
        for k, plane in enumerate(cut_planes(state, place, AROUND)):
            planes[16 * k : 16 * k + 16] = plane

    def turn(n, carry):
        solve_slice(cur, state, static, n)

        @pl.when(n == mine)
        def _():
            advanced[...] = pack(*cut_planes(state, place, (0,)))

        @pl.when(n == mine - 1)
        def _():
            around = cut_planes(state, place, AROUND)
            kept[...] = around[1]
            for k, plane in enumerate(around):
                planes[16 * k : 16 * k + 16] = plane - old[16 * k : 16 * k + 16]

        @pl.when(jnp.logical_and(n == 7, mine == 0))
        def _():
            (new,), (before,) = cut_planes(state, place, (0,)), cut_planes(begin, place, (0,))
            kept[...] = new - before

        state[...] = state[...] + correction[n]
        return carry

    lax.fori_loop(0, 8, turn, 0)


def last_sweep_kernel(where, cur, static, begin, kept, moved_first, moved_other, ours, theirs,
                      start, state, correction, plane):
    mine, place = where[0], where[1]
    load_corrections(where, ours, theirs, correction)
    state[...] = begin[...]
    plane[...] = kept[...]

    def turn(n, carry):
        solve_slice(cur, state, static, n)

        @pl.when(n == mine - 1)
        def _():
            (new,) = cut_planes(state, place, (0,))
            plane[...] = new - kept[...]

        state[...] = state[...] + correction[n]
        return carry

    lax.fori_loop(0, mine, turn, 0)
    (own,) = widen(plane[...])
    first = (mine == 0).astype(F32)
    start[...] = own[None] + (first * moved_first[0:4] + (1.0 - first) * moved_other[0:4])


def fine_beside(v):
    rows, lanes = iota(v.shape, 0), iota(v.shape, 1)
    out = jnp.where(rows == 0, 0.0, pltpu.roll(v, 1, 0)) + jnp.where(rows == 63, 0.0, pltpu.roll(v, 63, 0))
    return out + jnp.where(lanes == 0, 0.0, pltpu.roll(v, 1, 1)) + jnp.where(lanes == 255, 0.0, pltpu.roll(v, 255, 1))


def inside(plane):
    return jnp.logical_and(plane >= 0, plane < 128).astype(F32)


def guarded(value, plane, first):
    return value if 0 <= plane < 4 else inside(first + plane) * value


def part(value):
    folded = jnp.sum(value.reshape(8, 8, 256), axis=0)
    return folded[:, :128] + folded[:, 128:]


def fine_kernel(initial, where, planes, own, up, down, *refs):
    if initial:
        (rest_far,), refs = refs[:1], refs[1:]
        rest, rest_up, rest_down = own.at[3], up, down
    else:
        (rest, rest_up, rest_down), refs = refs[:3], refs[3:]
        rest_far = rest_down.at[4:5]
    fields, packed, u, r, w, q, a = refs
    first = 4 * where[1]
    zero = (where[0] == 0).astype(F32)
    scale = (1.0 - zero, zero) if initial else (1.0, 1.0 - zero)
    above, below = (6, 9) if initial else (0, 0)
    lifted = widen(planes[...])
    pieces = [(rest_up, above + k) for k in range(4)] + [(rest, k) for k in range(4)]
    pieces = pieces + [(rest_down, below + k) for k in range(4)] + [(rest_far, 0)]
    for j, (piece, k) in enumerate(pieces):
        u[j] = scale[0] * lifted[j // 4] + scale[1] * piece[k]

    def weight(plane):
        return up[2 + plane] if plane < 0 else own[0, plane] if plane < 4 else down[plane - 4]

    def source(step, plane):
        before, after = ((5, 3), (6, 7))[step]
        return up[before + plane] if plane < 0 else own[1 + step, plane] if plane < 4 else down[after + plane - 4]

    def beside(field, low, plane):
        j = plane - low
        return field[j - 1] + field[j + 1] + fine_beside(field[j])

    def spread(field, low, plane):
        return beside(field, low, plane) - 6.0 * field[plane - low]

    for plane in range(-3, 8):
        r[plane + 3] = guarded(source(0, plane) + spread(u, -4, plane), plane, first)
    for plane in range(-2, 7):
        w[plane + 2] = guarded(weight(plane) * r[plane + 3] - beside(r, -3, plane), plane, first)
    for plane in range(-1, 6):
        q[0, plane + 1] = guarded(source(1, plane) + spread(u, -4, plane), plane, first)
        q[1, plane + 1] = guarded(spread(r, -3, plane), plane, first)
        q[2, plane + 1] = guarded(spread(w, -2, plane), plane, first)
    for plane in range(5):
        for k in range(3):
            image = weight(plane) * q[k, plane + 1] - beside(q.at[k], -1, plane)
            a[k, plane] = guarded(image, plane, first)
    sums = [jnp.zeros((8, 128), F32)] * 28
    for plane in range(4):
        terms = []
        rv, wv = r[plane + 3], w[plane + 2]
        heavy = weight(plane) + 6.0
        terms += [rv * rv, rv * wv, wv * wv]
        terms += [wv * (heavy * wv - fine_beside(wv) - 2.0 * w[plane + 3])]
        qs = [q[k, plane + 1] for k in range(3)]
        images = [a[k, plane] for k in range(3)]
        twice = []
        for k in range(3):
            value = heavy * images[k] - fine_beside(images[k]) - a[k, plane + 1]
            twice.append(value - a[k, plane - 1] if plane else value)
        for i, j in PAIRS:
            last = images[i] * twice[j]
            if plane == 3:
                last = last - a[i, 4] * images[j]
            terms += [qs[i] * qs[j], qs[i] * images[j], images[i] * images[j], last]
        sums = [s + part(v) for s, v in zip(sums, terms)]
    lane = iota((1, 128), 1)
    row = jnp.zeros((1, 128), F32)
    for k in range(28):
        row = jnp.where(lane == k, total(sums[k]), row)
    packed[...] = jnp.broadcast_to(row, packed.shape)
    fields[0] = u[4:9]
    fields[1] = r[3:8]
    fields[2] = w[2:7]
    for k in range(3):
        fields[3 + k] = q[k, 1:6]
        fields[6 + k] = a[k, 0:5]


PAIRS = ((0, 0), (0, 1), (0, 2), (1, 1), (1, 2), (2, 2))


def weights(norm, cross, square, product):
    first = cross + 6.0 * norm
    step = norm / first
    keep = 1.0 - 6.0 * step
    new = keep * keep * norm - 2.0 * keep * step * cross + step * step * square
    second = keep * keep * first - 2.0 * keep * step * (square + 6.0 * cross) + step * step * product
    ratio = new / norm
    second = new / (second - ratio * new / step)
    return step + second * (keep + ratio), -second * step


def finish_kernel(sums, fields, advanced, fine, moved, ends):
    row = jnp.sum(sums[...], axis=0, keepdims=True)
    lane = iota((1, 128), 1)
    m = [jnp.sum(jnp.where(lane == k, row, 0.0), axis=1, keepdims=True) for k in range(28)]
    a, b = weights(*m[:4])
    factor = {(0, 0): 1.0, (0, 1): 2.0 * a, (0, 2): 2.0 * b, (1, 1): a * a, (1, 2): 2.0 * (a * b), (2, 2): b * b}
    after = [sum(factor[pair] * m[4 + 4 * p + k] for p, pair in enumerate(PAIRS)) for k in range(4)]
    c, d = weights(*after)
    scales = (None, a, b, c, c * a, c * b, d, d * a, d * b)
    for i in range(5):
        value = fields[0, i]
        for k in range(1, 9):
            value = value + scales[k] * fields[k, i]
        moved[i] = value
        if i < 4:
            fine[i] = value
    own = restrict_packed(jnp.sum(moved[0:4], axis=0))
    ends[...] = jnp.broadcast_to((own - advanced[...])[None], ends.shape)


def spread_kernel(ends, rest, packed):
    for half in range(2):
        rows = ends[4 * half : 4 * half + 4].reshape(1, 32, 128)
        for k in range(half, packed.shape[0], 2):
            packed[k : k + 1] = rows


def shifted(x, axis, by, ring):
    n = lax.axis_size(axis)
    pairs = [(i, (i + by) % n) for i in range(n) if ring or 0 <= i + by < n]
    return lax.ppermute(x, axis, pairs)


def exchange(x, axis):
    return lax.all_to_all(x, axis, split_axis=0, concat_axis=0, tiled=True)


def everywhere(ends, rest, halos=()):
    (packed,) = call(spread_kernel, ((32, 32, 128),), (exchange(ends, "tm"), rest), far=(1,))
    half = exchange(packed, "space")
    half, *halos = lax.optimization_barrier((half, *halos))
    places = lax.axis_size("space")
    return half, lax.ppermute(half, "space", [(i, i ^ 1) for i in range(places)]), *halos


def body(labels, conductivity, coil_pattern, currents, initial_state):
    tm, place = lax.axis_index("tm"), lax.axis_index("space")
    where = jnp.stack([tm, place]).astype(jnp.int32)
    block, field = (4, 64, 256), (16, 16, 128)

    slices, across = lax.axis_size("tm"), lax.axis_size("space")
    pairs = [
        (b * across + slices * a + t, t * across + slices * a + b)
        for t in range(slices)
        for b in range(slices)
        for a in range(across // slices)
    ]
    theirs = lax.ppermute(currents[0], ("tm", "space"), pairs)

    own, up, down, far, packed = call(
        setup_kernel,
        ((4, *block), (10, 64, 256), (13, 64, 256), (1, 64, 256), (32, 48, 128)),
        (conductivity, currents[0], theirs, labels, coil_pattern, initial_state),
        small=(0, 1, 2),
        far=(3, 4, 5),
        scratch=(pltpu.VMEM(block, jnp.int32), (3, *block), block),
        copies=3,
        limit=60 << 20,
    )
    whole = exchange(packed, "space")
    table = whole[:8, 40, :]
    up, down = shifted(up, "space", 1, False), shifted(down, "space", -1, False)
    far = shifted(far, "space", -2, False)
    static, planes, advanced, state = call(
        first_sweep_kernel,
        ((5, *field), (64, 128), (8, 128), field),
        (where, table, whole),
        small=(0, 1),
        flops=1 << 26,
    )

    def fine(initial, planes, advanced, rest):
        fields, sums = call(
            functools.partial(fine_kernel, initial),
            ((9, 5, 64, 256), (32, 128)),
            (where, planes, own, up, down, *rest),
            small=(0,),
            scratch=((13, 64, 256), (11, 64, 256), (9, 64, 256), (3, 7, 64, 256), (3, 5, 64, 256)),
        )
        return call(
            finish_kernel,
            (block, (5, 64, 256), (8, 8, 128)),
            (exchange(sums, "space"), fields, advanced),
        )

    _, moved, ends = fine(True, planes, advanced, (far,))
    moved_first = shifted(moved, "tm", 1, True)
    around = (shifted(moved_first, "space", 1, False), shifted(moved_first, "space", -1, False))
    ours, theirs, *around = everywhere(ends, moved_first, around)
    planes, advanced, state, kept = call(
        next_sweep_kernel,
        ((64, 128), (8, 128), field, (16, 128)),
        (where, table, static, state, planes, ours, theirs),
        small=(0, 1),
        scratch=((8, *field),),
        flops=1 << 26,
    )
    fine_state, moved, ends = fine(False, planes, advanced, (moved_first, *around))
    moved_other = shifted(moved, "tm", 1, False)
    (start,) = call(
        last_sweep_kernel,
        (block,),
        (where, table, static, state, kept, moved_first, moved_other, *everywhere(ends, moved_other)),
        small=(0, 1),
        scratch=(field, (8, *field), (16, 128)),
        flops=1 << 26,
    )
    return (start[None], fine_state[None])


def solution(mesh):
    in_specs = (
        P("space", None, None),
        P(),
        P(None, "space", None, None),
        P("tm", None, None),
        P("space", None, None),
    )
    out_specs = (P("tm", "space", None, None), P("tm", "space", None, None))
    return jax.shard_map(body, mesh=mesh, in_specs=in_specs, out_specs=out_specs, check_vma=False)
```

```python
import functools

import jax
import jax.numpy as jnp
from jax import lax
from jax.experimental import pallas as pl
from jax.experimental.pallas import tpu as pltpu
from jax.sharding import PartitionSpec as P

PHASES = 3
CG_COARSE = 4
F32 = jnp.float32
HIGHEST = lax.Precision.HIGHEST
VMEM = pltpu.MemorySpace.VMEM
SMEM = pltpu.MemorySpace.SMEM
INTERPRET = False
SHIFT = 4.0
LIMIT = 12 << 20


def iota(shape, dim):
    return lax.broadcasted_iota(jnp.int32, shape, dim)


def dot(a, b):
    return lax.dot_general(a, b, (((1,), (0,)), ((), ())), precision=HIGHEST, preferred_element_type=F32)


def total(x):
    while x.ndim > 2:
        x = jnp.sum(x, axis=0)
    return jnp.sum(jnp.sum(x, axis=0, keepdims=True), axis=1, keepdims=True)


def restrict_packed(summed):
    columns = (iota((256, 128), 0) >> 2) == (iota((256, 128), 1) & 63)
    rows = (iota((16, 64), 1) >> 2) == iota((16, 64), 0)
    half = dot(summed, jnp.where(columns, 1.0 / 64.0, 0.0).astype(F32))
    both = dot(jnp.where(rows, 1.0, 0.0).astype(F32), half)
    return jnp.where(iota((8, 128), 1) < 64, both[:8], both[8:])


def widen(planes):
    columns = (iota((128, 256), 1) >> 2) == iota((128, 256), 0)
    rows = (iota((64, 16), 0) >> 2) == iota((64, 16), 1)
    wide = dot(planes, jnp.where(columns, 1.0, 0.0).astype(F32))
    lift = jnp.where(rows, 1.0, 0.0).astype(F32)
    return [dot(lift, wide[k : k + 16]) for k in range(0, planes.shape[0], 16)]


def unpack(low, high):
    axis = low.ndim - 1
    left = iota(low.shape, axis) < 64
    top = jnp.where(left, low, pltpu.roll(high, 64, axis))
    bottom = jnp.where(left, pltpu.roll(low, 64, axis), high)
    return jnp.concatenate([top, bottom], axis=axis - 1)


def coarse_beside(v):
    one = (1, 16, 128)
    lane, row = iota(one, 2), iota(one, 1)
    left = lane < 64
    first, last = pltpu.roll(v[:1], 64, 2), pltpu.roll(v[15:], 64, 2)
    after = jnp.concatenate([v[1:], jnp.where(left, first, 0.0)], axis=0)
    before = jnp.concatenate([jnp.where(left, 0.0, last), v[:15]], axis=0)
    out = after + before
    out = out + jnp.where(row == 0, 0.0, pltpu.roll(v, 1, 1)) + jnp.where(row == 15, 0.0, pltpu.roll(v, 15, 1))
    inner = lane & 63
    return out + jnp.where(inner == 0, 0.0, pltpu.roll(v, 1, 2)) + jnp.where(inner == 63, 0.0, pltpu.roll(v, 127, 2))


def coarse_solve(start, source, diagonal):
    def apply(v):
        return diagonal * v - 0.0625 * coarse_beside(v)

    x = start
    residual = source - 0.375 * start + 0.0625 * coarse_beside(start)
    image = apply(residual)
    norm, product = total(residual * residual), total(residual * image)
    step = norm / product
    direction, moved = residual, image
    for turn in range(CG_COARSE):
        inverse = 1.0 / norm
        scaled = inverse / step
        x = x + step[None] * direction
        if turn + 1 < CG_COARSE:
            residual = residual - step[None] * moved
            image = apply(residual)
            new, product = total(residual * residual), total(residual * image)
            ratio = new * inverse
            step = new / (product - new * (new * scaled))
            direction = residual + ratio[None] * direction
            moved = image + ratio[None] * moved
            norm = new
    return x


def cut_planes(state, place, offsets):
    out = []
    lane = iota((16, 128), 1)
    for offset in offsets:
        at = place + offset
        inside = jnp.logical_and(at >= 0, at < 32).astype(jnp.int32)
        at = jnp.clip(at, 0, 31)
        plane = state[at & 15]
        plane = jnp.where((at >> 4) * jnp.ones_like(lane) == 1, pltpu.roll(plane, 64, 1), plane)
        out.append(jnp.where(lane < 64 * inside, plane, 0.0))
    return out


def call(body, outs, args, small=(), far=(), scratch=(), flops=0, copies=0, limit=LIMIT):
    spaces = [SMEM if k in small else pltpu.MemorySpace.HBM if k in far else VMEM for k in range(len(args))]
    specs = [pl.BlockSpec(memory_space=space) for space in spaces]
    return pl.pallas_call(
        body,
        out_shape=tuple(jax.ShapeDtypeStruct(s, F32) for s in outs),
        in_specs=specs,
        out_specs=tuple(pl.BlockSpec(memory_space=VMEM) for _ in outs),
        scratch_shapes=(
            *(pltpu.VMEM(s, F32) if isinstance(s, tuple) else s for s in scratch),
            *(pltpu.SemaphoreType.DMA for _ in range(copies)),
        ),
        cost_estimate=pl.CostEstimate(flops=flops, bytes_accessed=1 << 20, transcendentals=0) if flops else None,
        compiler_params=pltpu.CompilerParams(vmem_limit_bytes=limit),
        interpret=INTERPRET,
    )(*args)


def setup_kernel(cond, cur, theirs, labels_far, coils_far, initial_far, own, up, down, far, packed,
                 labels, coils, initial, labels_sem, coils_sem, initial_sem):
    copies = [
        pltpu.make_async_copy(labels_far, labels, labels_sem),
        pltpu.make_async_copy(coils_far, coils, coils_sem),
        pltpu.make_async_copy(initial_far, initial, initial_sem),
    ]
    for copy in copies:
        copy.start()
    for copy in copies:
        copy.wait()
    region = labels[...]
    cell = jnp.where(region == 0, cond[0], 0.0)
    for k in range(1, 4):
        cell = cell + jnp.where(region == k, cond[k], 0.0)
    own[0] = cell
    own[3] = initial[...]
    pattern = [coils[p] for p in range(PHASES)]
    for step in range(2):
        source = cur[step, 0] * pattern[0]
        for p in range(1, PHASES):
            source = source + cur[step, p] * pattern[p]
        own[1 + step] = source
    up[0:2] = own[0, 2:4]
    up[2:5] = own[1, 1:4]
    up[5:6] = own[2, 3:4]
    down[0:3] = own[0, 0:3]
    down[3:7] = own[1]
    down[7:9] = own[2, 0:2]
    up[6:10] = initial[...]
    down[9:13] = initial[...]
    far[...] = initial[0:1]
    fields = [initial[...], cell, *pattern]
    rows = [restrict_packed(jnp.sum(f, axis=0)) for f in fields]
    lane = iota((8, 128), 1)
    row = jnp.zeros((8, 128), F32)
    for k in range(6):
        row = jnp.where(lane == k, theirs[k // 3, k % 3], row)
    rows = jnp.concatenate([*rows, row], axis=0)
    packed[...] = jnp.broadcast_to(rows[None], packed.shape)


def unpack_all(whole, at):
    return unpack(whole[0:16, at : at + 8, :], whole[16:32, at : at + 8, :])


def slice_source(cur, static, n):
    source = jnp.zeros((16, 16, 128), F32)
    for p in range(PHASES):
        source = source + 0.5 * (cur[n, p] + cur[n, PHASES + p]) * static[2 + p]
    return source


def solve_slice(cur, state, static, n):
    state[...] = coarse_solve(state[...], slice_source(cur, static, n), 0.5 * static[1] + 0.375)


AROUND = (-1, 0, 1, 2)


def first_sweep_kernel(where, cur, whole, static, planes, advanced, state):
    mine, place = where[0], where[1]
    for k in range(5):
        static[k] = unpack_all(whole, 8 * k)
    state[...] = static[0]

    def turn(n, carry):
        @pl.when(n == mine)
        def _():
            for k, plane in enumerate(cut_planes(state, place, AROUND)):
                planes[16 * k : 16 * k + 16] = plane

        solve_slice(cur, state, static, n)

        @pl.when(n == mine)
        def _():
            advanced[...] = pack(*cut_planes(state, place, (0,)))

        return carry

    lax.fori_loop(0, 8, turn, 0)


def pack(plane):
    return plane[:8] + pltpu.roll(plane[8:], 64, 1)


def load_corrections(where, ours, theirs, correction):
    odd = where[1] & 1
    for k in range(4):
        correction[4 * odd + k] = unpack_all(ours, 8 * k)
        correction[4 * (1 - odd) + k] = unpack_all(theirs, 8 * k)


def next_sweep_kernel(where, cur, static, begin, old, ours, theirs, planes, advanced, state, kept, correction):
    mine, place = where[0], where[1]
    load_corrections(where, ours, theirs, correction)
    state[...] = begin[...]

    @pl.when(mine == 0)
    def _():
        for k, plane in enumerate(cut_planes(state, place, AROUND)):
            planes[16 * k : 16 * k + 16] = plane

    def turn(n, carry):
        solve_slice(cur, state, static, n)

        @pl.when(n == mine)
        def _():
            advanced[...] = pack(*cut_planes(state, place, (0,)))

        @pl.when(n == mine - 1)
        def _():
            around = cut_planes(state, place, AROUND)
            kept[...] = around[1]
            for k, plane in enumerate(around):
                planes[16 * k : 16 * k + 16] = plane - old[16 * k : 16 * k + 16]

        @pl.when(jnp.logical_and(n == 7, mine == 0))
        def _():
            (new,), (before,) = cut_planes(state, place, (0,)), cut_planes(begin, place, (0,))
            kept[...] = new - before

        state[...] = state[...] + correction[n]
        return carry

    lax.fori_loop(0, 8, turn, 0)


def last_sweep_kernel(where, cur, static, begin, kept, moved_first, moved_other, ours, theirs,
                      start, state, correction, plane):
    mine, place = where[0], where[1]
    load_corrections(where, ours, theirs, correction)
    state[...] = begin[...]
    plane[...] = kept[...]

    def turn(n, carry):
        solve_slice(cur, state, static, n)

        @pl.when(n == mine - 1)
        def _():
            (new,) = cut_planes(state, place, (0,))
            plane[...] = new - kept[...]

        state[...] = state[...] + correction[n]
        return carry

    lax.fori_loop(0, mine, turn, 0)
    (own,) = widen(plane[...])
    first = (mine == 0).astype(F32)
    start[...] = own[None] + (first * moved_first[0:4] + (1.0 - first) * moved_other[0:4])


def fine_beside(v):
    rows, lanes = iota(v.shape, 0), iota(v.shape, 1)
    out = jnp.where(rows == 0, 0.0, pltpu.roll(v, 1, 0)) + jnp.where(rows == 63, 0.0, pltpu.roll(v, 63, 0))
    return out + jnp.where(lanes == 0, 0.0, pltpu.roll(v, 1, 1)) + jnp.where(lanes == 255, 0.0, pltpu.roll(v, 255, 1))


def inside(plane):
    return jnp.logical_and(plane >= 0, plane < 128).astype(F32)


def guarded(value, plane, first):
    return value if 0 <= plane < 4 else inside(first + plane) * value


def part(value):
    folded = jnp.sum(value.reshape(8, 8, 256), axis=0)
    return folded[:, :128] + folded[:, 128:]


def fine_kernel(initial, where, planes, own, up, down, *refs):
    if initial:
        (rest_far,), refs = refs[:1], refs[1:]
        rest, rest_up, rest_down = own.at[3], up, down
    else:
        (rest, rest_up, rest_down), refs = refs[:3], refs[3:]
        rest_far = rest_down.at[4:5]
    fields, packed, u, r, w, q, a = refs
    first = 4 * where[1]
    zero = (where[0] == 0).astype(F32)
    scale = (1.0 - zero, zero) if initial else (1.0, 1.0 - zero)
    above, below = (6, 9) if initial else (0, 0)
    lifted = widen(planes[...])
    pieces = [(rest_up, above + k) for k in range(4)] + [(rest, k) for k in range(4)]
    pieces = pieces + [(rest_down, below + k) for k in range(4)] + [(rest_far, 0)]
    for j, (piece, k) in enumerate(pieces):
        u[j] = scale[0] * lifted[j // 4] + scale[1] * piece[k]

    def weight(plane):
        return up[2 + plane] if plane < 0 else own[0, plane] if plane < 4 else down[plane - 4]

    def source(step, plane):
        before, after = ((5, 3), (6, 7))[step]
        return up[before + plane] if plane < 0 else own[1 + step, plane] if plane < 4 else down[after + plane - 4]

    def beside(field, low, plane):
        j = plane - low
        return field[j - 1] + field[j + 1] + fine_beside(field[j])

    def spread(field, low, plane):
        return beside(field, low, plane) - 6.0 * field[plane - low]

    for plane in range(-3, 8):
        r[plane + 3] = guarded(source(0, plane) + spread(u, -4, plane), plane, first)
    for plane in range(-2, 7):
        w[plane + 2] = guarded((weight(plane) + (6.0 - SHIFT)) * r[plane + 3] - beside(r, -3, plane), plane, first)
    for plane in range(-1, 6):
        q[0, plane + 1] = guarded(source(1, plane) + spread(u, -4, plane), plane, first)
        q[1, plane + 1] = guarded(spread(r, -3, plane), plane, first)
        q[2, plane + 1] = guarded(spread(w, -2, plane), plane, first)
    for plane in range(5):
        for k in range(3):
            image = (weight(plane) + (6.0 - SHIFT)) * q[k, plane + 1] - beside(q.at[k], -1, plane)
            a[k, plane] = guarded(image, plane, first)
    sums = [jnp.zeros((8, 128), F32)] * 28
    for plane in range(4):
        terms = []
        rv, wv = r[plane + 3], w[plane + 2]
        heavy = weight(plane) + 6.0
        terms += [rv * rv, rv * wv, wv * wv]
        terms += [wv * (heavy * wv - fine_beside(wv) - 2.0 * w[plane + 3])]
        qs = [q[k, plane + 1] for k in range(3)]
        images = [a[k, plane] for k in range(3)]
        twice = []
        for k in range(3):
            value = heavy * images[k] - fine_beside(images[k]) - a[k, plane + 1]
            twice.append(value - a[k, plane - 1] if plane else value)
        for i, j in PAIRS:
            last = images[i] * twice[j]
            if plane == 3:
                last = last - a[i, 4] * images[j]
            terms += [qs[i] * qs[j], qs[i] * images[j], images[i] * images[j], last]
        sums = [s + part(v) for s, v in zip(sums, terms)]
    lane = iota((1, 128), 1)
    row = jnp.zeros((1, 128), F32)
    for k in range(28):
        row = jnp.where(lane == k, total(sums[k]), row)
    packed[...] = jnp.broadcast_to(row, packed.shape)
    fields[0] = u[4:9]
    fields[1] = r[3:8]
    fields[2] = w[2:7]
    for k in range(3):
        fields[3 + k] = q[k, 1:6]
        fields[6 + k] = a[k, 0:5]


PAIRS = ((0, 0), (0, 1), (0, 2), (1, 1), (1, 2), (2, 2))


def weights(norm, cross, square, product):
    first = cross + SHIFT * norm
    step = norm / first
    keep = 1.0 - SHIFT * step
    new = keep * keep * norm - 2.0 * keep * step * cross + step * step * square
    second = keep * keep * first - 2.0 * keep * step * (square + SHIFT * cross) + step * step * product
    ratio = new / norm
    second = new / (second - ratio * new / step)
    return step + second * (keep + ratio), -second * step


def finish_kernel(sums, fields, advanced, fine, moved, ends):
    row = jnp.sum(sums[...], axis=0, keepdims=True)
    lane = iota((1, 128), 1)
    m = [jnp.sum(jnp.where(lane == k, row, 0.0), axis=1, keepdims=True) for k in range(28)]
    a, b = weights(*m[:4])
    factor = {(0, 0): 1.0, (0, 1): 2.0 * a, (0, 2): 2.0 * b, (1, 1): a * a, (1, 2): 2.0 * (a * b), (2, 2): b * b}
    after = [sum(factor[pair] * m[4 + 4 * p + k] for p, pair in enumerate(PAIRS)) for k in range(4)]
    c, d = weights(*after)
    scales = (None, a, b, c, c * a, c * b, d, d * a, d * b)
    for i in range(5):
        value = fields[0, i]
        for k in range(1, 9):
            value = value + scales[k] * fields[k, i]
        moved[i] = value
        if i < 4:
            fine[i] = value
    own = restrict_packed(jnp.sum(moved[0:4], axis=0))
    ends[...] = jnp.broadcast_to((own - advanced[...])[None], ends.shape)


def spread_kernel(ends, rest, packed):
    for half in range(2):
        rows = ends[4 * half : 4 * half + 4].reshape(1, 32, 128)
        for k in range(half, packed.shape[0], 2):
            packed[k : k + 1] = rows


def shifted(x, axis, by, ring):
    n = lax.axis_size(axis)
    pairs = [(i, (i + by) % n) for i in range(n) if ring or 0 <= i + by < n]
    return lax.ppermute(x, axis, pairs)


def exchange(x, axis):
    return lax.all_to_all(x, axis, split_axis=0, concat_axis=0, tiled=True)


def everywhere(ends, rest):
    (packed,) = call(spread_kernel, ((32, 32, 128),), (exchange(ends, "tm"), rest), far=(1,))
    half = exchange(packed, "space")
    places = lax.axis_size("space")
    return half, lax.ppermute(half, "space", [(i, i ^ 1) for i in range(places)])


def body(labels, conductivity, coil_pattern, currents, initial_state):
    tm, place = lax.axis_index("tm"), lax.axis_index("space")
    where = jnp.stack([tm, place]).astype(jnp.int32)
    block, field = (4, 64, 256), (16, 16, 128)

    slices, across = lax.axis_size("tm"), lax.axis_size("space")
    pairs = [
        (b * across + slices * a + t, t * across + slices * a + b)
        for t in range(slices)
        for b in range(slices)
        for a in range(across // slices)
    ]
    theirs = lax.ppermute(currents[0], ("tm", "space"), pairs)

    own, up, down, far, packed = call(
        setup_kernel,
        ((4, *block), (10, 64, 256), (13, 64, 256), (1, 64, 256), (32, 48, 128)),
        (conductivity, currents[0], theirs, labels, coil_pattern, initial_state),
        small=(0, 1, 2),
        far=(3, 4, 5),
        scratch=(pltpu.VMEM(block, jnp.int32), (3, *block), block),
        copies=3,
        limit=60 << 20,
    )
    whole = exchange(packed, "space")
    table = whole[:8, 40, :]
    up, down = shifted(up, "space", 1, False), shifted(down, "space", -1, False)
    far = shifted(far, "space", -2, False)
    static, planes, advanced, state = call(
        first_sweep_kernel,
        ((5, *field), (64, 128), (8, 128), field),
        (where, table, whole),
        small=(0, 1),
        flops=1 << 26,
    )

    def fine(initial, planes, advanced, rest):
        fields, sums = call(
            functools.partial(fine_kernel, initial),
            ((9, 5, 64, 256), (32, 128)),
            (where, planes, own, up, down, *rest),
            small=(0,),
            scratch=((13, 64, 256), (11, 64, 256), (9, 64, 256), (3, 7, 64, 256), (3, 5, 64, 256)),
        )
        return call(
            finish_kernel,
            (block, (5, 64, 256), (8, 8, 128)),
            (exchange(sums, "space"), fields, advanced),
        )

    _, moved, ends = fine(True, planes, advanced, (far,))
    moved_first = shifted(moved, "tm", 1, True)
    planes, advanced, state, kept = call(
        next_sweep_kernel,
        ((64, 128), (8, 128), field, (16, 128)),
        (where, table, static, state, planes, *everywhere(ends, moved_first)),
        small=(0, 1),
        scratch=((8, *field),),
        flops=1 << 26,
    )
    around = (shifted(moved_first, "space", 1, False), shifted(moved_first, "space", -1, False))
    fine_state, moved, ends = fine(False, planes, advanced, (moved_first, *around))
    moved_other = shifted(moved, "tm", 1, False)
    (start,) = call(
        last_sweep_kernel,
        (block,),
        (where, table, static, state, kept, moved_first, moved_other, *everywhere(ends, moved_other)),
        small=(0, 1),
        scratch=(field, (8, *field), (16, 128)),
        flops=1 << 26,
    )
    return (start[None], fine_state[None])


def solution(mesh):
    in_specs = (
        P("space", None, None),
        P(),
        P(None, "space", None, None),
        P("tm", None, None),
        P("space", None, None),
    )
    out_specs = (P("tm", "space", None, None), P("tm", "space", None, None))
    return jax.shard_map(body, mesh=mesh, in_specs=in_specs, out_specs=out_specs, check_vma=False)
```

```python
import functools

import jax
import jax.numpy as jnp
from jax import lax
from jax.experimental import pallas as pl
from jax.experimental.pallas import tpu as pltpu
from jax.sharding import PartitionSpec as P

PHASES = 3
CG_COARSE = 4
F32 = jnp.float32
HIGHEST = lax.Precision.HIGHEST
VMEM = pltpu.MemorySpace.VMEM
SMEM = pltpu.MemorySpace.SMEM
INTERPRET = False
SHIFT = 4.0
LIMIT = 12 << 20


def iota(shape, dim):
    return lax.broadcasted_iota(jnp.int32, shape, dim)


def dot(a, b):
    return lax.dot_general(a, b, (((1,), (0,)), ((), ())), precision=HIGHEST, preferred_element_type=F32)


def total(x):
    while x.ndim > 2:
        x = jnp.sum(x, axis=0)
    return jnp.sum(jnp.sum(x, axis=0, keepdims=True), axis=1, keepdims=True)


def restrict_packed(summed):
    columns = (iota((256, 128), 0) >> 2) == (iota((256, 128), 1) & 63)
    rows = (iota((16, 64), 1) >> 2) == iota((16, 64), 0)
    half = dot(summed, jnp.where(columns, 1.0 / 64.0, 0.0).astype(F32))
    both = dot(jnp.where(rows, 1.0, 0.0).astype(F32), half)
    return jnp.where(iota((8, 128), 1) < 64, both[:8], both[8:])


def widen(planes):
    columns = (iota((128, 256), 1) >> 2) == iota((128, 256), 0)
    rows = (iota((64, 16), 0) >> 2) == iota((64, 16), 1)
    wide = dot(planes, jnp.where(columns, 1.0, 0.0).astype(F32))
    lift = jnp.where(rows, 1.0, 0.0).astype(F32)
    return [dot(lift, wide[k : k + 16]) for k in range(0, planes.shape[0], 16)]


def unpack(low, high):
    axis = low.ndim - 1
    left = iota(low.shape, axis) < 64
    top = jnp.where(left, low, pltpu.roll(high, 64, axis))
    bottom = jnp.where(left, pltpu.roll(low, 64, axis), high)
    return jnp.concatenate([top, bottom], axis=axis - 1)


def coarse_beside(v):
    one = (1, 16, 128)
    lane, row = iota(one, 2), iota((1, 8, 128), 1)
    left = lane < 64
    first, last = pltpu.roll(v[:1], 64, 2), pltpu.roll(v[15:], 64, 2)
    after = jnp.concatenate([v[1:], jnp.where(left, first, 0.0)], axis=0)
    before = jnp.concatenate([jnp.where(left, 0.0, last), v[:15]], axis=0)
    out = after + before
    up, down = pltpu.roll(v, 1, 1), pltpu.roll(v, 15, 1)
    up = jnp.concatenate([jnp.where(row == 0, 0.0, up[:, :8]), up[:, 8:]], axis=1)
    down = jnp.concatenate([down[:, :8], jnp.where(row == 7, 0.0, down[:, 8:])], axis=1)
    out = out + (up + down)
    inner = lane & 63
    return out + jnp.where(inner == 0, 0.0, pltpu.roll(v, 1, 2)) + jnp.where(inner == 63, 0.0, pltpu.roll(v, 127, 2))


def coarse_solve(start, source, diagonal):
    def apply(v):
        return diagonal * v - 0.0625 * coarse_beside(v)

    x = start
    residual = source - 0.375 * start + 0.0625 * coarse_beside(start)
    image = apply(residual)
    norm, product = total(residual * residual), total(residual * image)
    step = norm / product
    direction, moved = residual, image
    for turn in range(CG_COARSE):
        inverse = 1.0 / norm
        scaled = inverse / step
        x = x + step[None] * direction
        if turn + 1 < CG_COARSE:
            residual = residual - step[None] * moved
            image = apply(residual)
            new, product = total(residual * residual), total(residual * image)
            ratio = new * inverse
            step = new / (product - new * (new * scaled))
            direction = residual + ratio[None] * direction
            moved = image + ratio[None] * moved
            norm = new
    return x


def cut_planes(state, place, offsets):
    out = []
    lane = iota((16, 128), 1)
    for offset in offsets:
        at = place + offset
        inside = jnp.logical_and(at >= 0, at < 32).astype(jnp.int32)
        at = jnp.clip(at, 0, 31)
        plane = state[at & 15]
        plane = jnp.where((at >> 4) * jnp.ones_like(lane) == 1, pltpu.roll(plane, 64, 1), plane)
        out.append(jnp.where(lane < 64 * inside, plane, 0.0))
    return out


def call(body, outs, args, small=(), far=(), scratch=(), flops=0, copies=0, limit=LIMIT):
    spaces = [SMEM if k in small else pltpu.MemorySpace.HBM if k in far else VMEM for k in range(len(args))]
    specs = [pl.BlockSpec(memory_space=space) for space in spaces]
    return pl.pallas_call(
        body,
        out_shape=tuple(jax.ShapeDtypeStruct(s, F32) for s in outs),
        in_specs=specs,
        out_specs=tuple(pl.BlockSpec(memory_space=VMEM) for _ in outs),
        scratch_shapes=(
            *(pltpu.VMEM(s, F32) if isinstance(s, tuple) else s for s in scratch),
            *(pltpu.SemaphoreType.DMA for _ in range(copies)),
        ),
        cost_estimate=pl.CostEstimate(flops=flops, bytes_accessed=1 << 20, transcendentals=0) if flops else None,
        compiler_params=pltpu.CompilerParams(vmem_limit_bytes=limit),
        interpret=INTERPRET,
    )(*args)


def setup_kernel(cond, cur, theirs, labels_far, coils_far, initial_far, own, up, down, far, packed,
                 labels, coils, initial, labels_sem, coils_sem, initial_sem):
    copies = [
        pltpu.make_async_copy(labels_far, labels, labels_sem),
        pltpu.make_async_copy(coils_far, coils, coils_sem),
        pltpu.make_async_copy(initial_far, initial, initial_sem),
    ]
    for copy in copies:
        copy.start()
    for copy in copies:
        copy.wait()
    region = labels[...]
    cell = jnp.where(region == 0, cond[0], 0.0)
    for k in range(1, 4):
        cell = cell + jnp.where(region == k, cond[k], 0.0)
    own[0] = cell
    own[3] = initial[...]
    pattern = [coils[p] for p in range(PHASES)]
    for step in range(2):
        source = cur[step, 0] * pattern[0]
        for p in range(1, PHASES):
            source = source + cur[step, p] * pattern[p]
        own[1 + step] = source
    up[0:2] = own[0, 2:4]
    up[2:5] = own[1, 1:4]
    up[5:6] = own[2, 3:4]
    down[0:3] = own[0, 0:3]
    down[3:7] = own[1]
    down[7:9] = own[2, 0:2]
    up[6:10] = initial[...]
    down[9:13] = initial[...]
    far[...] = initial[0:1]
    fields = [initial[...], cell, *pattern]
    rows = [restrict_packed(jnp.sum(f, axis=0)) for f in fields]
    lane = iota((8, 128), 1)
    row = jnp.zeros((8, 128), F32)
    for k in range(6):
        row = jnp.where(lane == k, theirs[k // 3, k % 3], row)
    rows = jnp.concatenate([*rows, row], axis=0)
    packed[...] = jnp.broadcast_to(rows[None], packed.shape)


def unpack_all(whole, at):
    return unpack(whole[0:16, at : at + 8, :], whole[16:32, at : at + 8, :])


def slice_source(cur, static, n):
    source = jnp.zeros((16, 16, 128), F32)
    for p in range(PHASES):
        source = source + 0.5 * (cur[n, p] + cur[n, PHASES + p]) * static[2 + p]
    return source


def solve_slice(cur, state, static, n):
    state[...] = coarse_solve(state[...], slice_source(cur, static, n), 0.5 * static[1] + 0.375)


AROUND = (-1, 0, 1, 2)


def first_sweep_kernel(where, cur, whole, static, planes, advanced, state):
    mine, place = where[0], where[1]
    for k in range(5):
        static[k] = unpack_all(whole, 8 * k)
    state[...] = static[0]

    def turn(n, carry):
        @pl.when(n == mine)
        def _():
            for k, plane in enumerate(cut_planes(state, place, AROUND)):
                planes[16 * k : 16 * k + 16] = plane

        solve_slice(cur, state, static, n)

        @pl.when(n == mine)
        def _():
            advanced[...] = pack(*cut_planes(state, place, (0,)))

        return carry

    lax.fori_loop(0, 8, turn, 0)


def pack(plane):
    return plane[:8] + pltpu.roll(plane[8:], 64, 1)


def load_corrections(where, ours, theirs, correction):
    odd = where[1] & 1
    for k in range(4):
        correction[4 * odd + k] = unpack_all(ours, 8 * k)
        correction[4 * (1 - odd) + k] = unpack_all(theirs, 8 * k)


def next_sweep_kernel(where, cur, static, begin, old, ours, theirs, planes, advanced, state, kept, correction):
    mine, place = where[0], where[1]
    load_corrections(where, ours, theirs, correction)
    state[...] = begin[...]

    @pl.when(mine == 0)
    def _():
        for k, plane in enumerate(cut_planes(state, place, AROUND)):
            planes[16 * k : 16 * k + 16] = plane

    def turn(n, carry):
        solve_slice(cur, state, static, n)

        @pl.when(n == mine)
        def _():
            advanced[...] = pack(*cut_planes(state, place, (0,)))

        @pl.when(n == mine - 1)
        def _():
            around = cut_planes(state, place, AROUND)
            kept[...] = around[1]
            for k, plane in enumerate(around):
                planes[16 * k : 16 * k + 16] = plane - old[16 * k : 16 * k + 16]

        @pl.when(jnp.logical_and(n == 7, mine == 0))
        def _():
            (new,), (before,) = cut_planes(state, place, (0,)), cut_planes(begin, place, (0,))
            kept[...] = new - before

        state[...] = state[...] + correction[n]
        return carry

    lax.fori_loop(0, 8, turn, 0)


def last_sweep_kernel(where, cur, static, begin, kept, moved_first, moved_other, ours, theirs,
                      start, state, correction, plane):
    mine, place = where[0], where[1]
    load_corrections(where, ours, theirs, correction)
    state[...] = begin[...]
    plane[...] = kept[...]

    def turn(n, carry):
        solve_slice(cur, state, static, n)

        @pl.when(n == mine - 1)
        def _():
            (new,) = cut_planes(state, place, (0,))
            plane[...] = new - kept[...]

        state[...] = state[...] + correction[n]
        return carry

    lax.fori_loop(0, mine, turn, 0)
    (own,) = widen(plane[...])
    first = (mine == 0).astype(F32)
    start[...] = own[None] + (first * moved_first[0:4] + (1.0 - first) * moved_other[0:4])


def fine_beside(v):
    head, tail = iota((8, 256), 0), iota((64, 128), 1)
    before, after = pltpu.roll(v, 1, 0), pltpu.roll(v, 63, 0)
    before = jnp.concatenate([jnp.where(head == 0, 0.0, before[:8]), before[8:]], axis=0)
    after = jnp.concatenate([after[:56], jnp.where(head == 7, 0.0, after[56:])], axis=0)
    left, right = pltpu.roll(v, 1, 1), pltpu.roll(v, 255, 1)
    left = jnp.concatenate([jnp.where(tail == 0, 0.0, left[:, :128]), left[:, 128:]], axis=1)
    right = jnp.concatenate([right[:, :128], jnp.where(tail == 127, 0.0, right[:, 128:])], axis=1)
    return (before + after) + (left + right)


def inside(plane):
    return jnp.logical_and(plane >= 0, plane < 128).astype(F32)


def guarded(value, plane, first):
    return value if 0 <= plane < 4 else inside(first + plane) * value


def part(value):
    folded = jnp.sum(value.reshape(8, 8, 256), axis=0)
    return folded[:, :128] + folded[:, 128:]


def fine_kernel(initial, where, planes, own, up, down, *refs):
    if initial:
        (rest_far,), refs = refs[:1], refs[1:]
        rest, rest_up, rest_down = own.at[3], up, down
    else:
        (rest, rest_up, rest_down), refs = refs[:3], refs[3:]
        rest_far = rest_down.at[4:5]
    fields, packed, u, r, w, q, a = refs
    first = 4 * where[1]
    zero = (where[0] == 0).astype(F32)
    scale = (1.0 - zero, zero) if initial else (1.0, 1.0 - zero)
    above, below = (6, 9) if initial else (0, 0)
    lifted = widen(planes[...])
    pieces = [(rest_up, above + k) for k in range(4)] + [(rest, k) for k in range(4)]
    pieces = pieces + [(rest_down, below + k) for k in range(4)] + [(rest_far, 0)]
    for j, (piece, k) in enumerate(pieces):
        u[j] = scale[0] * lifted[j // 4] + scale[1] * piece[k]

    def weight(plane):
        return up[2 + plane] if plane < 0 else own[0, plane] if plane < 4 else down[plane - 4]

    def source(step, plane):
        before, after = ((5, 3), (6, 7))[step]
        return up[before + plane] if plane < 0 else own[1 + step, plane] if plane < 4 else down[after + plane - 4]

    def beside(field, low, plane):
        j = plane - low
        return field[j - 1] + field[j + 1] + fine_beside(field[j])

    def spread(field, low, plane):
        return beside(field, low, plane) - 6.0 * field[plane - low]

    for plane in range(-3, 8):
        lap = spread(u, -4, plane)
        r[plane + 3] = guarded(source(0, plane) + lap, plane, first)
        if -1 <= plane < 6:
            q[0, plane + 1] = guarded(source(1, plane) + lap, plane, first)
    for plane in range(-2, 7):
        v, around = r[plane + 3], beside(r, -3, plane)
        w[plane + 2] = guarded((weight(plane) + (6.0 - SHIFT)) * v - around, plane, first)
        if -1 <= plane < 6:
            q[1, plane + 1] = guarded(around - 6.0 * v, plane, first)
    for plane in range(-1, 6):
        q[2, plane + 1] = guarded(spread(w, -2, plane), plane, first)
    for plane in range(5):
        for k in range(3):
            image = (weight(plane) + (6.0 - SHIFT)) * q[k, plane + 1] - beside(q.at[k], -1, plane)
            a[k, plane] = guarded(image, plane, first)
    sums = [jnp.zeros((8, 128), F32)] * 28
    for plane in range(4):
        terms = []
        rv, wv = r[plane + 3], w[plane + 2]
        heavy = weight(plane) + 6.0
        terms += [rv * rv, rv * wv, wv * wv]
        terms += [wv * (weight(plane) * wv - q[2, plane + 1] + w[plane + 1] - w[plane + 3])]
        qs = [q[k, plane + 1] for k in range(3)]
        images = [a[k, plane] for k in range(3)]
        twice = []
        for k in range(3):
            value = heavy * images[k] - fine_beside(images[k]) - a[k, plane + 1]
            twice.append(value - a[k, plane - 1] if plane else value)
        for i, j in PAIRS:
            last = images[i] * twice[j]
            if plane == 3:
                last = last - a[i, 4] * images[j]
            terms += [qs[i] * qs[j], qs[i] * images[j], images[i] * images[j], last]
        sums = [s + part(v) for s, v in zip(sums, terms)]
    lane = iota((1, 128), 1)
    row = jnp.zeros((1, 128), F32)
    for k in range(28):
        row = jnp.where(lane == k, total(sums[k]), row)
    packed[...] = jnp.broadcast_to(row, packed.shape)
    fields[0] = u[4:9]
    fields[1] = r[3:8]
    fields[2] = w[2:7]
    for k in range(3):
        fields[3 + k] = q[k, 1:6]
        fields[6 + k] = a[k, 0:5]


PAIRS = ((0, 0), (0, 1), (0, 2), (1, 1), (1, 2), (2, 2))


def weights(norm, cross, square, product):
    first = cross + SHIFT * norm
    step = norm / first
    keep = 1.0 - SHIFT * step
    new = keep * keep * norm - 2.0 * keep * step * cross + step * step * square
    second = keep * keep * first - 2.0 * keep * step * (square + SHIFT * cross) + step * step * product
    ratio = new / norm
    second = new / (second - ratio * new / step)
    return step + second * (keep + ratio), -second * step


def finish_kernel(sums, fields, advanced, fine, moved, ends):
    row = jnp.sum(sums[...], axis=0, keepdims=True)
    lane = iota((1, 128), 1)
    m = [jnp.sum(jnp.where(lane == k, row, 0.0), axis=1, keepdims=True) for k in range(28)]
    a, b = weights(*m[:4])
    factor = {(0, 0): 1.0, (0, 1): 2.0 * a, (0, 2): 2.0 * b, (1, 1): a * a, (1, 2): 2.0 * (a * b), (2, 2): b * b}
    after = [sum(factor[pair] * m[4 + 4 * p + k] for p, pair in enumerate(PAIRS)) for k in range(4)]
    c, d = weights(*after)
    scales = (None, a, b, c, c * a, c * b, d, d * a, d * b)
    for i in range(5):
        value = fields[0, i]
        for k in range(1, 9):
            value = value + scales[k] * fields[k, i]
        moved[i] = value
        if i < 4:
            fine[i] = value
    own = restrict_packed(jnp.sum(moved[0:4], axis=0))
    ends[...] = jnp.broadcast_to((own - advanced[...])[None], ends.shape)


def spread_kernel(ends, rest, packed):
    for half in range(2):
        rows = ends[4 * half : 4 * half + 4].reshape(1, 32, 128)
        for k in range(half, packed.shape[0], 2):
            packed[k : k + 1] = rows


def shifted(x, axis, by, ring):
    n = lax.axis_size(axis)
    pairs = [(i, (i + by) % n) for i in range(n) if ring or 0 <= i + by < n]
    return lax.ppermute(x, axis, pairs)


def exchange(x, axis):
    return lax.all_to_all(x, axis, split_axis=0, concat_axis=0, tiled=True)


def everywhere(ends, rest):
    (packed,) = call(spread_kernel, ((32, 32, 128),), (exchange(ends, "tm"), rest), far=(1,))
    half = exchange(packed, "space")
    places = lax.axis_size("space")
    return half, lax.ppermute(half, "space", [(i, i ^ 1) for i in range(places)])


def body(labels, conductivity, coil_pattern, currents, initial_state):
    tm, place = lax.axis_index("tm"), lax.axis_index("space")
    where = jnp.stack([tm, place]).astype(jnp.int32)
    block, field = (4, 64, 256), (16, 16, 128)

    slices, across = lax.axis_size("tm"), lax.axis_size("space")
    pairs = [
        (b * across + slices * a + t, t * across + slices * a + b)
        for t in range(slices)
        for b in range(slices)
        for a in range(across // slices)
    ]
    theirs = lax.ppermute(currents[0], ("tm", "space"), pairs)

    own, up, down, far, packed = call(
        setup_kernel,
        ((4, *block), (10, 64, 256), (13, 64, 256), (1, 64, 256), (32, 48, 128)),
        (conductivity, currents[0], theirs, labels, coil_pattern, initial_state),
        small=(0, 1, 2),
        far=(3, 4, 5),
        scratch=(pltpu.VMEM(block, jnp.int32), (3, *block), block),
        copies=3,
        limit=60 << 20,
    )
    whole = exchange(packed, "space")
    table = whole[:8, 40, :]
    up, down = shifted(up, "space", 1, False), shifted(down, "space", -1, False)
    far = shifted(far, "space", -2, False)
    static, planes, advanced, state = call(
        first_sweep_kernel,
        ((5, *field), (64, 128), (8, 128), field),
        (where, table, whole),
        small=(0, 1),
        flops=1 << 26,
    )

    def fine(initial, planes, advanced, rest):
        fields, sums = call(
            functools.partial(fine_kernel, initial),
            ((9, 5, 64, 256), (32, 128)),
            (where, planes, own, up, down, *rest),
            small=(0,),
            scratch=((13, 64, 256), (11, 64, 256), (9, 64, 256), (3, 7, 64, 256), (3, 5, 64, 256)),
        )
        return call(
            finish_kernel,
            (block, (5, 64, 256), (8, 8, 128)),
            (exchange(sums, "space"), fields, advanced),
        )

    _, moved, ends = fine(True, planes, advanced, (far,))
    moved_first = shifted(moved, "tm", 1, True)
    planes, advanced, state, kept = call(
        next_sweep_kernel,
        ((64, 128), (8, 128), field, (16, 128)),
        (where, table, static, state, planes, *everywhere(ends, moved_first)),
        small=(0, 1),
        scratch=((8, *field),),
        flops=1 << 26,
    )
    around = (shifted(moved_first, "space", 1, False), shifted(moved_first, "space", -1, False))
    fine_state, moved, ends = fine(False, planes, advanced, (moved_first, *around))
    moved_other = shifted(moved, "tm", 1, False)
    (start,) = call(
        last_sweep_kernel,
        (block,),
        (where, table, static, state, kept, moved_first, moved_other, *everywhere(ends, moved_other)),
        small=(0, 1),
        scratch=(field, (8, *field), (16, 128)),
        flops=1 << 26,
    )
    return (start[None], fine_state[None])


def solution(mesh):
    in_specs = (
        P("space", None, None),
        P(),
        P(None, "space", None, None),
        P("tm", None, None),
        P("space", None, None),
    )
    out_specs = (P("tm", "space", None, None), P("tm", "space", None, None))
    return jax.shard_map(body, mesh=mesh, in_specs=in_specs, out_specs=out_specs, check_vma=False)
```

```python
import functools

import jax
import jax.numpy as jnp
from jax import lax
from jax.experimental import pallas as pl
from jax.experimental.pallas import tpu as pltpu
from jax.sharding import PartitionSpec as P

PHASES = 3
CG_COARSE = 4
F32 = jnp.float32
HIGHEST = lax.Precision.HIGHEST
VMEM = pltpu.MemorySpace.VMEM
SMEM = pltpu.MemorySpace.SMEM
INTERPRET = False
SHIFT = 4.0
LIMIT = 12 << 20


def iota(shape, dim):
    return lax.broadcasted_iota(jnp.int32, shape, dim)


def dot(a, b):
    return lax.dot_general(a, b, (((1,), (0,)), ((), ())), precision=HIGHEST, preferred_element_type=F32)


def total(x):
    while x.ndim > 2:
        x = jnp.sum(x, axis=0)
    return jnp.sum(jnp.sum(x, axis=0, keepdims=True), axis=1, keepdims=True)


def restrict_packed(summed):
    columns = (iota((256, 128), 0) >> 2) == (iota((256, 128), 1) & 63)
    rows = (iota((16, 64), 1) >> 2) == iota((16, 64), 0)
    half = dot(summed, jnp.where(columns, 1.0 / 64.0, 0.0).astype(F32))
    both = dot(jnp.where(rows, 1.0, 0.0).astype(F32), half)
    return jnp.where(iota((8, 128), 1) < 64, both[:8], both[8:])


def widen(planes):
    columns = (iota((128, 256), 1) >> 2) == iota((128, 256), 0)
    rows = (iota((64, 16), 0) >> 2) == iota((64, 16), 1)
    wide = dot(planes, jnp.where(columns, 1.0, 0.0).astype(F32))
    lift = jnp.where(rows, 1.0, 0.0).astype(F32)
    return [dot(lift, wide[k : k + 16]) for k in range(0, planes.shape[0], 16)]


def unpack(low, high):
    axis = low.ndim - 1
    left = iota(low.shape, axis) < 64
    top = jnp.where(left, low, pltpu.roll(high, 64, axis))
    bottom = jnp.where(left, pltpu.roll(low, 64, axis), high)
    return jnp.concatenate([top, bottom], axis=axis - 1)


def coarse_beside(v):
    one = (1, 16, 128)
    lane, row = iota(one, 2), iota((1, 8, 128), 1)
    left = lane < 64
    first, last = pltpu.roll(v[:1], 64, 2), pltpu.roll(v[15:], 64, 2)
    after = jnp.concatenate([v[1:], jnp.where(left, first, 0.0)], axis=0)
    before = jnp.concatenate([jnp.where(left, 0.0, last), v[:15]], axis=0)
    out = after + before
    up, down = pltpu.roll(v, 1, 1), pltpu.roll(v, 15, 1)
    up = jnp.concatenate([jnp.where(row == 0, 0.0, up[:, :8]), up[:, 8:]], axis=1)
    down = jnp.concatenate([down[:, :8], jnp.where(row == 7, 0.0, down[:, 8:])], axis=1)
    out = out + (up + down)
    inner = lane & 63
    return out + jnp.where(inner == 0, 0.0, pltpu.roll(v, 1, 2)) + jnp.where(inner == 63, 0.0, pltpu.roll(v, 127, 2))


def coarse_solve(start, source, diagonal):
    def apply(v):
        return diagonal * v - 0.0625 * coarse_beside(v)

    x = start
    residual = source - 0.375 * start + 0.0625 * coarse_beside(start)
    image = apply(residual)
    norm, product = total(residual * residual), total(residual * image)
    step = norm / product
    direction, moved = residual, image
    for turn in range(CG_COARSE):
        inverse = 1.0 / norm
        scaled = inverse / step
        x = x + step[None] * direction
        if turn + 1 < CG_COARSE:
            residual = residual - step[None] * moved
            image = apply(residual)
            new, product = total(residual * residual), total(residual * image)
            ratio = new * inverse
            step = new / (product - new * (new * scaled))
            direction = residual + ratio[None] * direction
            moved = image + ratio[None] * moved
            norm = new
    return x


def cut_planes(state, place, offsets):
    out = []
    lane = iota((16, 128), 1)
    for offset in offsets:
        at = place + offset
        inside = jnp.logical_and(at >= 0, at < 32).astype(jnp.int32)
        at = jnp.clip(at, 0, 31)
        plane = state[at & 15]
        plane = jnp.where((at >> 4) * jnp.ones_like(lane) == 1, pltpu.roll(plane, 64, 1), plane)
        out.append(jnp.where(lane < 64 * inside, plane, 0.0))
    return out


def call(body, outs, args, small=(), far=(), scratch=(), flops=0, copies=0, limit=LIMIT):
    spaces = [SMEM if k in small else pltpu.MemorySpace.HBM if k in far else VMEM for k in range(len(args))]
    specs = [pl.BlockSpec(memory_space=space) for space in spaces]
    return pl.pallas_call(
        body,
        out_shape=tuple(jax.ShapeDtypeStruct(s, F32) for s in outs),
        in_specs=specs,
        out_specs=tuple(pl.BlockSpec(memory_space=VMEM) for _ in outs),
        scratch_shapes=(
            *(pltpu.VMEM(s, F32) if isinstance(s, tuple) else s for s in scratch),
            *(pltpu.SemaphoreType.DMA for _ in range(copies)),
        ),
        cost_estimate=pl.CostEstimate(flops=flops, bytes_accessed=1 << 20, transcendentals=0) if flops else None,
        compiler_params=pltpu.CompilerParams(vmem_limit_bytes=limit),
        interpret=INTERPRET,
    )(*args)


def setup_kernel(cond, cur, theirs, labels_far, coils_far, initial_far, own, up, down, far, packed,
                 labels, coils, initial, labels_sem, coils_sem, initial_sem):
    copies = [
        pltpu.make_async_copy(labels_far, labels, labels_sem),
        pltpu.make_async_copy(coils_far, coils, coils_sem),
        pltpu.make_async_copy(initial_far, initial, initial_sem),
    ]
    for copy in copies:
        copy.start()
    copies[0].wait()
    region = labels[...]
    cell = jnp.where(region == 0, cond[0], 0.0)
    for k in range(1, 4):
        cell = cell + jnp.where(region == k, cond[k], 0.0)
    own[0] = cell
    copies[2].wait()
    own[3] = initial[...]
    copies[1].wait()
    pattern = [coils[p] for p in range(PHASES)]
    for step in range(2):
        source = cur[step, 0] * pattern[0]
        for p in range(1, PHASES):
            source = source + cur[step, p] * pattern[p]
        own[1 + step] = source
    up[0:2] = own[0, 2:4]
    up[2:5] = own[1, 1:4]
    up[5:6] = own[2, 3:4]
    down[0:3] = own[0, 0:3]
    down[3:7] = own[1]
    down[7:9] = own[2, 0:2]
    up[6:10] = initial[...]
    down[9:13] = initial[...]
    far[...] = initial[0:1]
    fields = [initial[...], cell, *pattern]
    rows = [restrict_packed(jnp.sum(f, axis=0)) for f in fields]
    lane = iota((8, 128), 1)
    row = jnp.zeros((8, 128), F32)
    for k in range(6):
        row = jnp.where(lane == k, theirs[k // 3, k % 3], row)
    rows = jnp.concatenate([*rows, row], axis=0)
    packed[...] = jnp.broadcast_to(rows[None], packed.shape)


def unpack_all(whole, at):
    return unpack(whole[0:16, at : at + 8, :], whole[16:32, at : at + 8, :])


def slice_source(cur, static, n):
    source = jnp.zeros((16, 16, 128), F32)
    for p in range(PHASES):
        source = source + 0.5 * (cur[n, p] + cur[n, PHASES + p]) * static[2 + p]
    return source


def solve_slice(cur, state, static, n):
    state[...] = coarse_solve(state[...], slice_source(cur, static, n), 0.5 * static[1] + 0.375)


AROUND = (-1, 0, 1, 2)


def first_sweep_kernel(where, cur, whole, static, planes, advanced, state):
    mine, place = where[0], where[1]
    for k in range(5):
        static[k] = unpack_all(whole, 8 * k)
    state[...] = static[0]

    def turn(n, carry):
        @pl.when(n == mine)
        def _():
            for k, plane in enumerate(cut_planes(state, place, AROUND)):
                planes[16 * k : 16 * k + 16] = plane

        solve_slice(cur, state, static, n)

        @pl.when(n == mine)
        def _():
            advanced[...] = pack(*cut_planes(state, place, (0,)))

        return carry

    lax.fori_loop(0, 8, turn, 0)


def pack(plane):
    return plane[:8] + pltpu.roll(plane[8:], 64, 1)


def load_corrections(where, ours, theirs, correction):
    odd = where[1] & 1
    for k in range(4):
        correction[4 * odd + k] = unpack_all(ours, 8 * k)
        correction[4 * (1 - odd) + k] = unpack_all(theirs, 8 * k)


def next_sweep_kernel(where, cur, static, begin, old, ours, theirs, planes, advanced, state, kept, correction):
    mine, place = where[0], where[1]
    load_corrections(where, ours, theirs, correction)
    state[...] = begin[...]

    @pl.when(mine == 0)
    def _():
        for k, plane in enumerate(cut_planes(state, place, AROUND)):
            planes[16 * k : 16 * k + 16] = plane

    def turn(n, carry):
        solve_slice(cur, state, static, n)

        @pl.when(n == mine)
        def _():
            advanced[...] = pack(*cut_planes(state, place, (0,)))

        @pl.when(n == mine - 1)
        def _():
            around = cut_planes(state, place, AROUND)
            kept[...] = around[1]
            for k, plane in enumerate(around):
                planes[16 * k : 16 * k + 16] = plane - old[16 * k : 16 * k + 16]

        @pl.when(jnp.logical_and(n == 7, mine == 0))
        def _():
            (new,), (before,) = cut_planes(state, place, (0,)), cut_planes(begin, place, (0,))
            kept[...] = new - before

        state[...] = state[...] + correction[n]
        return carry

    lax.fori_loop(0, 8, turn, 0)


def last_sweep_kernel(where, cur, static, begin, kept, moved_first, moved_other, ours, theirs,
                      start, state, correction, plane):
    mine, place = where[0], where[1]
    load_corrections(where, ours, theirs, correction)
    state[...] = begin[...]
    plane[...] = kept[...]

    def turn(n, carry):
        solve_slice(cur, state, static, n)

        @pl.when(n == mine - 1)
        def _():
            (new,) = cut_planes(state, place, (0,))
            plane[...] = new - kept[...]

        state[...] = state[...] + correction[n]
        return carry

    lax.fori_loop(0, mine, turn, 0)
    (own,) = widen(plane[...])
    first = (mine == 0).astype(F32)
    start[...] = own[None] + (first * moved_first[0:4] + (1.0 - first) * moved_other[0:4])


def fine_beside(v):
    head, tail = iota((8, 256), 0), iota((64, 128), 1)
    before, after = pltpu.roll(v, 1, 0), pltpu.roll(v, 63, 0)
    before = jnp.concatenate([jnp.where(head == 0, 0.0, before[:8]), before[8:]], axis=0)
    after = jnp.concatenate([after[:56], jnp.where(head == 7, 0.0, after[56:])], axis=0)
    left, right = pltpu.roll(v, 1, 1), pltpu.roll(v, 255, 1)
    left = jnp.concatenate([jnp.where(tail == 0, 0.0, left[:, :128]), left[:, 128:]], axis=1)
    right = jnp.concatenate([right[:, :128], jnp.where(tail == 127, 0.0, right[:, 128:])], axis=1)
    return (before + after) + (left + right)


def inside(plane):
    return jnp.logical_and(plane >= 0, plane < 128).astype(F32)


def guarded(value, plane, first):
    return value if 0 <= plane < 4 else inside(first + plane) * value


def part(value):
    folded = jnp.sum(value.reshape(8, 8, 256), axis=0)
    return folded[:, :128] + folded[:, 128:]


def fine_kernel(initial, where, planes, own, up, down, *refs):
    if initial:
        (rest_far,), refs = refs[:1], refs[1:]
        rest, rest_up, rest_down = own.at[3], up, down
    else:
        (rest, rest_up, rest_down), refs = refs[:3], refs[3:]
        rest_far = rest_down.at[4:5]
    fields, packed, u, r, w, q, a = refs
    first = 4 * where[1]
    zero = (where[0] == 0).astype(F32)
    scale = (1.0 - zero, zero) if initial else (1.0, 1.0 - zero)
    above, below = (6, 9) if initial else (0, 0)
    lifted = widen(planes[...])
    pieces = [(rest_up, above + k) for k in range(4)] + [(rest, k) for k in range(4)]
    pieces = pieces + [(rest_down, below + k) for k in range(4)] + [(rest_far, 0)]
    for j, (piece, k) in enumerate(pieces):
        u[j] = scale[0] * lifted[j // 4] + scale[1] * piece[k]

    def weight(plane):
        return up[2 + plane] if plane < 0 else own[0, plane] if plane < 4 else down[plane - 4]

    def source(step, plane):
        before, after = ((5, 3), (6, 7))[step]
        return up[before + plane] if plane < 0 else own[1 + step, plane] if plane < 4 else down[after + plane - 4]

    def beside(field, low, plane):
        j = plane - low
        return field[j - 1] + field[j + 1] + fine_beside(field[j])

    def spread(field, low, plane):
        return beside(field, low, plane) - 6.0 * field[plane - low]

    for plane in range(-3, 8):
        lap = spread(u, -4, plane)
        r[plane + 3] = guarded(source(0, plane) + lap, plane, first)
        if -1 <= plane < 6:
            q[0, plane + 1] = guarded(source(1, plane) + lap, plane, first)
    for plane in range(-2, 7):
        v, around = r[plane + 3], beside(r, -3, plane)
        w[plane + 2] = guarded((weight(plane) + (6.0 - SHIFT)) * v - around, plane, first)
        if -1 <= plane < 6:
            q[1, plane + 1] = guarded(around - 6.0 * v, plane, first)
    for plane in range(-1, 6):
        q[2, plane + 1] = guarded(spread(w, -2, plane), plane, first)
    for plane in range(5):
        for k in range(3):
            image = (weight(plane) + (6.0 - SHIFT)) * q[k, plane + 1] - beside(q.at[k], -1, plane)
            a[k, plane] = guarded(image, plane, first)
    sums = [jnp.zeros((8, 128), F32)] * 28
    for plane in range(4):
        terms = []
        rv, wv = r[plane + 3], w[plane + 2]
        heavy = weight(plane) + 6.0
        terms += [rv * rv, rv * wv, wv * wv]
        terms += [wv * (weight(plane) * wv - q[2, plane + 1] + w[plane + 1] - w[plane + 3])]
        qs = [q[k, plane + 1] for k in range(3)]
        images = [a[k, plane] for k in range(3)]
        twice = []
        for k in range(3):
            value = heavy * images[k] - fine_beside(images[k]) - a[k, plane + 1]
            twice.append(value - a[k, plane - 1] if plane else value)
        for i, j in PAIRS:
            last = images[i] * twice[j]
            if plane == 3:
                last = last - a[i, 4] * images[j]
            terms += [qs[i] * qs[j], qs[i] * images[j], images[i] * images[j], last]
        sums = [s + part(v) for s, v in zip(sums, terms)]
    lane = iota((1, 128), 1)
    row = jnp.zeros((1, 128), F32)
    for k in range(28):
        row = jnp.where(lane == k, total(sums[k]), row)
    packed[...] = jnp.broadcast_to(row, packed.shape)
    fields[0] = u[4:9]
    fields[1] = r[3:8]
    fields[2] = w[2:7]
    for k in range(3):
        fields[3 + k] = q[k, 1:6]
        fields[6 + k] = a[k, 0:5]


PAIRS = ((0, 0), (0, 1), (0, 2), (1, 1), (1, 2), (2, 2))


def weights(norm, cross, square, product):
    first = cross + SHIFT * norm
    step = norm / first
    keep = 1.0 - SHIFT * step
    new = keep * keep * norm - 2.0 * keep * step * cross + step * step * square
    second = keep * keep * first - 2.0 * keep * step * (square + SHIFT * cross) + step * step * product
    ratio = new / norm
    second = new / (second - ratio * new / step)
    return step + second * (keep + ratio), -second * step


def finish_kernel(sums, fields, advanced, fine, moved, ends):
    row = jnp.sum(sums[...], axis=0, keepdims=True)
    lane = iota((1, 128), 1)
    m = [jnp.sum(jnp.where(lane == k, row, 0.0), axis=1, keepdims=True) for k in range(28)]
    a, b = weights(*m[:4])
    factor = {(0, 0): 1.0, (0, 1): 2.0 * a, (0, 2): 2.0 * b, (1, 1): a * a, (1, 2): 2.0 * (a * b), (2, 2): b * b}
    after = [sum(factor[pair] * m[4 + 4 * p + k] for p, pair in enumerate(PAIRS)) for k in range(4)]
    c, d = weights(*after)
    scales = (None, a, b, c, c * a, c * b, d, d * a, d * b)
    for i in range(5):
        value = fields[0, i]
        for k in range(1, 9):
            value = value + scales[k] * fields[k, i]
        moved[i] = value
        if i < 4:
            fine[i] = value
    own = restrict_packed(jnp.sum(moved[0:4], axis=0))
    ends[...] = jnp.broadcast_to((own - advanced[...])[None], ends.shape)


def spread_kernel(ends, rest, packed):
    for half in range(2):
        rows = ends[4 * half : 4 * half + 4].reshape(1, 32, 128)
        for k in range(half, packed.shape[0], 2):
            packed[k : k + 1] = rows


def shifted(x, axis, by, ring):
    n = lax.axis_size(axis)
    pairs = [(i, (i + by) % n) for i in range(n) if ring or 0 <= i + by < n]
    return lax.ppermute(x, axis, pairs)


def exchange(x, axis):
    return lax.all_to_all(x, axis, split_axis=0, concat_axis=0, tiled=True)


def everywhere(ends, rest):
    (packed,) = call(spread_kernel, ((32, 32, 128),), (exchange(ends, "tm"), rest), far=(1,))
    half = exchange(packed, "space")
    places = lax.axis_size("space")
    return half, lax.ppermute(half, "space", [(i, i ^ 1) for i in range(places)])


def body(labels, conductivity, coil_pattern, currents, initial_state):
    tm, place = lax.axis_index("tm"), lax.axis_index("space")
    where = jnp.stack([tm, place]).astype(jnp.int32)
    block, field = (4, 64, 256), (16, 16, 128)

    slices, across = lax.axis_size("tm"), lax.axis_size("space")
    pairs = [
        (b * across + slices * a + t, t * across + slices * a + b)
        for t in range(slices)
        for b in range(slices)
        for a in range(across // slices)
    ]
    theirs = lax.ppermute(currents[0], ("tm", "space"), pairs)

    own, up, down, far, packed = call(
        setup_kernel,
        ((4, *block), (10, 64, 256), (13, 64, 256), (1, 64, 256), (32, 48, 128)),
        (conductivity, currents[0], theirs, labels, coil_pattern, initial_state),
        small=(0, 1, 2),
        far=(3, 4, 5),
        scratch=(pltpu.VMEM(block, jnp.int32), (3, *block), block),
        copies=3,
        limit=60 << 20,
    )
    whole = exchange(packed, "space")
    table = whole[:8, 40, :]
    up, down = shifted(up, "space", 1, False), shifted(down, "space", -1, False)
    far = shifted(far, "space", -2, False)
    static, planes, advanced, state = call(
        first_sweep_kernel,
        ((5, *field), (64, 128), (8, 128), field),
        (where, table, whole),
        small=(0, 1),
        flops=1 << 26,
    )

    def fine(initial, planes, advanced, rest):
        fields, sums = call(
            functools.partial(fine_kernel, initial),
            ((9, 5, 64, 256), (32, 128)),
            (where, planes, own, up, down, *rest),
            small=(0,),
            scratch=((13, 64, 256), (11, 64, 256), (9, 64, 256), (3, 7, 64, 256), (3, 5, 64, 256)),
        )
        return call(
            finish_kernel,
            (block, (5, 64, 256), (8, 8, 128)),
            (exchange(sums, "space"), fields, advanced),
        )

    _, moved, ends = fine(True, planes, advanced, (far,))
    moved_first = shifted(moved, "tm", 1, True)
    planes, advanced, state, kept = call(
        next_sweep_kernel,
        ((64, 128), (8, 128), field, (16, 128)),
        (where, table, static, state, planes, *everywhere(ends, moved_first)),
        small=(0, 1),
        scratch=((8, *field),),
        flops=1 << 26,
    )
    around = (shifted(moved_first, "space", 1, False), shifted(moved_first, "space", -1, False))
    fine_state, moved, ends = fine(False, planes, advanced, (moved_first, *around))
    moved_other = shifted(moved, "tm", 1, False)
    (start,) = call(
        last_sweep_kernel,
        (block,),
        (where, table, static, state, kept, moved_first, moved_other, *everywhere(ends, moved_other)),
        small=(0, 1),
        scratch=(field, (8, *field), (16, 128)),
        flops=1 << 26,
    )
    return (start[None], fine_state[None])


def solution(mesh):
    in_specs = (
        P("space", None, None),
        P(),
        P(None, "space", None, None),
        P("tm", None, None),
        P("space", None, None),
    )
    out_specs = (P("tm", "space", None, None), P("tm", "space", None, None))
    return jax.shard_map(body, mesh=mesh, in_specs=in_specs, out_specs=out_specs, check_vma=False)
```
